256 devices in a mesh: blk: 256 (over y, z, x, core).
Axes of the slice: x: 4, y: 4, z: 8, core: 2. Of those that a mesh axis runs over, the one named last changes fastest.
Arguments:
- image_features: bfloat16 [65536, 1536], P('blk'), may hold values from -0.5 to 0.5
- head_weight: bfloat16 [1536, 1152], P('blk'), may hold values from -0.15625 to 0.15625
- text_embeds: bfloat16 [65536, 1152], P('blk'), may hold values from -0.29882812 to 0.29882812
- natural_exponent_factor: float32 [1], replicated, may hold values from 1.6 to 2.6
- logit_bias: float32 [1], replicated, may hold values from -4 to -1
Outputs:
- grad_features: bfloat16 [65536, 1536], P('blk')
- grad_text: bfloat16 [65536, 1152], P('blk')
- grad_weight: float32 [1536, 1152], P('blk')
The draws below stay inside these ranges and needn't reach their ends.
All inputs are finite; a program needn't handle non-finite values.
Results may differ from the reference program's by a relative error of at most 0.0085.
Values may be sent and summed in bfloat16 or wider, within the bound.
A program may use at most 64 MiB of HBM per device.

```python
import jax
import jax.numpy as jnp
from jax import lax

D = 1536
E = 1152
R = 256
S = 4
TOTAL = 65536
N_BLK = 256


def strengthened(entries, rng, source, target, blocks, factor):
    owner, partner = [(jnp.arange(entries.shape[axis_at]) // (entries.shape[axis_at] // blocks)).reshape([-1 if axis == axis_at else 1 for axis in range(entries.ndim)]) for axis_at in (source, target)]
    chosen = jax.random.permutation(rng, blocks)[partner]
    strong = (owner == chosen) | (owner == (partner + blocks // 2) % blocks)
    return jnp.where(strong, factor * entries, entries)


def levels(rng, extent, split, least, largest):
    def one(position, parts):
        steps = jax.random.uniform(jax.random.fold_in(jax.random.fold_in(rng, 6), position), (parts,), jnp.float32, least / len(split), largest / len(split))
        return jnp.repeat(jnp.exp(steps), extent[position] // parts).reshape((-1,) + (1,) * (len(extent) - position - 1))

    level = one(*split[0])
    for cut in split[1:]:
        level = level * one(*cut)
    return level


def bell_draw(stream_key, dims, scale, bound, pieces=(), kind=jnp.bfloat16):
    drawn = jax.random.normal(stream_key, dims, jnp.float32) * scale
    if len(pieces) > 0:
        drawn = levels(stream_key, dims, pieces, -0.22, 0.18) * drawn
    return jnp.clip(drawn, min=-bound, max=bound).astype(kind)


def heavy_noise(key, shape, spread, reach, pieces, heavy, kind=jnp.bfloat16):
    drawn = spread * jax.random.normal(key, shape, jnp.float32)
    if pieces:
        drawn = drawn * levels(key, shape, pieces, -0.22, 0.18)
    return jnp.clip(strengthened(drawn, jax.random.fold_in(key, 3), *heavy), -reach, reach).astype(kind)


def setup_inputs(seed: int = 0) -> dict:
    streams_of = jax.random.split(jax.random.key(seed), 6)
    return {
        "image_features": heavy_noise(streams_of[0], (TOTAL, D), 0.02, 0.5, ((0, 256),), (0, 1, 256, 6.0)),
        "head_weight": bell_draw(streams_of[1], (D, E), D ** -0.5, 0.15625, ((0, 256),)),
        "text_embeds": bell_draw(streams_of[2], (TOTAL, E), 0.05, 0.29882812, ((0, 256),)),
        "natural_exponent_factor": jnp.clip(jax.random.uniform(streams_of[3], (1,), jnp.float32, 1.6, 2.6), 1.6, 2.6),
        "logit_bias": jnp.clip(jax.random.uniform(streams_of[4], (1,), jnp.float32, -4.0, -1.0), -4.0, -1.0),
    }


epsilon = 1e-06

def normalize(rows):
    squares = lax.optimization_barrier(jnp.sum(rows * rows, axis=1, keepdims=True))
    length = jnp.sqrt(squares + epsilon)
    return (rows / length, length)

def similarity_derivative(picture_sample_group, caption_sample_group, similarity_multiplier, neighbour_distance, outer_dimension_size):
    similarity_matrix = similarity_multiplier * lax.dot_general(picture_sample_group, caption_sample_group, (((1,), (1,)), ((), ())), preferred_element_type=jnp.float32) + neighbour_distance
    if outer_dimension_size:
        matched = lax.broadcasted_iota(jnp.int32, similarity_matrix.shape, 0) == lax.broadcasted_iota(jnp.int32, similarity_matrix.shape, 1)
        match_polarity = jnp.where(matched, 1.0, -1.0).astype(jnp.float32)
    else:
        match_polarity = -jnp.ones(similarity_matrix.shape, jnp.float32)
    return (-similarity_multiplier * match_polarity * jax.nn.sigmoid(-match_polarity * similarity_matrix)).astype(jnp.bfloat16)

def project_back(grad, unit_rows, length):
    return (grad - unit_rows * lax.optimization_barrier(jnp.sum(unit_rows * grad, axis=1, keepdims=True))) / length

def reference(image_features, head_weight, text_embeds, natural_exponent_factor, logit_bias):
    embedded = jnp.dot(image_features, head_weight, preferred_element_type=jnp.float32)
    image_unit, image_length = normalize(embedded)
    picture_embedding_mapped = image_unit.astype(jnp.bfloat16)
    text_unit, text_length = normalize(text_embeds.astype(jnp.float32))
    text_low = text_unit.astype(jnp.bfloat16)
    similarity_multiplier = jnp.exp(natural_exponent_factor[0])
    neighbour_distance = logit_bias[0]
    image_blocks = picture_embedding_mapped.reshape(N_BLK, R, E)
    text_blocks = text_low.reshape(N_BLK, R, E)

    def pick_block(blocks, block_id):
        where_at = ((block_id + N_BLK) % N_BLK).astype(jnp.int32)
        return lax.dynamic_index_in_dim(blocks, where_at, 0, keepdims=False)

    def image_side(block_id):
        picture_sample_group = pick_block(image_blocks, block_id)
        summed = jnp.zeros((R, E), jnp.float32)
        for partition_portion in range(S):
            caption_sample_group = pick_block(text_blocks, block_id + partition_portion)
            mapping_matrix = similarity_derivative(picture_sample_group, caption_sample_group, similarity_multiplier, neighbour_distance, partition_portion == 0)
            summed = summed + jnp.dot(mapping_matrix, caption_sample_group, preferred_element_type=jnp.float32)
        return summed

    def text_side(block_id):
        caption_sample_group = pick_block(text_blocks, block_id)
        summed = jnp.zeros((R, E), jnp.float32)
        for partition_portion in range(S):
            picture_sample_group = pick_block(image_blocks, block_id - partition_portion)
            mapping_matrix = similarity_derivative(picture_sample_group, caption_sample_group, similarity_multiplier, neighbour_distance, partition_portion == 0)
            summed = summed + lax.dot_general(mapping_matrix, picture_sample_group, (((0,), (0,)), ((), ())), preferred_element_type=jnp.float32)
        return summed
    block_ids = jnp.arange(N_BLK, dtype=jnp.int32)
    image_grad = lax.map(image_side, block_ids).reshape(-1, E)
    text_grad = lax.map(text_side, block_ids).reshape(-1, E)
    embed_grad = project_back(image_grad, image_unit, image_length).astype(jnp.bfloat16)
    grad_text = project_back(text_grad, text_unit, text_length).astype(jnp.bfloat16)
    grad_features = lax.dot_general(embed_grad, head_weight, (((1,), (1,)), ((), ())), preferred_element_type=jnp.float32).astype(jnp.bfloat16)
    grad_weight = lax.dot_general(image_features, embed_grad, (((0,), (0,)), ((), ())), preferred_element_type=jnp.float32)
    return (grad_features, grad_text, grad_weight)
```

```python
import jax
import jax.numpy as jnp
from jax import lax
from jax.experimental import pallas as pl
from jax.experimental.pallas import tpu as pltpu
from jax.sharding import PartitionSpec as P

MESH = pl.DeviceIdType.MESH
D, E, R, S = 1536, 1152, 256, 4
NY, NZ, NX = 4, 8, 4
N = NY * NZ * NX * 2
ROW = NX * 2
SH = D // N
BLK = SH * ROW
YROWS = BLK * NZ
W1 = 640
COLS = ((W1, E - W1), (0, W1))
EPS = 1e-06
F32, BF16 = jnp.float32, jnp.bfloat16
Z_ORDER = (4, 3, 5, 2, 6, 1, 7)
Z_ARRIVAL = (0, 1, 7, 2, 6, 3, 5, 4)
ORDER_NT = (((1,), (1,)), ((), ()))


def dot(a, b):
    return jnp.dot(a, b, preferred_element_type=F32)


def dot_nt(a, b):
    return lax.dot_general(a, b, ORDER_NT, preferred_element_type=F32)


def kernel(
    feat_hbm, w_hbm, text_hbm, nef_ref, bias_ref,
    gf_hbm, gt_hbm, gw_hbm,
    w_ref, feat, feat2, feat_t, unit, length, img, traw, tlow, tlen, pair, eg, gfeat, gtext,
    gpart, xbuf, wrow, rbuf, sbuf, xrow, xs, xr, gout,
    in_sem, out_sem, xw_s, xw_r, ag_s, ag_r, dd_s, dd_r, ex_s, ex_r, rs_s, rs_r, xg_s, xg_r,
):
    me = lax.axis_index("blk")
    core = lax.rem(me, 2)
    r = lax.rem(me, ROW)
    z = lax.rem(lax.div(me, ROW), NZ)
    y = lax.div(me, ROW * NZ)
    pending = []

    def dev(dy=0, dz=0):
        return (lax.rem(y + (dy + NY) , NY) * NZ + lax.rem(z + (dz + NZ), NZ)) * ROW + r

    def row_dev(k):
        return me - r + lax.rem(r + k, ROW)

    def near(k):
        return lax.rem(me + (k + N), N)

    def remote(src, dst, ss, rs, to):
        return pltpu.make_async_remote_copy(
            src_ref=src, dst_ref=dst, send_sem=ss, recv_sem=rs, device_id=(to,), device_id_type=MESH
        )

    def send(only, src, dst, ss, rs, to, like=None):
        sems, i = ss
        remote(src, dst, sems.at[i], rs, to).start()

        def wait():
            ref = src if like is None else like()
            remote(ref, ref, sems.at[i], sems.at[i], near(1)).wait_send()

        pending.append((only, wait))

    def arrived(dst, ss, rs):
        remote(dst, dst, ss, rs, near(1)).wait_recv()

    def wblock(ref, yy, zz, c0, cw):
        start = pl.multiple_of(lax.rem(yy, NY) * YROWS + lax.rem(zz, NZ) * BLK, 8)
        return ref.at[pl.ds(start, BLK), pl.ds(c0, cw)]

    cp_w = pltpu.make_async_copy(w_hbm, xbuf.at[r], in_sem.at[0])
    cp_t = pltpu.make_async_copy(text_hbm, traw.at[0], in_sem.at[1])
    cp_f = pltpu.make_async_copy(feat_hbm, feat, in_sem.at[2])
    cp_w.start()
    cp_t.start()
    cp_f.start()

    barrier = pltpu.get_barrier_semaphore()
    peers = [row_dev(k) for k in range(1, ROW)] + [dev(dz=k) for k in range(1, NZ)]
    peers += [dev(dy=k) for k in range(1, NY)] + [near(k) for k in (-3, -2, -1, 1, 2, 3)]
    for peer in peers:
        pl.semaphore_signal(barrier, inc=1, device_id=(peer,), device_id_type=MESH)
    pl.semaphore_wait(barrier, len(peers))

    cp_w.wait()
    for k in (4, 3, 5, 2, 6, 1, 7):
        send(None, xbuf.at[r], xbuf.at[r], (xw_s, k), xw_r.at[k], row_dev(k), lambda: xbuf.at[0])

    cp_t.wait()

    @pl.when(core == 0)
    def _():
        send(0, traw.at[0], traw.at[1], (ex_s, 0), ex_r.at[1], near(-1), lambda: traw.at[0])
        send(0, traw.at[0], traw.at[3], (ex_s, 1), ex_r.at[3], near(-3), lambda: traw.at[0])

    @pl.when(core == 1)
    def _():
        send(1, traw.at[0], traw.at[1], (ex_s, 0), ex_r.at[1], near(-1), lambda: traw.at[0])
        send(1, traw.at[0], traw.at[2], (ex_s, 1), ex_r.at[2], near(-2), lambda: traw.at[0])

    cp_f.wait()
    send(None, feat, feat2, (ex_s, 4), ex_r.at[0], me + 1 - 2 * core)

    for k in range(1, ROW):
        arrived(xbuf.at[lax.rem(r + (ROW - k), ROW)], xw_s.at[k], xw_r.at[k])
    for k in range(ROW):
        wrow[pl.ds(SH * k, SH), :] = xbuf[k].astype(F32)
    own = pl.multiple_of(y * YROWS + z * BLK, 8)
    w_ref[pl.ds(own, BLK), :] = wrow[...].astype(BF16)

    def gather(c):
        c0, cw = COLS[c]
        sibling = me + (1 - 2 * c)
        count = [0]
        like = lambda: w_ref.at[pl.ds(0, BLK), pl.ds(c0, cw)]

        def put(j, k, dy, dz):
            part = wblock(w_ref, y + (NY - j), z + (NZ - k), c0, cw)
            idx = ((j + dy) % NY) * NZ + (k + dz) % NZ
            send(c, part, part, (ag_s, count[0]), ag_r.at[idx], dev(dy, dz), like)
            count[0] += 1

        def share(j, k):
            part = wblock(w_ref, y + (NY - j), z + (NZ - k), c0, cw)
            send(c, part, part, (dd_s, j * NZ + k), dd_r.at[j * NZ + k], sibling, like)

        def got(j, k):
            part = wblock(w_ref, y + (NY - j), z + (NZ - k), c0, cw)
            arrived(part, ag_s.at[0], ag_r.at[j * NZ + k])
            return part

        if c == 1:
            for k in Z_ORDER:
                put(0, 0, 0, k)

            def stage1(i):
                k = Z_ARRIVAL[i]
                if k:
                    got(0, k)
                put(0, k, 1, 0)
                put(0, k, -1, 0)
                if k:
                    share(0, k)

            def stage2(i):
                k = Z_ARRIVAL[i]
                got(1, k)
                if i % 2 == 0:
                    put(1, k, 1, 0)
                share(1, k)
                got(3, k)
                if i % 2 == 1:
                    put(3, k, -1, 0)
                share(3, k)

            def stage3(i):
                k = Z_ARRIVAL[i]
                got(2, k)
                share(2, k)

            for i in range(NZ + 4):
                if i < NZ:
                    stage1(i)
                if 2 <= i < NZ + 2:
                    stage2(i - 2)
                if 4 <= i:
                    stage3(i - 4)
        else:
            for j in (2, 1, 3):
                put(0, 0, j, 0)
            for j in (0, 1, 3, 2):
                if j:
                    got(j, 0)
                put(j, 0, 0, 1)
                put(j, 0, 0, -1)
                if j:
                    share(j, 0)
            for h in (1, 2, 3):
                for j in (0, 1, 3, 2):
                    got(j, h)
                    if h < 3 or j in (0, 3):
                        put(j, h, 0, 1)
                    share(j, h)
                    got(j, NZ - h)
                    if h < 3 or j in (1, 2):
                        put(j, NZ - h, 0, -1)
                    share(j, NZ - h)
            for j in (0, 1, 3, 2):
                got(j, 4)
                share(j, 4)
        o0, ow = COLS[1 - c]
        if c == 1:
            arrived(traw.at[1], ex_s.at[0], ex_r.at[1])
            send(1, traw.at[1], traw.at[2], (ex_s, 2), ex_r.at[2], near(-1), lambda: traw.at[0])
            arrived(traw.at[2], ex_s.at[0], ex_r.at[2])
            send(1, traw.at[2], traw.at[3], (ex_s, 3), ex_r.at[3], near(-1), lambda: traw.at[0])
        for j in range(NY):
            for k in range(NZ):
                if j or k:
                    part = wblock(w_ref, y + (NY - j), z + (NZ - k), o0, ow)
                    arrived(part, dd_s.at[0], dd_r.at[j * NZ + k])

    def text_norm(s):
        @pl.loop(0, R // 32)
        def _(i):
            rows = pl.ds(pl.multiple_of(i * 32, 32), 32)
            t = traw[s, rows, :].astype(F32)
            inv = 1.0 / jnp.sqrt(jnp.sum(t * t, axis=1, keepdims=True) + EPS)
            tlow[pl.ds(pl.multiple_of(s * R + i * 32, 32), 32), :] = (t * inv).astype(BF16)
            if s == 0:
                tlen[rows, :] = inv

    def transpose(src, col):
        @pl.loop(0, D // 256)
        def _(i):
            cols = pl.ds(pl.multiple_of(i * 256, 256), 256)
            feat_t[cols, pl.ds(col, R)] = jnp.transpose(src[:, cols])

    @pl.when(core == 0)
    def _():
        gather(0)

    @pl.when(core == 1)
    def _():
        gather(1)

    @pl.loop(0, E // 384)
    def _(i):
        cols = pl.ds(pl.multiple_of(i * 384, 384), 384)
        unit[:, cols] = dot(feat[...], w_ref[:, cols])

    @pl.loop(0, R // 32)
    def _(i):
        rows = pl.ds(pl.multiple_of(i * 32, 32), 32)
        e = unit[rows, :]
        inv = 1.0 / jnp.sqrt(jnp.sum(e * e, axis=1, keepdims=True) + EPS)
        u = e * inv
        unit[rows, :] = u
        length[rows, :] = inv
        img[rows, :] = u.astype(BF16)

    def slot(k):
        return img.at[pl.ds(k * R, R), :]

    @pl.when(core == 1)
    def _():
        send(1, slot(0), slot(1), (ex_s, 5), ex_r.at[5], near(1), lambda: slot(0))
        send(1, slot(0), slot(3), (ex_s, 6), ex_r.at[7], near(3), lambda: slot(0))

    @pl.when(core == 0)
    def _():
        send(0, slot(0), slot(1), (ex_s, 5), ex_r.at[5], near(1), lambda: slot(0))
        send(0, slot(0), slot(2), (ex_s, 6), ex_r.at[6], near(2), lambda: slot(0))

    text_norm(0)
    transpose(feat, 0)
    arrived(feat2, ex_s.at[4], ex_r.at[0])
    transpose(feat2, R)

    @pl.when(core == 0)
    def _():
        arrived(traw.at[1], ex_s.at[0], ex_r.at[1])
        arrived(traw.at[2], ex_s.at[0], ex_r.at[2])

    arrived(traw.at[3], ex_s.at[0], ex_r.at[3])
    for s in range(1, S):
        text_norm(s)

    factor = jnp.exp(jnp.full((1, R), nef_ref[0], F32))
    bias = bias_ref[0]

    def derivative(logit_dot, diagonal):
        logits = factor * logit_dot + bias
        if diagonal:
            same = lax.broadcasted_iota(jnp.int32, (R, R), 0) == lax.broadcasted_iota(jnp.int32, (R, R), 1)
            label = jnp.where(same, 1.0, -1.0).astype(F32)
            g = -factor * label / (1.0 + jnp.exp(label * logits))
        else:
            g = factor / (1.0 + jnp.exp(-logits))
        return g.astype(BF16)

    def back(grad, u, inv):
        return (grad - u * jnp.sum(u * grad, axis=1, keepdims=True)) * inv

    for s in range(S):
        pair[:, pl.ds(s * R, R)] = derivative(dot_nt(img[pl.ds(0, R), :], tlow[pl.ds(s * R, R), :]), s == 0)

    @pl.loop(0, R // 32)
    def _(i):
        rows = pl.ds(pl.multiple_of(i * 32, 32), 32)
        grad = dot(pair[rows, :], tlow[...])
        eg[rows, :] = back(grad, unit[rows, :], length[rows, :]).astype(BF16)

    @pl.when(core == 0)
    def _():
        part = pl.ds(COLS[1][0], COLS[1][1])
        send(0, eg.at[pl.ds(0, R), part], eg.at[pl.ds(R, R), part], (ex_s, 9), ex_r.at[9], me + 1, lambda: eg.at[pl.ds(0, R), pl.ds(COLS[1][0], COLS[1][1])])

    @pl.when(core == 1)
    def _():
        part = pl.ds(COLS[0][0], COLS[0][1])
        send(1, eg.at[pl.ds(0, R), part], eg.at[pl.ds(R, R), part], (ex_s, 9), ex_r.at[9], me - 1, lambda: eg.at[pl.ds(0, R), pl.ds(COLS[0][0], COLS[0][1])])

    @pl.loop(0, D // 384)
    def _(i):
        cols = pl.ds(pl.multiple_of(i * 384, 384), 384)
        gfeat[:, cols] = dot_nt(eg[pl.ds(0, R), :], w_ref[cols, :]).astype(BF16)

    cp_gf = pltpu.make_async_copy(gfeat, gf_hbm, out_sem.at[0])
    cp_gf.start()

    def text_forward():
        @pl.when(core == 0)
        def _():
            arrived(slot(1), ex_s.at[0], ex_r.at[5])
            send(0, slot(1), slot(2), (ex_s, 7), ex_r.at[6], near(1), lambda: slot(0))
            arrived(slot(2), ex_s.at[0], ex_r.at[6])
            send(0, slot(2), slot(3), (ex_s, 8), ex_r.at[7], near(1), lambda: slot(0))

        @pl.when(core == 1)
        def _():
            arrived(slot(1), ex_s.at[0], ex_r.at[5])
            arrived(slot(2), ex_s.at[0], ex_r.at[6])

        arrived(slot(3), ex_s.at[0], ex_r.at[7])

    def reduce_weight(c):
        c0, cw = COLS[c]
        count = [0]
        arrived(eg.at[pl.ds(R, R), pl.ds(c0, cw)], ex_s.at[0], ex_r.at[9])

        def product(j):
            rows = pl.ds(pl.multiple_of(lax.rem(y + j, NY) * YROWS, 8), YROWS)
            gpart[rows, pl.ds(0, cw)] = dot(feat_t[rows, :], eg[:, pl.ds(c0, cw)]).astype(BF16)

        def mine(dy, dz):
            return wblock(gpart, y + (dy + NY), z + (dz + NZ), 0, cw)

        def buf(i):
            return rbuf.at[i, :, pl.ds(0, cw)]

        def emit(src, i, dy, dz):
            send(c, src, buf(i), (rs_s, count[0]), rs_r.at[i], dev(dy, dz), lambda: buf(0))
            count[0] += 1

        def take(i):
            arrived(buf(i), rs_s.at[0], rs_r.at[i])
            return buf(i)[...].astype(F32)

        if c == 1:
            product(2)
            for i, k in enumerate(Z_ORDER + (0,)):
                emit(mine(2, k), k, 1 if i % 2 == 0 else -1, 0)
            product(1)
            product(3)
            product(0)
            for i, k in enumerate(Z_ORDER + (0,)):
                step = 1 if i % 2 == 0 else -1
                part = mine(step, k)
                other = mine(-step, k)
                emit(other, 8 + k if step == -1 else 16 + k, -step, 0)
                part[...] = (part[...].astype(F32) + take(k)).astype(BF16)
                emit(part, 8 + k if step == 1 else 16 + k, step, 0)
            for i, k in enumerate(Z_ORDER + (0,)):
                total = mine(0, k)[...].astype(F32) + take(8 + k) + take(16 + k)
                if k:
                    sbuf[k, :, pl.ds(0, cw)] = total.astype(BF16)
                    emit(sbuf.at[k, :, pl.ds(0, cw)], 24 + k, 0, k)
            for k in Z_ARRIVAL[1:]:
                total = total + take(24 + k)
        else:
            for j in range(NY):
                product(j)
            order = (2, 1, 3, 0)
            plus, minus = (2, 1), (3, 0)
            for j in order:
                emit(mine(j, 4), j if j in plus else 16 + j, 0, 1 if j in plus else -1)
            for h in (3, 2, 1):
                s = 3 - h
                for j in order:
                    for sign, base in ((1, 0), (-1, 16)):
                        part = mine(j, sign * h)
                        if s or j in (plus if sign == 1 else minus):
                            part[...] = (part[...].astype(F32) + take(base + 4 * s + j)).astype(BF16)
                        emit(part, base + 4 * (s + 1) + j, 0, sign)
            for j in order:
                total = mine(j, 0)[...].astype(F32) + take(12 + j) + take(28 + j)
                if j:
                    sbuf[j, :, pl.ds(0, cw)] = total.astype(BF16)
                    emit(sbuf.at[j, :, pl.ds(0, cw)], 32 + j, j, 0)
            for j in (1, 3, 2):
                total = total + take(32 + j)

        xrow[:, pl.ds(0, cw)] = total
        for k in range(ROW):
            xs[k, :, pl.ds(0, cw)] = xrow[pl.ds(SH * k, SH), pl.ds(0, cw)]
        for k in (4, 3, 5, 2, 6, 1, 7):
            send(
                c, xs.at[lax.rem(r + k, ROW), :, pl.ds(0, cw)], xr.at[r, :, pl.ds(0, cw)],
                (xg_s, k), xg_r.at[k], row_dev(k), lambda: xs.at[0, :, pl.ds(0, cw)],
            )
        xr[r, :, pl.ds(0, cw)] = xs[r, :, pl.ds(0, cw)]

    @pl.when(core == 0)
    def _():
        reduce_weight(0)

    @pl.when(core == 1)
    def _():
        reduce_weight(1)

    text_forward()
    for s in range(S):
        pair[:, pl.ds(s * R, R)] = derivative(dot_nt(tlow[pl.ds(0, R), :], img[pl.ds(s * R, R), :]), s == 0)

    @pl.loop(0, R // 32)
    def _(i):
        rows = pl.ds(pl.multiple_of(i * 32, 32), 32)
        grad = dot(pair[rows, :], img[...])
        inv = tlen[rows, :]
        gtext[rows, :] = back(grad, traw[0, rows, :].astype(F32) * inv, inv).astype(BF16)

    cp_gt = pltpu.make_async_copy(gtext, gt_hbm, out_sem.at[1])
    cp_gt.start()

    for k in range(1, ROW):
        source = lax.rem(r + (ROW - k), ROW)

        @pl.when(lax.rem(source, 2) == 1)
        def _():
            arrived(xr.at[source, :, pl.ds(0, COLS[1][1])], xg_s.at[k], xg_r.at[k])

        @pl.when(lax.rem(source, 2) == 0)
        def _():
            arrived(xr.at[source, :, pl.ds(0, COLS[0][1])], xg_s.at[k], xg_r.at[k])

    for c in range(2):
        c0, cw = COLS[c]
        total = xr[c, :, pl.ds(0, cw)]
        for k in range(1, NX):
            total = total + xr[2 * k + c, :, pl.ds(0, cw)]
        gout[:, pl.ds(c0, cw)] = total
    cp_gw = pltpu.make_async_copy(gout, gw_hbm, out_sem.at[2])
    cp_gw.start()

    for only, wait in pending:
        if only is None:
            wait()
    for c in range(2):

        @pl.when(core == c)
        def _():
            for only, wait in pending:
                if only == c:
                    wait()

    cp_gf.wait()
    cp_gt.wait()
    cp_gw.wait()


def on_device(image_features, head_weight, text_embeds, natural_exponent_factor, logit_bias):
    dma = pltpu.SemaphoreType.DMA
    anywhere = pl.BlockSpec(memory_space=pl.ANY)
    scalar = pl.BlockSpec(memory_space=pltpu.SMEM)
    return pl.pallas_call(
        kernel,
        out_shape=(
            jax.ShapeDtypeStruct((R, D), BF16),
            jax.ShapeDtypeStruct((R, E), BF16),
            jax.ShapeDtypeStruct((SH, E), F32),
        ),
        in_specs=[anywhere, anywhere, anywhere, scalar, scalar],
        out_specs=(anywhere, anywhere, anywhere),
        scratch_shapes=[
            pltpu.VMEM((D, E), BF16),
            pltpu.VMEM((R, D), BF16),
            pltpu.VMEM((R, D), BF16),
            pltpu.VMEM((D, 2 * R), BF16),
            pltpu.VMEM((R, E), F32),
            pltpu.VMEM((R, 1), F32),
            pltpu.VMEM((S * R, E), BF16),
            pltpu.VMEM((S, R, E), BF16),
            pltpu.VMEM((S * R, E), BF16),
            pltpu.VMEM((R, 1), F32),
            pltpu.VMEM((R, S * R), BF16),
            pltpu.VMEM((2 * R, E), BF16),
            pltpu.VMEM((R, D), BF16),
            pltpu.VMEM((R, E), BF16),
            pltpu.VMEM((D, W1), BF16),
            pltpu.VMEM((ROW, SH, E), BF16),
            pltpu.VMEM((BLK, E), F32),
            pltpu.VMEM((36, BLK, W1), BF16),
            pltpu.VMEM((8, BLK, W1), BF16),
            pltpu.VMEM((BLK, W1), F32),
            pltpu.VMEM((ROW, SH, W1), F32),
            pltpu.VMEM((ROW, SH, W1), F32),
            pltpu.VMEM((SH, E), F32),
            dma((3,)), dma((3,)),
            dma((ROW,)), dma((ROW,)),
            dma((32,)), dma((32,)),
            dma((32,)), dma((32,)),
            dma((10,)), dma((10,)),
            dma((40,)), dma((36,)),
            dma((ROW,)), dma((ROW,)),
        ],
        compiler_params=pltpu.CompilerParams(
            collective_id=0, has_side_effects=True, vmem_limit_bytes=56 * 1024 * 1024
        ),
    )(image_features, head_weight, text_embeds, natural_exponent_factor, logit_bias)


def solution(mesh):
    split = P("blk", None)
    return jax.shard_map(
        on_device,
        mesh=mesh,
        in_specs=(split, split, split, P(), P()),
        out_specs=(split, split, split),
        check_vma=False,
    )
```

```python
import jax
import jax.numpy as jnp
from jax import lax
from jax.experimental import pallas as pl
from jax.experimental.pallas import tpu as pltpu
from jax.sharding import PartitionSpec as P

MESH = pl.DeviceIdType.MESH
D, E, R, S = 1536, 1152, 256, 4
NY, NZ, NX = 4, 8, 4
N = NY * NZ * NX * 2
ROW = NX * 2
SH = D // N
BLK = SH * ROW
YROWS = BLK * NZ
W1 = 640
COLS = ((0, W1), (W1, E - W1))
Y_CORE = 0
EPS = 1e-06
TILES = ((0, 512), (512, 512), (1024, 128))
F32, BF16 = jnp.float32, jnp.bfloat16
Z_ORDER = (4, 3, 5, 2, 6, 1, 7)
Z_ARRIVAL = (0, 1, 7, 2, 6, 3, 5, 4)
ORDER_NT = (((1,), (1,)), ((), ()))


def dot(a, b):
    return jnp.dot(a, b, preferred_element_type=F32)


def dot_nt(a, b):
    return lax.dot_general(a, b, ORDER_NT, preferred_element_type=F32)


def kernel(
    feat_hbm, w_hbm, text_hbm, nef_ref, bias_ref,
    gfeat, gtext, gout,
    w_ref, feat, feat2, feat_t, unit, length, img, traw, tlow, tlen, pair, eg,
    gpart, xbuf, wrow, rbuf, sbuf, xrow, xs, xr, igrad,
    in_sem, xw_s, xw_r, ag_s, ag_r, dd_s, dd_r, ex_s, ex_r, rs_s, rs_r, xg_s, xg_r,
):
    me = lax.axis_index("blk")
    core = lax.rem(me, 2)
    r = lax.rem(me, ROW)
    z = lax.rem(lax.div(me, ROW), NZ)
    y = lax.div(me, ROW * NZ)
    pending = []

    def dev(dy=0, dz=0):
        return (lax.rem(y + (dy + NY) , NY) * NZ + lax.rem(z + (dz + NZ), NZ)) * ROW + r

    def row_dev(k):
        return me - r + lax.rem(r + k, ROW)

    def near(k):
        return lax.rem(me + (k + N), N)

    def remote(src, dst, ss, rs, to):
        return pltpu.make_async_remote_copy(
            src_ref=src, dst_ref=dst, send_sem=ss, recv_sem=rs, device_id=(to,), device_id_type=MESH
        )

    def send(only, src, dst, ss, rs, to, like=None):
        sems, i = ss
        remote(src, dst, sems.at[i], rs, to).start()

        def wait():
            ref = src if like is None else like()
            remote(ref, ref, sems.at[i], sems.at[i], near(1)).wait_send()

        pending.append((only, wait))

    def arrived(dst, ss, rs):
        remote(dst, dst, ss, rs, near(1)).wait_recv()

    def wblock(ref, yy, zz, c0, cw):
        start = pl.multiple_of(lax.rem(yy, NY) * YROWS + lax.rem(zz, NZ) * BLK, 8)
        return ref.at[pl.ds(start, BLK), pl.ds(c0, cw)]

    def transpose(src, col):
        if col:
            arrived(feat2, ex_s.at[4], ex_r.at[0])

        @pl.loop(0, D // 256)
        def _(i):
            cols = pl.ds(pl.multiple_of(i * 256, 256), 256)
            feat_t[cols, pl.ds(col, R)] = jnp.transpose(src[:, cols])

    def tslot(k):
        return tlow.at[pl.ds(k * R, R), :]

    def slot(k):
        return img.at[pl.ds(k * R, R), :]

    cp_w = pltpu.make_async_copy(w_hbm, xbuf.at[r], in_sem.at[0])
    cp_t = pltpu.make_async_copy(text_hbm, traw, in_sem.at[1])
    cp_f = pltpu.make_async_copy(feat_hbm, feat, in_sem.at[2])
    cp_w.start()
    cp_t.start()
    cp_f.start()

    with jax.named_scope("barrier"):
        barrier = pltpu.get_barrier_semaphore()
        peers = [row_dev(k) for k in range(1, ROW)] + [dev(dz=k) for k in range(1, NZ)]
        peers += [dev(dy=k) for k in range(1, NY)] + [near(k) for k in (-2, -1, 1, 2)]
        for peer in peers:
            pl.semaphore_signal(barrier, inc=1, device_id=(peer,), device_id_type=MESH)
        pl.semaphore_wait(barrier, len(peers))

    with jax.named_scope("w_row_send"):
        cp_w.wait()
        for k in (4, 3, 5, 2, 6, 1, 7):
            send(None, xbuf.at[r], xbuf.at[r], (xw_s, k), xw_r.at[k], row_dev(k), lambda: xbuf.at[0])

    with jax.named_scope("own_text"):
        cp_t.wait()

        @pl.loop(0, R // 32)
        def _(i):
            rows = pl.ds(pl.multiple_of(i * 32, 32), 32)
            t = traw[rows, :].astype(F32)
            inv = 1.0 / jnp.sqrt(jnp.sum(t * t, axis=1, keepdims=True) + EPS)
            tlow[rows, :] = (t * inv).astype(BF16)
            tlen[rows, :] = inv

        cp_f.wait()
        send(None, feat, feat2, (ex_s, 4), ex_r.at[0], me + 1 - 2 * core)
        transpose(feat, 0)

    with jax.named_scope("w_row"):
        for k in range(1, ROW):
            arrived(xbuf.at[lax.rem(r + (ROW - k), ROW)], xw_s.at[k], xw_r.at[k])
        for k in range(ROW):
            wrow[pl.ds(SH * k, SH), :] = xbuf[k].astype(F32)
        own = pl.multiple_of(y * YROWS + z * BLK, 8)
        w_ref[pl.ds(own, BLK), :] = wrow[...].astype(BF16)

    with jax.named_scope("text_send"):
        @pl.when(core == 0)
        def _():
            send(0, tslot(0), tslot(1), (ex_s, 0), ex_r.at[1], near(-1), lambda: tslot(0))

        @pl.when(core == 1)
        def _():
            send(1, tslot(0), tslot(1), (ex_s, 0), ex_r.at[1], near(-1), lambda: tslot(0))
            send(1, tslot(0), tslot(2), (ex_s, 1), ex_r.at[2], near(-2), lambda: tslot(0))


    def gather(c):
        c0, cw = COLS[c]
        sibling = me + (1 - 2 * c)
        count = [0]
        like = lambda: w_ref.at[pl.ds(0, BLK), pl.ds(c0, cw)]

        def put(j, k, dy, dz):
            part = wblock(w_ref, y + (NY - j), z + (NZ - k), c0, cw)
            idx = ((j + dy) % NY) * NZ + (k + dz) % NZ
            send(c, part, part, (ag_s, count[0]), ag_r.at[idx], dev(dy, dz), like)
            count[0] += 1

        def share(j, k):
            part = wblock(w_ref, y + (NY - j), z + (NZ - k), c0, cw)
            send(c, part, part, (dd_s, j * NZ + k), dd_r.at[j * NZ + k], sibling, like)

        def got(j, k):
            part = wblock(w_ref, y + (NY - j), z + (NZ - k), c0, cw)
            arrived(part, ag_s.at[0], ag_r.at[j * NZ + k])
            return part

        if c == Y_CORE:
            for k in Z_ARRIVAL[1:]:
                put(0, 0, 0, k)
            transpose(feat2, R)

            def stage1(i):
                k = Z_ARRIVAL[i]
                if k:
                    got(0, k)
                put(0, k, 1, 0)
                put(0, k, -1, 0)
                if k:
                    share(0, k)

            def stage2(i):
                k = Z_ARRIVAL[i]
                got(1, k)
                if i % 2 == 0:
                    put(1, k, 1, 0)
                share(1, k)
                got(3, k)
                if i % 2 == 1:
                    put(3, k, -1, 0)
                share(3, k)

            def stage3(i):
                k = Z_ARRIVAL[i]
                got(2, k)
                share(2, k)

            for i in range(NZ + 4):
                if i < NZ:
                    stage1(i)
                if 2 <= i < NZ + 2:
                    stage2(i - 2)
                if 4 <= i:
                    stage3(i - 4)
        else:
            for j in (1, 3, 2):
                put(0, 0, j, 0)
            for j in (0, 1, 3, 2):
                if j:
                    got(j, 0)
                put(j, 0, 0, 1)
                put(j, 0, 0, -1)
                if j == 0:
                    transpose(feat2, R)
                if j:
                    share(j, 0)
            for h in (1, 2, 3):
                for j in (0, 1, 3, 2):
                    got(j, h)
                    if h < 3 or j in (0, 3):
                        put(j, h, 0, 1)
                    share(j, h)
                    got(j, NZ - h)
                    if h < 3 or j in (1, 2):
                        put(j, NZ - h, 0, -1)
                    share(j, NZ - h)
            for j in (0, 1, 3, 2):
                got(j, 4)
                share(j, 4)
            arrived(tslot(1), ex_s.at[0], ex_r.at[1])
            send(1, tslot(1), tslot(3), (ex_s, 2), ex_r.at[3], near(-2), lambda: tslot(0))
            send(1, tslot(1), tslot(2), (ex_s, 3), ex_r.at[2], near(-1), lambda: tslot(0))
            arrived(tslot(2), ex_s.at[0], ex_r.at[2])
            send(1, tslot(2), tslot(3), (ex_s, 10), ex_r.at[3], near(-1), lambda: tslot(0))
        o0, ow = COLS[1 - c]
        for j in range(NY):
            for k in range(NZ):
                if j or k:
                    part = wblock(w_ref, y + (NY - j), z + (NZ - k), o0, ow)
                    arrived(part, dd_s.at[0], dd_r.at[j * NZ + k])

    with jax.named_scope("gather"):
        @pl.when(core == 0)
        def _():
            gather(0)

        @pl.when(core == 1)
        def _():
            gather(1)

    with jax.named_scope("embed"):
        for c0, cw in TILES:
            unit[:, pl.ds(c0, cw)] = dot(feat[...], w_ref[:, pl.ds(c0, cw)])

        @pl.loop(0, R // 32)
        def _(i):
            rows = pl.ds(pl.multiple_of(i * 32, 32), 32)
            e = unit[rows, :]
            inv = 1.0 / jnp.sqrt(jnp.sum(e * e, axis=1, keepdims=True) + EPS)
            u = e * inv
            unit[rows, :] = u
            length[rows, :] = inv
            img[rows, :] = u.astype(BF16)

    with jax.named_scope("image_send"):
        @pl.when(core == 1)
        def _():
            send(1, slot(0), slot(1), (ex_s, 5), ex_r.at[5], near(1), lambda: slot(0))

        @pl.when(core == 0)
        def _():
            send(0, slot(0), slot(1), (ex_s, 5), ex_r.at[5], near(1), lambda: slot(0))
            send(0, slot(0), slot(2), (ex_s, 6), ex_r.at[6], near(2), lambda: slot(0))

    factor = jnp.exp(jnp.full((1, R), nef_ref[0], F32))
    bias = bias_ref[0]

    def derivative(logit_dot, diagonal):
        logits = factor * logit_dot + bias
        if diagonal:
            same = lax.broadcasted_iota(jnp.int32, (R, R), 0) == lax.broadcasted_iota(jnp.int32, (R, R), 1)
            label = jnp.where(same, 1.0, -1.0).astype(F32)
            g = -factor * label / (1.0 + jnp.exp(label * logits))
        else:
            g = factor / (1.0 + jnp.exp(-logits))
        return g.astype(BF16)

    def back(grad, u, inv):
        return (grad - u * jnp.sum(u * grad, axis=1, keepdims=True)) * inv

    with jax.named_scope("image_side"):
        for s in range(S):
            if s == 1:

                @pl.when(core == 0)
                def _():
                    arrived(tslot(1), ex_s.at[0], ex_r.at[1])
                    arrived(tslot(2), ex_s.at[0], ex_r.at[2])

            if s == 3:
                with jax.named_scope("text_wait"):
                    arrived(tslot(3), ex_s.at[0], ex_r.at[3])
            pair[:, pl.ds(s * R, R)] = derivative(dot_nt(img[pl.ds(0, R), :], tlow[pl.ds(s * R, R), :]), s == 0)
        for c0, cw in TILES:
            igrad[:, pl.ds(c0, cw)] = dot(pair[...], tlow[:, pl.ds(c0, cw)])

        @pl.loop(0, R // 32)
        def _(i):
            rows = pl.ds(pl.multiple_of(i * 32, 32), 32)
            eg[rows, :] = back(igrad[rows, :], unit[rows, :], length[rows, :]).astype(BF16)

    with jax.named_scope("eg_send"):
        @pl.when(core == 0)
        def _():
            part = pl.ds(COLS[1][0], COLS[1][1])
            send(0, eg.at[pl.ds(0, R), part], eg.at[pl.ds(R, R), part], (ex_s, 9), ex_r.at[9], me + 1, lambda: eg.at[pl.ds(0, R), pl.ds(COLS[1][0], COLS[1][1])])

        @pl.when(core == 1)
        def _():
            part = pl.ds(COLS[0][0], COLS[0][1])
            send(1, eg.at[pl.ds(0, R), part], eg.at[pl.ds(R, R), part], (ex_s, 9), ex_r.at[9], me - 1, lambda: eg.at[pl.ds(0, R), pl.ds(COLS[0][0], COLS[0][1])])

    with jax.named_scope("feat_grad"):
        @pl.loop(0, D // 512)
        def _(i):
            cols = pl.ds(pl.multiple_of(i * 512, 512), 512)
            gfeat[:, cols] = dot_nt(eg[pl.ds(0, R), :], w_ref[cols, :]).astype(BF16)


    def reduce_weight(c):
        c0, cw = COLS[c]
        count = [0]
        arrived(eg.at[pl.ds(R, R), pl.ds(c0, cw)], ex_s.at[0], ex_r.at[9])

        def product(j):
            rows = pl.ds(pl.multiple_of(lax.rem(y + j, NY) * YROWS, 8), YROWS)
            gpart[rows, pl.ds(0, cw)] = dot(feat_t[rows, :], eg[:, pl.ds(c0, cw)]).astype(BF16)

        def mine(dy, dz):
            return wblock(gpart, y + (dy + NY), z + (dz + NZ), 0, cw)

        def buf(i):
            return rbuf.at[i, :, pl.ds(0, cw)]

        def emit(src, i, dy, dz):
            send(c, src, buf(i), (rs_s, count[0]), rs_r.at[i], dev(dy, dz), lambda: buf(0))
            count[0] += 1

        def take(i):
            arrived(buf(i), rs_s.at[0], rs_r.at[i])
            return buf(i)[...].astype(F32)

        if c == Y_CORE:
            product(2)
            for i, k in enumerate(Z_ORDER + (0,)):
                emit(mine(2, k), k, 1 if i % 2 == 0 else -1, 0)
            product(1)
            product(3)
            product(0)
            for i, k in enumerate(Z_ORDER + (0,)):
                step = 1 if i % 2 == 0 else -1
                part = mine(step, k)
                other = mine(-step, k)
                emit(other, 8 + k if step == -1 else 16 + k, -step, 0)
                part[...] = (part[...].astype(F32) + take(k)).astype(BF16)
                emit(part, 8 + k if step == 1 else 16 + k, step, 0)
            for i, k in enumerate(Z_ORDER + (0,)):
                total = mine(0, k)[...].astype(F32) + take(8 + k) + take(16 + k)
                if k:
                    sbuf[k, :, pl.ds(0, cw)] = total.astype(BF16)
                    emit(sbuf.at[k, :, pl.ds(0, cw)], 24 + k, 0, k)
            arrived(slot(1), ex_s.at[0], ex_r.at[5])
            send(0, slot(1), slot(3), (ex_s, 7), ex_r.at[7], near(2), lambda: slot(0))
            send(0, slot(1), slot(2), (ex_s, 8), ex_r.at[6], near(1), lambda: slot(0))
            arrived(slot(2), ex_s.at[0], ex_r.at[6])
            send(0, slot(2), slot(3), (ex_s, 11), ex_r.at[7], near(1), lambda: slot(0))
            for k in Z_ARRIVAL[1:]:
                total = total + take(24 + k)
        else:
            for j in range(NY):
                product(j)
            order = (2, 1, 3, 0)
            plus, minus = (2, 1), (3, 0)
            for j in order:
                emit(mine(j, 4), j if j in plus else 16 + j, 0, 1 if j in plus else -1)
            for h in (3, 2, 1):
                s = 3 - h
                for j in order:
                    for sign, base in ((1, 0), (-1, 16)):
                        part = mine(j, sign * h)
                        if s or j in (plus if sign == 1 else minus):
                            part[...] = (part[...].astype(F32) + take(base + 4 * s + j)).astype(BF16)
                        emit(part, base + 4 * (s + 1) + j, 0, sign)
            for j in order:
                total = mine(j, 0)[...].astype(F32) + take(12 + j) + take(28 + j)
                if j:
                    sbuf[j, :, pl.ds(0, cw)] = total.astype(BF16)
                    emit(sbuf.at[j, :, pl.ds(0, cw)], 32 + j, j, 0)
            for j in (1, 3, 2):
                total = total + take(32 + j)

        xrow[:, pl.ds(0, cw)] = total
        for k in range(ROW):
            xs[k, :, pl.ds(0, cw)] = xrow[pl.ds(SH * k, SH), pl.ds(0, cw)]
        for k in (4, 3, 5, 2, 6, 1, 7):
            send(
                c, xs.at[lax.rem(r + k, ROW), :, pl.ds(0, cw)], xr.at[r, :, pl.ds(0, cw)],
                (xg_s, k), xg_r.at[k], row_dev(k), lambda: xs.at[0, :, pl.ds(0, cw)],
            )
        xr[r, :, pl.ds(0, cw)] = xs[r, :, pl.ds(0, cw)]

    with jax.named_scope("reduce"):
        @pl.when(core == 0)
        def _():
            reduce_weight(0)

        @pl.when(core == 1)
        def _():
            reduce_weight(1)

    with jax.named_scope("image_wait"):
        @pl.when(core == 1)
        def _():
            arrived(slot(1), ex_s.at[0], ex_r.at[5])
            arrived(slot(2), ex_s.at[0], ex_r.at[6])

        arrived(slot(3), ex_s.at[0], ex_r.at[7])
    with jax.named_scope("text_side"):
        for s in range(S):
            pair[:, pl.ds(s * R, R)] = derivative(dot_nt(tlow[pl.ds(0, R), :], img[pl.ds(s * R, R), :]), s == 0)
        for c0, cw in TILES:
            igrad[:, pl.ds(c0, cw)] = dot(pair[...], img[:, pl.ds(c0, cw)])

        @pl.loop(0, R // 32)
        def _(i):
            rows = pl.ds(pl.multiple_of(i * 32, 32), 32)
            inv = tlen[rows, :]
            gtext[rows, :] = back(igrad[rows, :], traw[rows, :].astype(F32) * inv, inv).astype(BF16)

    with jax.named_scope("final"):
        for k in range(1, ROW):
            source = lax.rem(r + (ROW - k), ROW)

            @pl.when(lax.rem(source, 2) == 1)
            def _():
                arrived(xr.at[source, :, pl.ds(0, COLS[1][1])], xg_s.at[k], xg_r.at[k])

            @pl.when(lax.rem(source, 2) == 0)
            def _():
                arrived(xr.at[source, :, pl.ds(0, COLS[0][1])], xg_s.at[k], xg_r.at[k])

        for c in range(2):
            c0, cw = COLS[c]
            total = xr[c, :, pl.ds(0, cw)]
            for k in range(1, NX):
                total = total + xr[2 * k + c, :, pl.ds(0, cw)]
            gout[:, pl.ds(c0, cw)] = total

    with jax.named_scope("drain"):
        for only, wait in pending:
            if only is None:
                wait()
        for c in range(2):

            @pl.when(core == c)
            def _():
                for only, wait in pending:
                    if only == c:
                        wait()


def on_device(image_features, head_weight, text_embeds, natural_exponent_factor, logit_bias):
    dma = pltpu.SemaphoreType.DMA
    anywhere = pl.BlockSpec(memory_space=pl.ANY)
    local = pl.BlockSpec(memory_space=pltpu.VMEM)
    scalar = pl.BlockSpec(memory_space=pltpu.SMEM)
    return pl.pallas_call(
        kernel,
        out_shape=(
            jax.ShapeDtypeStruct((R, D), BF16),
            jax.ShapeDtypeStruct((R, E), BF16),
            jax.ShapeDtypeStruct((SH, E), F32),
        ),
        in_specs=[anywhere, anywhere, anywhere, scalar, scalar],
        out_specs=(local, local, local),
        scratch_shapes=[
            pltpu.VMEM((D, E), BF16),
            pltpu.VMEM((R, D), BF16),
            pltpu.VMEM((R, D), BF16),
            pltpu.VMEM((D, 2 * R), BF16),
            pltpu.VMEM((R, E), F32),
            pltpu.VMEM((R, 1), F32),
            pltpu.VMEM((S * R, E), BF16),
            pltpu.VMEM((R, E), BF16),
            pltpu.VMEM((S * R, E), BF16),
            pltpu.VMEM((R, 1), F32),
            pltpu.VMEM((R, S * R), BF16),
            pltpu.VMEM((2 * R, E), BF16),
            pltpu.VMEM((D, W1), BF16),
            pltpu.VMEM((ROW, SH, E), BF16),
            pltpu.VMEM((BLK, E), F32),
            pltpu.VMEM((36, BLK, W1), BF16),
            pltpu.VMEM((8, BLK, W1), BF16),
            pltpu.VMEM((BLK, W1), F32),
            pltpu.VMEM((ROW, SH, W1), F32),
            pltpu.VMEM((ROW, SH, W1), F32),
            pltpu.VMEM((R, E), F32),
            dma((3,)),
            dma((ROW,)), dma((ROW,)),
            dma((32,)), dma((32,)),
            dma((32,)), dma((32,)),
            dma((12,)), dma((10,)),
            dma((40,)), dma((36,)),
            dma((ROW,)), dma((ROW,)),
        ],
        compiler_params=pltpu.CompilerParams(
            collective_id=0, has_side_effects=True, vmem_limit_bytes=32 * 1024 * 1024
        ),
    )(image_features, head_weight, text_embeds, natural_exponent_factor, logit_bias)


def solution(mesh):
    split = P("blk", None)
    return jax.shard_map(
        on_device,
        mesh=mesh,
        in_specs=(split, split, split, P(), P()),
        out_specs=(split, split, split),
        check_vma=False,
    )
```

```python
import jax
import jax.numpy as jnp
from jax import lax
from jax.experimental import pallas as pl
from jax.experimental.pallas import tpu as pltpu
from jax.sharding import PartitionSpec as P

MESH = pl.DeviceIdType.MESH
D, E, R, S = 1536, 1152, 256, 4
NY, NZ, NX = 4, 8, 4
N = NY * NZ * NX * 2
ROW = NX * 2
SH = D // N
BLK = SH * ROW
YROWS = BLK * NZ
W1 = 640
COLS = ((0, W1), (W1, E - W1))
Y_CORE = 0
EPS = 1e-06
TILES = ((0, 512), (512, 512), (1024, 128))
F32, BF16 = jnp.float32, jnp.bfloat16
Z_ORDER = (4, 3, 5, 2, 6, 1, 7)
Z_ARRIVAL = (0, 1, 7, 2, 6, 3, 5, 4)
ORDER_NT = (((1,), (1,)), ((), ()))


def dot(a, b):
    return jnp.dot(a, b, preferred_element_type=F32)


def dot_nt(a, b):
    return lax.dot_general(a, b, ORDER_NT, preferred_element_type=F32)


def kernel(
    feat_hbm, w_hbm, text_hbm, nef_ref, bias_ref,
    gfeat, gtext, gout,
    w_ref, feat, feat2, feat_t, unit, length, img, traw, tlow, tlen, pair, eg,
    gpart, xbuf, wrow, rbuf, sbuf, xrow, xs, xr, igrad, cross,
    in_sem, xw_s, xw_r, ag_s, ag_r, dd_s, dd_r, ex_s, ex_r, rs_s, rs_r, xg_s, xg_r,
):
    me = lax.axis_index("blk")
    core = lax.rem(me, 2)
    r = lax.rem(me, ROW)
    z = lax.rem(lax.div(me, ROW), NZ)
    y = lax.div(me, ROW * NZ)
    pending = []

    def dev(dy=0, dz=0):
        return (lax.rem(y + (dy + NY) , NY) * NZ + lax.rem(z + (dz + NZ), NZ)) * ROW + r

    def row_dev(k):
        return me - r + lax.rem(r + k, ROW)

    def near(k):
        return lax.rem(me + (k + N), N)

    def remote(src, dst, ss, rs, to):
        return pltpu.make_async_remote_copy(
            src_ref=src, dst_ref=dst, send_sem=ss, recv_sem=rs, device_id=(to,), device_id_type=MESH
        )

    def send(only, src, dst, ss, rs, to, like=None):
        sems, i = ss
        remote(src, dst, sems.at[i], rs, to).start()

        def wait():
            ref = src if like is None else like()
            remote(ref, ref, sems.at[i], sems.at[i], near(1)).wait_send()

        pending.append((only, wait))

    def arrived(dst, ss, rs):
        remote(dst, dst, ss, rs, near(1)).wait_recv()

    def wblock(ref, yy, zz, c0, cw):
        start = pl.multiple_of(lax.rem(yy, NY) * YROWS + lax.rem(zz, NZ) * BLK, 8)
        return ref.at[pl.ds(start, BLK), pl.ds(c0, cw)]

    def transpose(src, col):
        if col:
            arrived(feat2, ex_s.at[12], ex_r.at[0])

        @pl.loop(0, D // 256)
        def _(i):
            cols = pl.ds(pl.multiple_of(i * 256, 256), 256)
            feat_t[cols, pl.ds(col, R)] = jnp.transpose(src[:, cols])

    def tslot(k):
        return tlow.at[pl.ds(k * R, R), :]

    def slot(k):
        return img.at[pl.ds(k * R, R), :]

    cp_w = pltpu.make_async_copy(w_hbm, xbuf.at[r], in_sem.at[0])
    cp_t = pltpu.make_async_copy(text_hbm, traw, in_sem.at[1])
    cp_f = pltpu.make_async_copy(feat_hbm, feat, in_sem.at[2])
    cp_w.start()
    cp_t.start()
    cp_f.start()

    with jax.named_scope("barrier"):
        barrier = pltpu.get_barrier_semaphore()
        peers = [row_dev(k) for k in range(1, ROW)] + [dev(dz=k) for k in range(1, NZ)]
        peers += [dev(dy=k) for k in range(1, NY)] + [near(k) for k in (-ROW, -3, -2, -1, 1, 2, 3, ROW)]
        for peer in peers:
            pl.semaphore_signal(barrier, inc=1, device_id=(peer,), device_id_type=MESH)
        pl.semaphore_wait(barrier, len(peers))

    with jax.named_scope("w_row_send"):
        cp_w.wait()
        for k in (4, 3, 5, 2, 6, 1, 7):
            send(None, xbuf.at[r], xbuf.at[r], (xw_s, k), xw_r.at[k], row_dev(k), lambda: xbuf.at[0])

    with jax.named_scope("own_text"):
        cp_t.wait()

        @pl.loop(0, R // 32)
        def _(i):
            rows = pl.ds(pl.multiple_of(i * 32, 32), 32)
            t = traw[rows, :].astype(F32)
            inv = 1.0 / jnp.sqrt(jnp.sum(t * t, axis=1, keepdims=True) + EPS)
            tlow[rows, :] = (t * inv).astype(BF16)
            tlen[rows, :] = inv

        cp_f.wait()
        send(None, feat, feat2, (ex_s, 12), ex_r.at[0], me + 1 - 2 * core)
        transpose(feat, 0)

    with jax.named_scope("text_send"):
        @pl.when(core == 0)
        def _():
            send(0, tslot(0), tslot(1), (ex_s, 0), ex_r.at[1], near(-1), lambda: tslot(0))

        @pl.when((core == 0) & (r != 0))
        def _():
            send("t3", tslot(0), tslot(3), (ex_s, 1), ex_r.at[3], near(-3), lambda: tslot(0))

        @pl.when(core == 1)
        def _():
            send(1, tslot(0), tslot(1), (ex_s, 0), ex_r.at[1], near(-1), lambda: tslot(0))

        @pl.when((core == 1) & (r != 1))
        def _():
            send("t2", tslot(0), tslot(2), (ex_s, 1), ex_r.at[2], near(-2), lambda: tslot(0))

        @pl.when(r == 1)
        def _():
            send("t1", tslot(0), cross, (ex_s, 1), ex_r.at[8], near(6), lambda: tslot(0))

    with jax.named_scope("w_row"):
        for k in range(1, ROW):
            arrived(xbuf.at[lax.rem(r + (ROW - k), ROW)], xw_s.at[k], xw_r.at[k])
        for k in range(ROW):
            wrow[pl.ds(SH * k, SH), :] = xbuf[k].astype(F32)
        own = pl.multiple_of(y * YROWS + z * BLK, 8)
        w_ref[pl.ds(own, BLK), :] = wrow[...].astype(BF16)

    def gather(c):
        c0, cw = COLS[c]
        sibling = me + (1 - 2 * c)
        count = [0]
        like = lambda: w_ref.at[pl.ds(0, BLK), pl.ds(c0, cw)]

        def put(j, k, dy, dz):
            part = wblock(w_ref, y + (NY - j), z + (NZ - k), c0, cw)
            idx = ((j + dy) % NY) * NZ + (k + dz) % NZ
            send(c, part, part, (ag_s, count[0]), ag_r.at[idx], dev(dy, dz), like)
            count[0] += 1

        def share(j, k):
            part = wblock(w_ref, y + (NY - j), z + (NZ - k), c0, cw)
            send(c, part, part, (dd_s, j * NZ + k), dd_r.at[j * NZ + k], sibling, like)

        def got(j, k):
            part = wblock(w_ref, y + (NY - j), z + (NZ - k), c0, cw)
            arrived(part, ag_s.at[0], ag_r.at[j * NZ + k])
            return part

        if c == Y_CORE:
            for k in Z_ARRIVAL[1:]:
                put(0, 0, 0, k)
            transpose(feat2, R)

            def stage1(i):
                k = Z_ARRIVAL[i]
                if k:
                    got(0, k)
                put(0, k, 1, 0)
                put(0, k, -1, 0)
                if k:
                    share(0, k)

            def stage2(i):
                k = Z_ARRIVAL[i]
                got(1, k)
                if i % 2 == 0:
                    put(1, k, 1, 0)
                share(1, k)
                got(3, k)
                if i % 2 == 1:
                    put(3, k, -1, 0)
                share(3, k)

            def stage3(i):
                k = Z_ARRIVAL[i]
                got(2, k)
                share(2, k)

            for i in range(NZ + 4):
                if i < NZ:
                    stage1(i)
                if 2 <= i < NZ + 2:
                    stage2(i - 2)
                if 4 <= i:
                    stage3(i - 4)
        else:
            for j in (1, 3, 2):
                put(0, 0, j, 0)
            for j in (0, 1, 3, 2):
                if j:
                    got(j, 0)
                put(j, 0, 0, 1)
                put(j, 0, 0, -1)
                if j == 0:
                    transpose(feat2, R)
                if j:
                    share(j, 0)
            for h in (1, 2, 3):
                for j in (0, 1, 3, 2):
                    got(j, h)
                    if h < 3 or j in (0, 3):
                        put(j, h, 0, 1)
                    share(j, h)
                    got(j, NZ - h)
                    if h < 3 or j in (1, 2):
                        put(j, NZ - h, 0, -1)
                    share(j, NZ - h)
                if h == 2:

                    @pl.when(r == ROW - 1)
                    def _():
                        arrived(cross, ex_s.at[0], ex_r.at[8])
                        send("t7", cross, tslot(2), (ex_s, 2), ex_r.at[2], near(-ROW), lambda: tslot(0))

                if h == 3:
                    arrived(tslot(1), ex_s.at[0], ex_r.at[1])
                    send(1, tslot(1), tslot(2), (ex_s, 3), ex_r.at[2], near(-1), lambda: tslot(0))

                    @pl.when(r == ROW - 1)
                    def _():
                        send("t7", tslot(1), tslot(3), (ex_s, 4), ex_r.at[3], near(-2), lambda: tslot(0))

            for j in (0, 1, 3, 2):
                got(j, 4)
                share(j, 4)
            arrived(tslot(2), ex_s.at[0], ex_r.at[2])
            send(1, tslot(2), tslot(3), (ex_s, 10), ex_r.at[3], near(-1), lambda: tslot(0))
        o0, ow = COLS[1 - c]
        for j in range(NY):
            for k in range(NZ):
                if j or k:
                    part = wblock(w_ref, y + (NY - j), z + (NZ - k), o0, ow)
                    arrived(part, dd_s.at[0], dd_r.at[j * NZ + k])

    with jax.named_scope("gather"):
        @pl.when(core == 0)
        def _():
            gather(0)

        @pl.when(core == 1)
        def _():
            gather(1)

    with jax.named_scope("embed"):
        for c0, cw in TILES:
            unit[:, pl.ds(c0, cw)] = dot(feat[...], w_ref[:, pl.ds(c0, cw)])

        @pl.loop(0, R // 32)
        def _(i):
            rows = pl.ds(pl.multiple_of(i * 32, 32), 32)
            e = unit[rows, :]
            inv = 1.0 / jnp.sqrt(jnp.sum(e * e, axis=1, keepdims=True) + EPS)
            u = e * inv
            unit[rows, :] = u
            length[rows, :] = inv
            img[rows, :] = u.astype(BF16)

    with jax.named_scope("image_send"):
        @pl.when(core == 1)
        def _():
            send(1, slot(0), slot(1), (ex_s, 5), ex_r.at[5], near(1), lambda: slot(0))

        @pl.when((core == 1) & (r != ROW - 1))
        def _():
            send("i3", slot(0), slot(3), (ex_s, 6), ex_r.at[7], near(3), lambda: slot(0))

        @pl.when(core == 0)
        def _():
            send(0, slot(0), slot(1), (ex_s, 5), ex_r.at[5], near(1), lambda: slot(0))

        @pl.when((core == 0) & (r != ROW - 2))
        def _():
            send("i2", slot(0), slot(2), (ex_s, 6), ex_r.at[6], near(2), lambda: slot(0))

        @pl.when(r == ROW - 2)
        def _():
            send("i6", slot(0), cross, (ex_s, 6), ex_r.at[9], near(-6), lambda: slot(0))

    factor = jnp.exp(jnp.full((1, R), nef_ref[0], F32))
    bias = bias_ref[0]

    def derivative(logit_dot, diagonal):
        logits = factor * logit_dot + bias
        if diagonal:
            same = lax.broadcasted_iota(jnp.int32, (R, R), 0) == lax.broadcasted_iota(jnp.int32, (R, R), 1)
            label = jnp.where(same, 1.0, -1.0).astype(F32)
            g = -factor * label / (1.0 + jnp.exp(label * logits))
        else:
            g = factor / (1.0 + jnp.exp(-logits))
        return g.astype(BF16)

    def back(grad, u, inv):
        return (grad - u * jnp.sum(u * grad, axis=1, keepdims=True)) * inv

    with jax.named_scope("image_side"):
        for s in range(S):
            if s == 1:

                @pl.when(core == 0)
                def _():
                    arrived(tslot(1), ex_s.at[0], ex_r.at[1])
                    arrived(tslot(2), ex_s.at[0], ex_r.at[2])

            if s == 3:
                with jax.named_scope("text_wait"):
                    arrived(tslot(3), ex_s.at[0], ex_r.at[3])
            pair[:, pl.ds(s * R, R)] = derivative(dot_nt(img[pl.ds(0, R), :], tlow[pl.ds(s * R, R), :]), s == 0)
        for c0, cw in TILES:
            igrad[:, pl.ds(c0, cw)] = dot(pair[...], tlow[:, pl.ds(c0, cw)])

        @pl.loop(0, R // 32)
        def _(i):
            rows = pl.ds(pl.multiple_of(i * 32, 32), 32)
            eg[rows, :] = back(igrad[rows, :], unit[rows, :], length[rows, :]).astype(BF16)

    with jax.named_scope("eg_send"):
        @pl.when(core == 0)
        def _():
            part = pl.ds(COLS[1][0], COLS[1][1])
            send(0, eg.at[pl.ds(0, R), part], eg.at[pl.ds(R, R), part], (ex_s, 9), ex_r.at[10], me + 1, lambda: eg.at[pl.ds(0, R), pl.ds(COLS[1][0], COLS[1][1])])

        @pl.when(core == 1)
        def _():
            part = pl.ds(COLS[0][0], COLS[0][1])
            send(1, eg.at[pl.ds(0, R), part], eg.at[pl.ds(R, R), part], (ex_s, 9), ex_r.at[10], me - 1, lambda: eg.at[pl.ds(0, R), pl.ds(COLS[0][0], COLS[0][1])])

    with jax.named_scope("feat_grad"):
        @pl.loop(0, D // 512)
        def _(i):
            cols = pl.ds(pl.multiple_of(i * 512, 512), 512)
            gfeat[:, cols] = dot_nt(eg[pl.ds(0, R), :], w_ref[cols, :]).astype(BF16)


    def reduce_weight(c):
        c0, cw = COLS[c]
        count = [0]
        arrived(eg.at[pl.ds(R, R), pl.ds(c0, cw)], ex_s.at[0], ex_r.at[10])

        def product(j):
            rows = pl.ds(pl.multiple_of(lax.rem(y + j, NY) * YROWS, 8), YROWS)
            gpart[rows, pl.ds(0, cw)] = dot(feat_t[rows, :], eg[:, pl.ds(c0, cw)]).astype(BF16)

        def mine(dy, dz):
            return wblock(gpart, y + (dy + NY), z + (dz + NZ), 0, cw)

        def buf(i):
            return rbuf.at[i, :, pl.ds(0, cw)]

        def emit(src, i, dy, dz):
            send(c, src, buf(i), (rs_s, count[0]), rs_r.at[i], dev(dy, dz), lambda: buf(0))
            count[0] += 1

        def take(i):
            arrived(buf(i), rs_s.at[0], rs_r.at[i])
            return buf(i)[...].astype(F32)

        if c == Y_CORE:
            product(2)
            for i, k in enumerate(Z_ORDER + (0,)):
                emit(mine(2, k), k, 1 if i % 2 == 0 else -1, 0)
            product(1)
            product(3)
            product(0)
            for i, k in enumerate(Z_ORDER + (0,)):
                step = 1 if i % 2 == 0 else -1
                part = mine(step, k)
                other = mine(-step, k)
                emit(other, 8 + k if step == -1 else 16 + k, -step, 0)
                part[...] = (part[...].astype(F32) + take(k)).astype(BF16)
                emit(part, 8 + k if step == 1 else 16 + k, step, 0)
            arrived(slot(1), ex_s.at[0], ex_r.at[5])
            send(0, slot(1), slot(2), (ex_s, 8), ex_r.at[6], near(1), lambda: slot(0))

            @pl.when(r == 0)
            def _():
                send("i0", slot(1), slot(3), (ex_s, 7), ex_r.at[7], near(2), lambda: slot(0))
                arrived(cross, ex_s.at[0], ex_r.at[9])
                send("i0", cross, slot(2), (ex_s, 13), ex_r.at[6], near(ROW), lambda: slot(0))

            for i, k in enumerate(Z_ORDER + (0,)):
                total = mine(0, k)[...].astype(F32) + take(8 + k) + take(16 + k)
                if k:
                    sbuf[k, :, pl.ds(0, cw)] = total.astype(BF16)
                    emit(sbuf.at[k, :, pl.ds(0, cw)], 24 + k, 0, k)
            arrived(slot(2), ex_s.at[0], ex_r.at[6])
            send(0, slot(2), slot(3), (ex_s, 11), ex_r.at[7], near(1), lambda: slot(0))
            for k in Z_ARRIVAL[1:]:
                total = total + take(24 + k)
        else:
            for j in range(NY):
                product(j)
            order = (2, 1, 3, 0)
            plus, minus = (2, 1), (3, 0)
            for j in order:
                emit(mine(j, 4), j if j in plus else 16 + j, 0, 1 if j in plus else -1)
            for h in (3, 2, 1):
                s = 3 - h
                for j in order:
                    for sign, base in ((1, 0), (-1, 16)):
                        part = mine(j, sign * h)
                        if s or j in (plus if sign == 1 else minus):
                            part[...] = (part[...].astype(F32) + take(base + 4 * s + j)).astype(BF16)
                        emit(part, base + 4 * (s + 1) + j, 0, sign)
            for j in order:
                total = mine(j, 0)[...].astype(F32) + take(12 + j) + take(28 + j)
                if j:
                    sbuf[j, :, pl.ds(0, cw)] = total.astype(BF16)
                    emit(sbuf.at[j, :, pl.ds(0, cw)], 32 + j, j, 0)
            for j in (1, 3, 2):
                total = total + take(32 + j)

        xrow[:, pl.ds(0, cw)] = total
        for k in range(ROW):
            xs[k, :, pl.ds(0, cw)] = xrow[pl.ds(SH * k, SH), pl.ds(0, cw)]
        for k in (4, 3, 5, 2, 6, 1, 7):
            send(
                c, xs.at[lax.rem(r + k, ROW), :, pl.ds(0, cw)], xr.at[r, :, pl.ds(0, cw)],
                (xg_s, k), xg_r.at[k], row_dev(k), lambda: xs.at[0, :, pl.ds(0, cw)],
            )
        xr[r, :, pl.ds(0, cw)] = xs[r, :, pl.ds(0, cw)]

    with jax.named_scope("reduce"):
        @pl.when(core == 0)
        def _():
            reduce_weight(0)

        @pl.when(core == 1)
        def _():
            reduce_weight(1)

    with jax.named_scope("image_wait"):
        @pl.when(core == 1)
        def _():
            arrived(slot(1), ex_s.at[0], ex_r.at[5])
            arrived(slot(2), ex_s.at[0], ex_r.at[6])

        arrived(slot(3), ex_s.at[0], ex_r.at[7])
    with jax.named_scope("text_side"):
        for s in range(S):
            pair[:, pl.ds(s * R, R)] = derivative(dot_nt(tlow[pl.ds(0, R), :], img[pl.ds(s * R, R), :]), s == 0)
        for c0, cw in TILES:
            igrad[:, pl.ds(c0, cw)] = dot(pair[...], img[:, pl.ds(c0, cw)])

        @pl.loop(0, R // 32)
        def _(i):
            rows = pl.ds(pl.multiple_of(i * 32, 32), 32)
            inv = tlen[rows, :]
            gtext[rows, :] = back(igrad[rows, :], traw[rows, :].astype(F32) * inv, inv).astype(BF16)

    with jax.named_scope("final"):
        for k in range(1, ROW):
            source = lax.rem(r + (ROW - k), ROW)

            @pl.when(lax.rem(source, 2) == 1)
            def _():
                arrived(xr.at[source, :, pl.ds(0, COLS[1][1])], xg_s.at[k], xg_r.at[k])

            @pl.when(lax.rem(source, 2) == 0)
            def _():
                arrived(xr.at[source, :, pl.ds(0, COLS[0][1])], xg_s.at[k], xg_r.at[k])

        for c in range(2):
            c0, cw = COLS[c]
            total = xr[c, :, pl.ds(0, cw)]
            for k in range(1, NX):
                total = total + xr[2 * k + c, :, pl.ds(0, cw)]
            gout[:, pl.ds(c0, cw)] = total

    with jax.named_scope("drain"):
        for only, wait in pending:
            if only is None:
                wait()
        groups = {
            0: core == 0, 1: core == 1, "t1": r == 1, "t7": r == ROW - 1, "i6": r == ROW - 2, "i0": r == 0,
            "t3": (core == 0) & (r != 0), "t2": (core == 1) & (r != 1),
            "i3": (core == 1) & (r != ROW - 1), "i2": (core == 0) & (r != ROW - 2),
        }
        for group, inside in groups.items():

            @pl.when(inside)
            def _():
                for only, wait in pending:
                    if only == group:
                        wait()


def put_out(gf, gt, gw, gf_out, gt_out, gw_out, sem):
    copies = [pltpu.make_async_copy(a, b, sem.at[i]) for i, (a, b) in enumerate(((gf, gf_out), (gt, gt_out), (gw, gw_out)))]
    for copy in copies:
        copy.start()
    for copy in copies:
        copy.wait()


def on_device(image_features, head_weight, text_embeds, natural_exponent_factor, logit_bias):
    dma = pltpu.SemaphoreType.DMA
    hbm = pl.BlockSpec(memory_space=pltpu.HBM)
    local = pl.BlockSpec(memory_space=pltpu.VMEM)
    scalar = pl.BlockSpec(memory_space=pltpu.SMEM)
    results = pl.pallas_call(
        kernel,
        out_shape=(
            jax.ShapeDtypeStruct((R, D), BF16),
            jax.ShapeDtypeStruct((R, E), BF16),
            jax.ShapeDtypeStruct((SH, E), F32),
        ),
        in_specs=[hbm, hbm, hbm, scalar, scalar],
        out_specs=(local, local, local),
        scratch_shapes=[
            pltpu.VMEM((D, E), BF16),
            pltpu.VMEM((R, D), BF16),
            pltpu.VMEM((R, D), BF16),
            pltpu.VMEM((D, 2 * R), BF16),
            pltpu.VMEM((R, E), F32),
            pltpu.VMEM((R, 1), F32),
            pltpu.VMEM((S * R, E), BF16),
            pltpu.VMEM((R, E), BF16),
            pltpu.VMEM((S * R, E), BF16),
            pltpu.VMEM((R, 1), F32),
            pltpu.VMEM((R, S * R), BF16),
            pltpu.VMEM((2 * R, E), BF16),
            pltpu.VMEM((D, W1), BF16),
            pltpu.VMEM((ROW, SH, E), BF16),
            pltpu.VMEM((BLK, E), F32),
            pltpu.VMEM((36, BLK, W1), BF16),
            pltpu.VMEM((8, BLK, W1), BF16),
            pltpu.VMEM((BLK, W1), F32),
            pltpu.VMEM((ROW, SH, W1), F32),
            pltpu.VMEM((ROW, SH, W1), F32),
            pltpu.VMEM((R, E), F32),
            pltpu.VMEM((R, E), BF16),
            dma((3,)),
            dma((ROW,)), dma((ROW,)),
            dma((32,)), dma((32,)),
            dma((32,)), dma((32,)),
            dma((14,)), dma((11,)),
            dma((40,)), dma((36,)),
            dma((ROW,)), dma((ROW,)),
        ],
        compiler_params=pltpu.CompilerParams(
            collective_id=0, has_side_effects=True, vmem_limit_bytes=32 * 1024 * 1024
        ),
    )(image_features, head_weight, text_embeds, natural_exponent_factor, logit_bias)
    return pl.pallas_call(
        put_out,
        out_shape=tuple(jax.ShapeDtypeStruct(a.shape, a.dtype) for a in results),
        in_specs=[local] * 3,
        out_specs=[hbm] * 3,
        scratch_shapes=[dma((3,))],
        compiler_params=pltpu.CompilerParams(vmem_limit_bytes=8 * 1024 * 1024),
    )(*results)


def solution(mesh):
    split = P("blk", None)
    return jax.shard_map(
        on_device,
        mesh=mesh,
        in_specs=(split, split, split, P(), P()),
        out_specs=(split, split, split),
        check_vma=False,
    )
```

```python
import jax
import jax.numpy as jnp
from jax import lax
from jax.experimental import pallas as pl
from jax.experimental.pallas import tpu as pltpu
from jax.sharding import PartitionSpec as P

MESH = pl.DeviceIdType.MESH
D, E, R, S = 1536, 1152, 256, 4
NY, NZ, NX = 4, 8, 4
N = NY * NZ * NX * 2
ROW = NX * 2
SH = D // N
BLK = SH * ROW
YROWS = BLK * NZ
W1 = 640
COLS = ((0, W1), (W1, E - W1))
Y_CORE = 0
EPS = 1e-06
TILES = ((0, 512), (512, 512), (1024, 128))
F32, BF16 = jnp.float32, jnp.bfloat16
Z_ORDER = (4, 3, 5, 2, 6, 1, 7)
Z_ARRIVAL = (0, 1, 7, 2, 6, 3, 5, 4)
ORDER_NT = (((1,), (1,)), ((), ()))


def dot(a, b):
    return jnp.dot(a, b, preferred_element_type=F32)


def dot_nt(a, b):
    return lax.dot_general(a, b, ORDER_NT, preferred_element_type=F32)


def kernel(
    feat_hbm, w_hbm, text_hbm, nef_ref, bias_ref,
    gfeat, gtext, gout,
    w_ref, feat, feat2, feat_t, unit, length, img, traw, tlow, tlen, pair, eg,
    gpart, xbuf, wrow, rbuf, sbuf, xrow, xs, xr, igrad, cross, cross2,
    in_sem, xw_s, xw_r, ag_s, ag_r, dd_s, dd_r, ex_s, ex_r, rs_s, rs_r, xg_s, xg_r,
):
    me = lax.axis_index("blk")
    core = lax.rem(me, 2)
    r = lax.rem(me, ROW)
    z = lax.rem(lax.div(me, ROW), NZ)
    y = lax.div(me, ROW * NZ)
    pending = []

    row_y = [lax.rem(y + j, NY) for j in range(NY)]
    row_z = [lax.rem(z + k, NZ) for k in range(NZ)]
    dev_y = [v * (NZ * ROW) for v in row_y]
    dev_z = [v * ROW + r for v in row_z]
    at_y = [v * YROWS for v in row_y]
    at_z = [v * BLK for v in row_z]

    def dev(dy=0, dz=0):
        return dev_y[dy % NY] + dev_z[dz % NZ]

    wrap = 1 - lax.div(z + (NZ - 1), NZ)
    first = me - r
    pre_row = first + wrap * (dev_y[NY - 1] - dev_y[0])
    below_row = dev(0, -1) - r

    def row_dev(k):
        return me - r + lax.rem(r + k, ROW)

    def near(k):
        return lax.rem(me + (k + N), N)

    def remote(src, dst, ss, rs, to):
        return pltpu.make_async_remote_copy(
            src_ref=src, dst_ref=dst, send_sem=ss, recv_sem=rs, device_id=(to,), device_id_type=MESH
        )

    def send(only, src, dst, ss, rs, to, like=None):
        sems, i = ss
        remote(src, dst, sems.at[i], rs, to).start()

        def wait():
            ref = src if like is None else like()
            remote(ref, ref, sems.at[i], sems.at[i], near(1)).wait_send()

        pending.append((only, wait))

    def arrived(dst, ss, rs):
        remote(dst, dst, ss, rs, near(1)).wait_recv()

    def wblock(ref, dy, dz, c0, cw):
        start = pl.multiple_of(at_y[dy % NY] + at_z[dz % NZ], 8)
        return ref.at[pl.ds(start, BLK), pl.ds(c0, cw)]

    def transpose(src, col):
        if col:
            arrived(feat2, ex_s.at[12], ex_r.at[0])

        @pl.loop(0, D // 256)
        def _(i):
            cols = pl.ds(pl.multiple_of(i * 256, 256), 256)
            feat_t[cols, pl.ds(col, R)] = jnp.transpose(src[:, cols])

    def tslot(k):
        return tlow.at[pl.ds(k * R, R), :]

    def slot(k):
        return img.at[pl.ds(k * R, R), :]

    cp_w = pltpu.make_async_copy(w_hbm, xbuf.at[r], in_sem.at[0])
    cp_t = pltpu.make_async_copy(text_hbm, traw, in_sem.at[1])
    cp_f = pltpu.make_async_copy(feat_hbm, feat, in_sem.at[2])
    cp_w.start()
    cp_t.start()
    cp_f.start()

    with jax.named_scope("barrier"):
        barrier = pltpu.get_barrier_semaphore()
        peers = [row_dev(k) for k in range(1, ROW)] + [dev(dz=k) for k in range(1, NZ)]
        peers += [dev(d) - r + lax.rem(r + d * -k + ROW, ROW) for d in (-1, 1) for k in (3, 7)]
        peers += [dev(0, d) - r + lax.rem(r + d * -k + ROW, ROW) for d in (-1, 1) for k in (2, 6)]
        peers += [dev(dy=k) for k in range(1, NY)] + [near(k) for k in (-ROW, -5, -3, -2, -1, 1, 2, 3, 5, ROW)]
        for peer in peers:
            pl.semaphore_signal(barrier, inc=1, device_id=(peer,), device_id_type=MESH)
        pl.semaphore_wait(barrier, len(peers))

    with jax.named_scope("w_row_send"):
        cp_w.wait()
        for k in (4, 3, 5, 2, 6, 1, 7):
            send(None, xbuf.at[r], xbuf.at[r], (xw_s, k), xw_r.at[k], row_dev(k), lambda: xbuf.at[0])

    with jax.named_scope("own_text"):
        cp_t.wait()

        @pl.loop(0, R // 32)
        def _(i):
            rows = pl.ds(pl.multiple_of(i * 32, 32), 32)
            t = traw[rows, :].astype(F32)
            inv = 1.0 / jnp.sqrt(jnp.sum(t * t, axis=1, keepdims=True) + EPS)
            tlow[rows, :] = (t * inv).astype(BF16)
            tlen[rows, :] = inv

        cp_f.wait()
        send(None, feat, feat2, (ex_s, 12), ex_r.at[0], me + 1 - 2 * core)
        transpose(feat, 0)

    with jax.named_scope("w_row"):
        for k in range(1, ROW):
            arrived(xbuf.at[lax.rem(r + (ROW - k), ROW)], xw_s.at[k], xw_r.at[k])
        for k in range(ROW):
            wrow[pl.ds(SH * k, SH), :] = xbuf[k].astype(F32)
        own = pl.multiple_of(y * YROWS + z * BLK, 8)
        w_ref[pl.ds(own, BLK), :] = wrow[...].astype(BF16)

    with jax.named_scope("text_send"):
        @pl.when((core == 0) & (r != 0))
        def _():
            send("t3", tslot(0), tslot(1), (ex_s, 0), ex_r.at[1], near(-1), lambda: tslot(0))

        @pl.when((core == 0) & (r > 2))
        def _():
            send("t4", tslot(0), tslot(3), (ex_s, 1), ex_r.at[3], near(-3), lambda: tslot(0))

        @pl.when(core == 1)
        def _():
            send(1, tslot(0), tslot(1), (ex_s, 0), ex_r.at[1], near(-1), lambda: tslot(0))

        @pl.when((core == 1) & (r != 1))
        def _():
            send("t2", tslot(0), tslot(2), (ex_s, 1), ex_r.at[2], near(-2), lambda: tslot(0))

        @pl.when(r == 0)
        def _():
            send("r0", tslot(0), cross, (ex_s, 0), ex_r.at[8], pre_row + 7, lambda: tslot(0))
            send("r0", tslot(0), cross, (ex_s, 1), ex_r.at[8], pre_row + 3, lambda: tslot(0))

        @pl.when(r == 2)
        def _():
            send("r2", tslot(0), cross, (ex_s, 1), ex_r.at[8], pre_row + 5, lambda: tslot(0))


    def gather(c):
        c0, cw = COLS[c]
        sibling = me + (1 - 2 * c)
        count = [0]
        like = lambda: w_ref.at[pl.ds(0, BLK), pl.ds(c0, cw)]

        def put(j, k, dy, dz):
            part = wblock(w_ref, -j, -k, c0, cw)
            idx = ((j + dy) % NY) * NZ + (k + dz) % NZ
            send(c, part, part, (ag_s, count[0]), ag_r.at[idx], dev(dy, dz), like)
            count[0] += 1

        def share(j, k):
            part = wblock(w_ref, -j, -k, c0, cw)
            send(c, part, part, (dd_s, j * NZ + k), dd_r.at[j * NZ + k], sibling, like)

        def got(j, k):
            part = wblock(w_ref, -j, -k, c0, cw)
            arrived(part, ag_s.at[0], ag_r.at[j * NZ + k])
            return part

        if c == Y_CORE:
            for k in Z_ARRIVAL[1:]:
                put(0, 0, 0, k)
            transpose(feat2, R)

            def stage1(i):
                k = Z_ARRIVAL[i]
                if k:
                    got(0, k)
                put(0, k, 1, 0)
                put(0, k, -1, 0)
                if k:
                    share(0, k)

            def stage2(i):
                k = Z_ARRIVAL[i]
                got(1, k)
                if i % 2 == 0:
                    put(1, k, 1, 0)
                share(1, k)
                got(3, k)
                if i % 2 == 1:
                    put(3, k, -1, 0)
                share(3, k)

            def stage3(i):
                k = Z_ARRIVAL[i]
                got(2, k)
                share(2, k)

            for i in range(NZ + 4):
                if i < NZ:
                    stage1(i)
                if 2 <= i < NZ + 2:
                    stage2(i - 2)
                if 4 <= i:
                    stage3(i - 4)
        else:
            for j in (1, 3, 2):
                put(0, 0, j, 0)

            @pl.when((r == 1) & (z == 0))
            def _():
                send("r1z", tslot(0), cross, (ex_s, 1), ex_r.at[8], pre_row + 1, lambda: tslot(0))

            for j in (0, 1, 3, 2):
                if j:
                    got(j, 0)
                put(j, 0, 0, 1)
                put(j, 0, 0, -1)
                if j == 0:
                    transpose(feat2, R)
                if j:
                    share(j, 0)
            for h in (1, 2, 3):
                for j in (0, 1, 3, 2):
                    got(j, h)
                    put(j, h, 0, 1)
                    share(j, h)
                    got(j, NZ - h)
                    if h < 3:
                        put(j, NZ - h, 0, -1)
                    share(j, NZ - h)
                if h == 3:

                    @pl.when((r > 1) | (z == 0))
                    def _():
                        arrived(cross, ex_s.at[0], ex_r.at[8])

                    @pl.when((r == 1) & (z == 0))
                    def _():
                        send("r1z", cross, tslot(2), (ex_s, 2), ex_r.at[2], below_row + 7, lambda: tslot(0))

                    @pl.when((r == 1) & (z != 0))
                    def _():
                        send("r1n", tslot(0), tslot(2), (ex_s, 1), ex_r.at[2], below_row + 7, lambda: tslot(0))

                    @pl.when(r == 3)
                    def _():
                        send("r3", cross, tslot(3), (ex_s, 2), ex_r.at[3], below_row + 5, lambda: tslot(0))

                    @pl.when(r == 5)
                    def _():
                        send("r5", cross, tslot(3), (ex_s, 2), ex_r.at[3], below_row + 7, lambda: tslot(0))

                    @pl.when(r == 7)
                    def _():
                        send("r7", cross, tslot(1), (ex_s, 2), ex_r.at[1], below_row + 7, lambda: tslot(0))

            for j in (0, 1, 3, 2):
                got(j, 4)
                share(j, 4)
            @pl.when(r != ROW - 1)
            def _():
                arrived(tslot(1), ex_s.at[0], ex_r.at[1])
                send("o7", tslot(1), tslot(2), (ex_s, 3), ex_r.at[2], near(-1), lambda: tslot(0))
                arrived(tslot(2), ex_s.at[0], ex_r.at[2])
                send("o7", tslot(2), tslot(3), (ex_s, 10), ex_r.at[3], near(-1), lambda: tslot(0))

        o0, ow = COLS[1 - c]
        for j in range(NY):
            for k in range(NZ):
                if j or k:
                    part = wblock(w_ref, -j, -k, o0, ow)
                    arrived(part, dd_s.at[0], dd_r.at[j * NZ + k])

    with jax.named_scope("gather"):
        @pl.when(core == 0)
        def _():
            gather(0)

        @pl.when(core == 1)
        def _():
            gather(1)

    with jax.named_scope("embed"):
        for c0, cw in TILES:
            unit[:, pl.ds(c0, cw)] = dot(feat[...], w_ref[:, pl.ds(c0, cw)])

        @pl.loop(0, R // 32)
        def _(i):
            rows = pl.ds(pl.multiple_of(i * 32, 32), 32)
            e = unit[rows, :]
            inv = 1.0 / jnp.sqrt(jnp.sum(e * e, axis=1, keepdims=True) + EPS)
            u = e * inv
            unit[rows, :] = u
            length[rows, :] = inv
            img[rows, :] = u.astype(BF16)

    @pl.when(r == ROW - 1)
    def _():
        arrived(tslot(1), ex_s.at[0], ex_r.at[1])
        send("r7", tslot(1), tslot(2), (ex_s, 3), ex_r.at[2], near(-1), lambda: tslot(0))
        arrived(tslot(2), ex_s.at[0], ex_r.at[2])
        send("r7", tslot(2), tslot(3), (ex_s, 10), ex_r.at[3], near(-1), lambda: tslot(0))

    with jax.named_scope("image_send"):
        i3 = (core == 1) & (r != ROW - 1) & (r != 5)

        @pl.when(r == 5)
        def _():
            send("i5", slot(0), cross2, (ex_s, 6), ex_r.at[9], near(5), lambda: slot(0))

        @pl.when(r == ROW - 2)
        def _():
            send("i6", slot(0), cross2, (ex_s, 6), ex_r.at[9], first, lambda: slot(0))

        i5_early = (core == 1) & (r != ROW - 1) & ((r != 5) | (z != NZ - 1))

        @pl.when(core == 1)
        def _():
            send(1, slot(0), slot(1), (ex_s, 5), ex_r.at[5], near(1), lambda: slot(0))

        @pl.when(i3)
        def _():
            send("i3", slot(0), slot(3), (ex_s, 6), ex_r.at[7], near(3), lambda: slot(0))

        @pl.when(core == 0)
        def _():
            send(0, slot(0), slot(1), (ex_s, 5), ex_r.at[5], near(1), lambda: slot(0))

        @pl.when((core == 0) & (r != ROW - 2))
        def _():
            send("i2", slot(0), slot(2), (ex_s, 6), ex_r.at[6], near(2), lambda: slot(0))

    factor = jnp.exp(jnp.full((1, R), nef_ref[0], F32))
    bias = bias_ref[0]

    def derivative(logit_dot, diagonal):
        logits = factor * logit_dot + bias
        if diagonal:
            same = lax.broadcasted_iota(jnp.int32, (R, R), 0) == lax.broadcasted_iota(jnp.int32, (R, R), 1)
            label = jnp.where(same, 1.0, -1.0).astype(F32)
            g = -factor * label / (1.0 + jnp.exp(label * logits))
        else:
            g = factor / (1.0 + jnp.exp(-logits))
        return g.astype(BF16)

    def back(grad, u, inv):
        return (grad - u * jnp.sum(u * grad, axis=1, keepdims=True)) * inv

    with jax.named_scope("image_side"):
        for s in range(S):
            if s == 1:

                @pl.when(core == 0)
                def _():
                    arrived(tslot(1), ex_s.at[0], ex_r.at[1])
                    arrived(tslot(2), ex_s.at[0], ex_r.at[2])

            if s == 3:
                with jax.named_scope("text_wait"):
                    arrived(tslot(3), ex_s.at[0], ex_r.at[3])
            pair[:, pl.ds(s * R, R)] = derivative(dot_nt(img[pl.ds(0, R), :], tlow[pl.ds(s * R, R), :]), s == 0)
        for c0, cw in TILES:
            igrad[:, pl.ds(c0, cw)] = dot(pair[...], tlow[:, pl.ds(c0, cw)])

        @pl.loop(0, R // 32)
        def _(i):
            rows = pl.ds(pl.multiple_of(i * 32, 32), 32)
            eg[rows, :] = back(igrad[rows, :], unit[rows, :], length[rows, :]).astype(BF16)

    with jax.named_scope("eg_send"):
        @pl.when(core == 0)
        def _():
            part = pl.ds(COLS[1][0], COLS[1][1])
            send(0, eg.at[pl.ds(0, R), part], eg.at[pl.ds(R, R), part], (ex_s, 9), ex_r.at[10], me + 1, lambda: eg.at[pl.ds(0, R), pl.ds(COLS[1][0], COLS[1][1])])

        @pl.when(core == 1)
        def _():
            part = pl.ds(COLS[0][0], COLS[0][1])
            send(1, eg.at[pl.ds(0, R), part], eg.at[pl.ds(R, R), part], (ex_s, 9), ex_r.at[10], me - 1, lambda: eg.at[pl.ds(0, R), pl.ds(COLS[0][0], COLS[0][1])])

    with jax.named_scope("feat_grad"):
        @pl.loop(0, D // 512)
        def _(i):
            cols = pl.ds(pl.multiple_of(i * 512, 512), 512)
            gfeat[:, cols] = dot_nt(eg[pl.ds(0, R), :], w_ref[cols, :]).astype(BF16)


    def reduce_weight(c):
        c0, cw = COLS[c]
        count = [0]
        arrived(eg.at[pl.ds(R, R), pl.ds(c0, cw)], ex_s.at[0], ex_r.at[10])

        def product(j):
            rows = pl.ds(pl.multiple_of(at_y[j], 8), YROWS)
            gpart[rows, pl.ds(0, cw)] = dot(feat_t[rows, :], eg[:, pl.ds(c0, cw)]).astype(BF16)

        def mine(dy, dz):
            return wblock(gpart, dy, dz, 0, cw)

        def buf(i):
            return rbuf.at[i, :, pl.ds(0, cw)]

        def emit(src, i, dy, dz):
            send(c, src, buf(i), (rs_s, count[0]), rs_r.at[i], dev(dy, dz), lambda: buf(0))
            count[0] += 1

        def take(i):
            arrived(buf(i), rs_s.at[0], rs_r.at[i])
            return buf(i)[...].astype(F32)

        if c == Y_CORE:
            product(2)
            for i, k in enumerate(Z_ORDER + (0,)):
                emit(mine(2, k), k, 1 if i % 2 == 0 else -1, 0)
            product(1)
            product(3)
            product(0)
            for i, k in enumerate(Z_ORDER + (0,)):
                step = 1 if i % 2 == 0 else -1
                part = mine(step, k)
                other = mine(-step, k)
                emit(other, 8 + k if step == -1 else 16 + k, -step, 0)
                part[...] = (part[...].astype(F32) + take(k)).astype(BF16)
                emit(part, 8 + k if step == 1 else 16 + k, step, 0)
            @pl.when((r == 0) | (r == 2))
            def _():
                arrived(cross2, ex_s.at[0], ex_r.at[9])

            @pl.when(r == 0)
            def _():
                send("i0", cross2, slot(2), (ex_s, 13), ex_r.at[6], near(ROW), lambda: slot(0))

            @pl.when(r == 2)
            def _():
                send("i2r", cross2, slot(3), (ex_s, 13), ex_r.at[7], first, lambda: slot(0))

            for i, k in enumerate(Z_ORDER + (0,)):
                total = mine(0, k)[...].astype(F32) + take(8 + k) + take(16 + k)
                if k:
                    sbuf[k, :, pl.ds(0, cw)] = total.astype(BF16)
                    emit(sbuf.at[k, :, pl.ds(0, cw)], 24 + k, 0, k)
            arrived(slot(1), ex_s.at[0], ex_r.at[5])
            send(0, slot(1), slot(2), (ex_s, 8), ex_r.at[6], near(1), lambda: slot(0))

            @pl.when(r == 0)
            def _():
                send("i0", slot(1), slot(3), (ex_s, 7), ex_r.at[7], near(2), lambda: slot(0))


            for k in Z_ARRIVAL[1:]:
                total = total + take(24 + k)
        else:
            for j in range(NY):
                product(j)
            order = (2, 1, 3, 0)
            for j in order:
                emit(mine(j, 4), 16 + j, 0, -1)
            for h in (3, 2, 1):
                s = 3 - h
                for j in order:
                    for sign, base in ((1, 0), (-1, 16)):
                        part = mine(j, sign * h)
                        if s or sign == -1:
                            part[...] = (part[...].astype(F32) + take(base + 4 * s + j)).astype(BF16)
                        emit(part, base + 4 * (s + 1) + j, 0, sign)
            for j in order:
                total = mine(j, 0)[...].astype(F32) + take(12 + j) + take(28 + j)
                if j:
                    sbuf[j, :, pl.ds(0, cw)] = total.astype(BF16)
                    emit(sbuf.at[j, :, pl.ds(0, cw)], 32 + j, j, 0)
            for j in (1, 3, 2):
                total = total + take(32 + j)

        xrow[:, pl.ds(0, cw)] = total
        for k in range(ROW):
            xs[k, :, pl.ds(0, cw)] = xrow[pl.ds(SH * k, SH), pl.ds(0, cw)]
        for k in (4, 3, 5, 2, 6, 1, 7):
            send(
                c, xs.at[lax.rem(r + k, ROW), :, pl.ds(0, cw)], xr.at[r, :, pl.ds(0, cw)],
                (xg_s, k), xg_r.at[k], row_dev(k), lambda: xs.at[0, :, pl.ds(0, cw)],
            )
        xr[r, :, pl.ds(0, cw)] = xs[r, :, pl.ds(0, cw)]

    with jax.named_scope("reduce"):
        @pl.when(core == 0)
        def _():
            reduce_weight(0)

        @pl.when(core == 1)
        def _():
            reduce_weight(1)

    with jax.named_scope("image_wait"):
        @pl.when(core == 0)
        def _():
            arrived(slot(2), ex_s.at[0], ex_r.at[6])
            send(0, slot(2), slot(3), (ex_s, 11), ex_r.at[7], near(1), lambda: slot(0))

        @pl.when(core == 1)
        def _():
            arrived(slot(1), ex_s.at[0], ex_r.at[5])
            arrived(slot(2), ex_s.at[0], ex_r.at[6])

        arrived(slot(3), ex_s.at[0], ex_r.at[7])

    with jax.named_scope("text_side"):
        for s in range(S):
            pair[:, pl.ds(s * R, R)] = derivative(dot_nt(tlow[pl.ds(0, R), :], img[pl.ds(s * R, R), :]), s == 0)
        for c0, cw in TILES:
            igrad[:, pl.ds(c0, cw)] = dot(pair[...], img[:, pl.ds(c0, cw)])

        @pl.loop(0, R // 32)
        def _(i):
            rows = pl.ds(pl.multiple_of(i * 32, 32), 32)
            inv = tlen[rows, :]
            gtext[rows, :] = back(igrad[rows, :], traw[rows, :].astype(F32) * inv, inv).astype(BF16)

    with jax.named_scope("final"):
        for k in range(1, ROW):
            source = lax.rem(r + (ROW - k), ROW)

            @pl.when(lax.rem(source, 2) == 1)
            def _():
                arrived(xr.at[source, :, pl.ds(0, COLS[1][1])], xg_s.at[k], xg_r.at[k])

            @pl.when(lax.rem(source, 2) == 0)
            def _():
                arrived(xr.at[source, :, pl.ds(0, COLS[0][1])], xg_s.at[k], xg_r.at[k])

        for c in range(2):
            c0, cw = COLS[c]
            total = xr[c, :, pl.ds(0, cw)]
            for k in range(1, NX):
                total = total + xr[2 * k + c, :, pl.ds(0, cw)]
            gout[:, pl.ds(c0, cw)] = total

    with jax.named_scope("drain"):
        for only, wait in pending:
            if only is None:
                wait()
        groups = {
            0: core == 0, 1: core == 1, "r0": r == 0, "r2": r == 2, "r3": r == 3, "r5": r == 5, "r1z": (r == 1) & (z == 0), "r1n": (r == 1) & (z != 0), "r7": r == ROW - 1, "i0": r == 0,
            "o7": (core == 1) & (r != ROW - 1), "t3": (core == 0) & (r != 0), "t4": (core == 0) & (r > 2),
            "t2": (core == 1) & (r != 1), "i3": i3, "i5": r == 5, "i2r": r == 2, "i6": r == ROW - 2,
            "i2": (core == 0) & (r != ROW - 2),
        }
        for group, inside in groups.items():

            @pl.when(inside)
            def _():
                for only, wait in pending:
                    if only == group:
                        wait()


def put_out(gf, gt, gw, gf_out, gt_out, gw_out, sem):
    copies = [pltpu.make_async_copy(a, b, sem.at[i]) for i, (a, b) in enumerate(((gf, gf_out), (gt, gt_out), (gw, gw_out)))]
    for copy in copies:
        copy.start()
    for copy in copies:
        copy.wait()


def on_device(image_features, head_weight, text_embeds, natural_exponent_factor, logit_bias):
    dma = pltpu.SemaphoreType.DMA
    hbm = pl.BlockSpec(memory_space=pltpu.HBM)
    local = pl.BlockSpec(memory_space=pltpu.VMEM)
    scalar = pl.BlockSpec(memory_space=pltpu.SMEM)
    results = pl.pallas_call(
        kernel,
        out_shape=(
            jax.ShapeDtypeStruct((R, D), BF16),
            jax.ShapeDtypeStruct((R, E), BF16),
            jax.ShapeDtypeStruct((SH, E), F32),
        ),
        in_specs=[hbm, hbm, hbm, scalar, scalar],
        out_specs=(local, local, local),
        scratch_shapes=[
            pltpu.VMEM((D, E), BF16),
            pltpu.VMEM((R, D), BF16),
            pltpu.VMEM((R, D), BF16),
            pltpu.VMEM((D, 2 * R), BF16),
            pltpu.VMEM((R, E), F32),
            pltpu.VMEM((R, 1), F32),
            pltpu.VMEM((S * R, E), BF16),
            pltpu.VMEM((R, E), BF16),
            pltpu.VMEM((S * R, E), BF16),
            pltpu.VMEM((R, 1), F32),
            pltpu.VMEM((R, S * R), BF16),
            pltpu.VMEM((2 * R, E), BF16),
            pltpu.VMEM((D, W1), BF16),
            pltpu.VMEM((ROW, SH, E), BF16),
            pltpu.VMEM((BLK, E), F32),
            pltpu.VMEM((36, BLK, W1), BF16),
            pltpu.VMEM((8, BLK, W1), BF16),
            pltpu.VMEM((BLK, W1), F32),
            pltpu.VMEM((ROW, SH, W1), F32),
            pltpu.VMEM((ROW, SH, W1), F32),
            pltpu.VMEM((R, E), F32),
            pltpu.VMEM((R, E), BF16),
            pltpu.VMEM((R, E), BF16),
            dma((3,)),
            dma((ROW,)), dma((ROW,)),
            dma((32,)), dma((32,)),
            dma((32,)), dma((32,)),
            dma((14,)), dma((11,)),
            dma((40,)), dma((36,)),
            dma((ROW,)), dma((ROW,)),
        ],
        compiler_params=pltpu.CompilerParams(
            collective_id=0, has_side_effects=True, vmem_limit_bytes=32 * 1024 * 1024
        ),
    )(image_features, head_weight, text_embeds, natural_exponent_factor, logit_bias)
    return pl.pallas_call(
        put_out,
        out_shape=tuple(jax.ShapeDtypeStruct(a.shape, a.dtype) for a in results),
        in_specs=[local] * 3,
        out_specs=[hbm] * 3,
        scratch_shapes=[dma((3,))],
        compiler_params=pltpu.CompilerParams(vmem_limit_bytes=8 * 1024 * 1024),
    )(*results)


def solution(mesh):
    split = P("blk", None)
    return jax.shard_map(
        on_device,
        mesh=mesh,
        in_specs=(split, split, split, P(), P()),
        out_specs=(split, split, split),
        check_vma=False,
    )
```

```python
import jax
import jax.numpy as jnp
from jax import lax
from jax.experimental import pallas as pl
from jax.experimental.pallas import tpu as pltpu
from jax.sharding import PartitionSpec as P

MESH = pl.DeviceIdType.MESH
D, E, R, S = 1536, 1152, 256, 4
NY, NZ, NX = 4, 8, 4
N = NY * NZ * NX * 2
ROW = NX * 2
SH = D // N
BLK = SH * ROW
YROWS = BLK * NZ
W1 = 640
COLS = ((0, W1), (W1, E - W1))
FAR, NEAR = 5, 0
Y_CORE = 0
EPS = 1e-06
TILES = ((0, 512), (512, 512), (1024, 128))
F32, BF16 = jnp.float32, jnp.bfloat16
Z_ORDER = (4, 3, 5, 2, 6, 1, 7)
Z_ARRIVAL = (0, 1, 7, 2, 6, 3, 5, 4)
ORDER_NT = (((1,), (1,)), ((), ()))


def dot(a, b):
    return jnp.dot(a, b, preferred_element_type=F32)


def dot_nt(a, b):
    return lax.dot_general(a, b, ORDER_NT, preferred_element_type=F32)


def kernel(
    feat_hbm, w_hbm, text_hbm, nef_ref, bias_ref,
    gfeat, gtext, gout,
    w_ref, feat, feat2, feat_t, unit, length, img, traw, tlow, tlen, pair, eg,
    gpart, xbuf, wrow, rbuf, sbuf, xrow, xs, xr, igrad, cross, cross2,
    in_sem, xw_s, xw_r, ag_s, ag_r, dd_s, dd_r, ex_s, ex_r, rs_s, rs_r, xg_s, xg_r,
):
    me = lax.axis_index("blk")
    core = lax.rem(me, 2)
    r = lax.rem(me, ROW)
    z = lax.rem(lax.div(me, ROW), NZ)
    y = lax.div(me, ROW * NZ)
    pending = []

    row_y = [lax.rem(y + j, NY) for j in range(NY)]
    row_z = [lax.rem(z + k, NZ) for k in range(NZ)]
    dev_y = [v * (NZ * ROW) for v in row_y]
    dev_z = [v * ROW + r for v in row_z]
    at_y = [v * YROWS for v in row_y]
    at_z = [v * BLK for v in row_z]

    def dev(dy=0, dz=0):
        return dev_y[dy % NY] + dev_z[dz % NZ]

    wrap = 1 - lax.div(z + (NZ - 1), NZ)
    first = me - r
    pre_row = first + wrap * (dev_y[NY - 1] - dev_y[0])
    below_row = dev(0, -1) - r

    def row_dev(k):
        return me - r + lax.rem(r + k, ROW)

    def near(k):
        return lax.rem(me + (k + N), N)

    def remote(src, dst, ss, rs, to):
        return pltpu.make_async_remote_copy(
            src_ref=src, dst_ref=dst, send_sem=ss, recv_sem=rs, device_id=(to,), device_id_type=MESH
        )

    def send(only, src, dst, ss, rs, to, like=None):
        sems, i = ss
        remote(src, dst, sems.at[i], rs, to).start()

        def wait():
            ref = src if like is None else like()
            remote(ref, ref, sems.at[i], sems.at[i], near(1)).wait_send()

        pending.append((only, wait))

    def arrived(dst, ss, rs):
        remote(dst, dst, ss, rs, near(1)).wait_recv()

    def wblock(ref, dy, dz, c0, cw):
        start = pl.multiple_of(at_y[dy % NY] + at_z[dz % NZ], 8)
        return ref.at[pl.ds(start, BLK), pl.ds(c0, cw)]

    def transpose(src, col):
        if col:
            arrived(feat2, ex_s.at[12], ex_r.at[0])

        @pl.loop(0, D // 256)
        def _(i):
            cols = pl.ds(pl.multiple_of(i * 256, 256), 256)
            feat_t[cols, pl.ds(col, R)] = jnp.transpose(src[:, cols])

    def tslot(k):
        return tlow.at[pl.ds(k * R, R), :]

    def slot(k):
        return img.at[pl.ds(k * R, R), :]

    cp_w = pltpu.make_async_copy(w_hbm, xbuf.at[r], in_sem.at[0])
    cp_t = pltpu.make_async_copy(text_hbm, traw, in_sem.at[1])
    cp_f = pltpu.make_async_copy(feat_hbm, feat, in_sem.at[2])
    cp_w.start()
    cp_t.start()
    cp_f.start()

    with jax.named_scope("barrier"):
        barrier = pltpu.get_barrier_semaphore()
        peers = [row_dev(k) for k in range(1, ROW)] + [dev(dz=k) for k in range(1, NZ)]
        peers += [dev(d) - r + lax.rem(r + d * -k + ROW, ROW) for d in (-1, 1) for k in (1, 3, 7)]
        peers += [dev(0, d) - r + lax.rem(r + d * -k + ROW, ROW) for d in (-1, 1) for k in (2, 6)]
        peers += [dev(dy=k) for k in range(1, NY)] + [near(k) for k in (-ROW, -5, -3, -2, -1, 1, 2, 3, 5, ROW)]
        for peer in peers:
            pl.semaphore_signal(barrier, inc=1, device_id=(peer,), device_id_type=MESH)
        pl.semaphore_wait(barrier, len(peers))

    with jax.named_scope("w_row_send"):
        cp_w.wait()
        for k in (4, 3, 5, 2, 6, 1, 7):
            send(None, xbuf.at[r], xbuf.at[r], (xw_s, k), xw_r.at[k], row_dev(k), lambda: xbuf.at[0])

    with jax.named_scope("own_text"):
        cp_t.wait()

        @pl.loop(0, R // 32)
        def _(i):
            rows = pl.ds(pl.multiple_of(i * 32, 32), 32)
            t = traw[rows, :].astype(F32)
            inv = 1.0 / jnp.sqrt(jnp.sum(t * t, axis=1, keepdims=True) + EPS)
            tlow[rows, :] = (t * inv).astype(BF16)
            tlen[rows, :] = inv

        cp_f.wait()
        send(None, feat, feat2, (ex_s, 12), ex_r.at[0], me + 1 - 2 * core)
        transpose(feat, 0)

    with jax.named_scope("w_row"):
        for k in range(1, ROW):
            arrived(xbuf.at[lax.rem(r + (ROW - k), ROW)], xw_s.at[k], xw_r.at[k])
        for k in range(ROW):
            wrow[pl.ds(SH * k, SH), :] = xbuf[k].astype(F32)
        own = pl.multiple_of(y * YROWS + z * BLK, 8)
        w_ref[pl.ds(own, BLK), :] = wrow[...].astype(BF16)

    with jax.named_scope("text_send"):
        @pl.when((core == 0) & (r != 0))
        def _():
            send("t3", tslot(0), tslot(1), (ex_s, 0), ex_r.at[1], near(-1), lambda: tslot(0))

        @pl.when((core == 0) & (r > 2))
        def _():
            send("t4", tslot(0), tslot(3), (ex_s, 1), ex_r.at[3], near(-3), lambda: tslot(0))

        @pl.when(core == 1)
        def _():
            send(1, tslot(0), tslot(1), (ex_s, 0), ex_r.at[1], near(-1), lambda: tslot(0))

        @pl.when((core == 1) & (r != 1))
        def _():
            send("t2", tslot(0), tslot(2), (ex_s, 1), ex_r.at[2], near(-2), lambda: tslot(0))

        @pl.when(r == 0)
        def _():
            send("r0", tslot(0), cross, (ex_s, 0), ex_r.at[8], pre_row + 7, lambda: tslot(0))
            send("r0", tslot(0), cross, (ex_s, 1), ex_r.at[8], pre_row + 3, lambda: tslot(0))

        @pl.when(r == 2)
        def _():
            send("r2", tslot(0), cross, (ex_s, 1), ex_r.at[8], pre_row + 5, lambda: tslot(0))


    def gather(c):
        c0, cw = COLS[c]
        sibling = me + (1 - 2 * c)
        count = [0]
        like = lambda: w_ref.at[pl.ds(0, BLK), pl.ds(c0, cw)]

        def put(j, k, dy, dz):
            part = wblock(w_ref, -j, -k, c0, cw)
            idx = ((j + dy) % NY) * NZ + (k + dz) % NZ
            send(c, part, part, (ag_s, count[0]), ag_r.at[idx], dev(dy, dz), like)
            count[0] += 1

        def share(j, k):
            part = wblock(w_ref, -j, -k, c0, cw)
            send(c, part, part, (dd_s, j * NZ + k), dd_r.at[j * NZ + k], sibling, like)

        def got(j, k):
            part = wblock(w_ref, -j, -k, c0, cw)
            arrived(part, ag_s.at[0], ag_r.at[j * NZ + k])
            return part

        if c == Y_CORE:
            for k in Z_ARRIVAL[1:]:
                put(0, 0, 0, k)
            transpose(feat2, R)

            def stage1(i):
                k = Z_ARRIVAL[i]
                if k:
                    got(0, k)
                put(0, k, 1, 0)
                put(0, k, -1, 0)
                if i >= FAR:
                    put(0, k, 2, 0)
                if k:
                    share(0, k)

            def stage2(i):
                k = Z_ARRIVAL[i]
                got(1, k)
                if i < FAR and i % 2 == 0:
                    put(1, k, 1, 0)
                share(1, k)
                got(3, k)
                if i < FAR and i % 2 == 1:
                    put(3, k, -1, 0)
                share(3, k)

            def stage3(i):
                k = Z_ARRIVAL[i]
                got(2, k)
                share(2, k)

            for i in range(NZ + 4):
                if i < NZ:
                    stage1(i)
                if 2 <= i < NZ + 2:
                    stage2(i - 2)
                if 4 <= i:
                    stage3(i - 4)
        else:
            for j in (1, 3, 2):
                put(0, 0, j, 0)

            @pl.when((r == 1) & (z == 0))
            def _():
                send("r1z", tslot(0), cross, (ex_s, 1), ex_r.at[8], pre_row + 1, lambda: tslot(0))

            for j in (0, 1, 3, 2):
                if j:
                    got(j, 0)
                put(j, 0, 0, 1)
                put(j, 0, 0, -1)
                if j == 0:
                    transpose(feat2, R)
                if j:
                    share(j, 0)
            for h in (1, 2, 3):
                for j in (0, 1, 3, 2):
                    got(j, h)
                    put(j, h, 0, 1)
                    share(j, h)
                    got(j, NZ - h)
                    if h < 3:
                        put(j, NZ - h, 0, -1)
                    share(j, NZ - h)
                if h == 3:

                    @pl.when((r > 1) | (z == 0))
                    def _():
                        arrived(cross, ex_s.at[0], ex_r.at[8])

                    @pl.when((r == 1) & (z == 0))
                    def _():
                        send("r1z", cross, tslot(2), (ex_s, 2), ex_r.at[2], below_row + 7, lambda: tslot(0))

                    @pl.when((r == 1) & (z != 0))
                    def _():
                        send("r1n", tslot(0), tslot(2), (ex_s, 1), ex_r.at[2], below_row + 7, lambda: tslot(0))

                    @pl.when(r == 3)
                    def _():
                        send("r3", cross, tslot(3), (ex_s, 2), ex_r.at[3], below_row + 5, lambda: tslot(0))

                    @pl.when(r == 5)
                    def _():
                        send("r5", cross, tslot(3), (ex_s, 2), ex_r.at[3], below_row + 7, lambda: tslot(0))

                    @pl.when(r == 7)
                    def _():
                        send("r7", cross, tslot(1), (ex_s, 2), ex_r.at[1], below_row + 7, lambda: tslot(0))

            for j in (0, 1, 3, 2):
                got(j, 4)
                share(j, 4)
            @pl.when(r != ROW - 1)
            def _():
                arrived(tslot(1), ex_s.at[0], ex_r.at[1])
                send("o7", tslot(1), tslot(2), (ex_s, 3), ex_r.at[2], near(-1), lambda: tslot(0))
                arrived(tslot(2), ex_s.at[0], ex_r.at[2])
                send("o7", tslot(2), tslot(3), (ex_s, 10), ex_r.at[3], near(-1), lambda: tslot(0))

        o0, ow = COLS[1 - c]
        for j in range(NY):
            for k in range(NZ):
                if j or k:
                    part = wblock(w_ref, -j, -k, o0, ow)
                    arrived(part, dd_s.at[0], dd_r.at[j * NZ + k])

    with jax.named_scope("gather"):
        @pl.when(core == 0)
        def _():
            gather(0)

        @pl.when(core == 1)
        def _():
            gather(1)

    with jax.named_scope("embed"):
        for c0, cw in TILES:
            unit[:, pl.ds(c0, cw)] = dot(feat[...], w_ref[:, pl.ds(c0, cw)])

        @pl.loop(0, R // 32)
        def _(i):
            rows = pl.ds(pl.multiple_of(i * 32, 32), 32)
            e = unit[rows, :]
            inv = 1.0 / jnp.sqrt(jnp.sum(e * e, axis=1, keepdims=True) + EPS)
            u = e * inv
            unit[rows, :] = u
            length[rows, :] = inv
            img[rows, :] = u.astype(BF16)

    @pl.when(r == ROW - 1)
    def _():
        arrived(tslot(1), ex_s.at[0], ex_r.at[1])
        send("r7", tslot(1), tslot(2), (ex_s, 3), ex_r.at[2], near(-1), lambda: tslot(0))
        arrived(tslot(2), ex_s.at[0], ex_r.at[2])
        send("r7", tslot(2), tslot(3), (ex_s, 10), ex_r.at[3], near(-1), lambda: tslot(0))

    with jax.named_scope("image_send"):
        i3 = (core == 1) & (r != ROW - 1) & (r != 5)
        last = z == NZ - 1
        i7_last = (r == ROW - 1) & last

        @pl.when(i7_last)
        def _():
            send("i7", slot(0), cross2, (ex_s, 5), ex_r.at[9], dev(1) - 1, lambda: slot(0))
            send("i7", slot(0), cross2, (ex_s, 6), ex_r.at[9], dev(1) - 3, lambda: slot(0))

        early = (r == 0) & (z != 0)

        @pl.when(r == 5)
        def _():
            send("i5", slot(0), cross2, (ex_s, 6), ex_r.at[9], near(5), lambda: slot(0))

        i5_early = (core == 1) & (r != ROW - 1) & ((r != 5) | (z != NZ - 1))

        @pl.when((core == 1) & ((r != ROW - 1) | (z != NZ - 1)))
        def _():
            send("i1", slot(0), slot(1), (ex_s, 5), ex_r.at[5], near(1), lambda: slot(0))

        @pl.when(i3)
        def _():
            send("i3", slot(0), slot(3), (ex_s, 6), ex_r.at[7], near(3), lambda: slot(0))

        @pl.when(core == 0)
        def _():
            send(0, slot(0), slot(1), (ex_s, 5), ex_r.at[5], near(1), lambda: slot(0))

        @pl.when((core == 0) & (r != ROW - 2))
        def _():
            send("i2", slot(0), slot(2), (ex_s, 6), ex_r.at[6], near(2), lambda: slot(0))

    factor = jnp.exp(jnp.full((1, R), nef_ref[0], F32))
    bias = bias_ref[0]

    def derivative(logit_dot, diagonal):
        logits = factor * logit_dot + bias
        if diagonal:
            same = lax.broadcasted_iota(jnp.int32, (R, R), 0) == lax.broadcasted_iota(jnp.int32, (R, R), 1)
            label = jnp.where(same, 1.0, -1.0).astype(F32)
            g = -factor * label / (1.0 + jnp.exp(label * logits))
        else:
            g = factor / (1.0 + jnp.exp(-logits))
        return g.astype(BF16)

    def back(grad, u, inv):
        return (grad - u * jnp.sum(u * grad, axis=1, keepdims=True)) * inv

    with jax.named_scope("image_side"):
        for s in range(S):
            if s == 1:

                @pl.when(core == 0)
                def _():
                    arrived(tslot(1), ex_s.at[0], ex_r.at[1])
                    arrived(tslot(2), ex_s.at[0], ex_r.at[2])

            if s == 3:
                with jax.named_scope("text_wait"):
                    arrived(tslot(3), ex_s.at[0], ex_r.at[3])
            pair[:, pl.ds(s * R, R)] = derivative(dot_nt(img[pl.ds(0, R), :], tlow[pl.ds(s * R, R), :]), s == 0)
        for c0, cw in TILES:
            igrad[:, pl.ds(c0, cw)] = dot(pair[...], tlow[:, pl.ds(c0, cw)])

        @pl.loop(0, R // 32)
        def _(i):
            rows = pl.ds(pl.multiple_of(i * 32, 32), 32)
            eg[rows, :] = back(igrad[rows, :], unit[rows, :], length[rows, :]).astype(BF16)

    with jax.named_scope("eg_send"):
        @pl.when(core == 0)
        def _():
            part = pl.ds(COLS[1][0], COLS[1][1])
            send(0, eg.at[pl.ds(0, R), part], eg.at[pl.ds(R, R), part], (ex_s, 9), ex_r.at[10], me + 1, lambda: eg.at[pl.ds(0, R), pl.ds(COLS[1][0], COLS[1][1])])

        @pl.when(core == 1)
        def _():
            part = pl.ds(COLS[0][0], COLS[0][1])
            send(1, eg.at[pl.ds(0, R), part], eg.at[pl.ds(R, R), part], (ex_s, 9), ex_r.at[10], me - 1, lambda: eg.at[pl.ds(0, R), pl.ds(COLS[0][0], COLS[0][1])])

    def feature_gradient(i):
        cols = pl.ds(i * 512, 512)
        gfeat[:, cols] = dot_nt(eg[pl.ds(0, R), :], w_ref[cols, :]).astype(BF16)

    with jax.named_scope("feat_grad"):
        feature_gradient(0)
        feature_gradient(1)

    def reduce_weight(c):
        c0, cw = COLS[c]
        count = [0]
        arrived(eg.at[pl.ds(R, R), pl.ds(c0, cw)], ex_s.at[0], ex_r.at[10])

        def product(j):
            rows = pl.ds(pl.multiple_of(at_y[j], 8), YROWS)
            gpart[rows, pl.ds(0, cw)] = dot(feat_t[rows, :], eg[:, pl.ds(c0, cw)]).astype(BF16)

        def mine(dy, dz):
            return wblock(gpart, dy, dz, 0, cw)

        def buf(i):
            return rbuf.at[i, :, pl.ds(0, cw)]

        def emit(src, i, dy, dz):
            send(c, src, buf(i), (rs_s, count[0]), rs_r.at[i], dev(dy, dz), lambda: buf(0))
            count[0] += 1

        def take(i):
            arrived(buf(i), rs_s.at[0], rs_r.at[i])
            return buf(i)[...].astype(F32)

        if c == Y_CORE:
            product(2)

            @pl.when(r == ROW - 2)
            def _():
                send("i6", slot(0), cross2, (ex_s, 6), ex_r.at[9], first, lambda: slot(0))

            for i, k in enumerate(Z_ORDER + (0,)):
                emit(mine(2, k), k, 2 if i < NEAR else 1 if i % 2 == 0 else -1, 0)
            product(1)
            product(3)
            product(0)
            feature_gradient(2)
            for i, k in enumerate(Z_ORDER + (0,)):
                step = 1 if i % 2 == 0 else -1
                part = mine(step, k)
                other = mine(-step, k)
                emit(other, 8 + k if step == -1 else 16 + k, -step, 0)
                if i >= NEAR:
                    part[...] = (part[...].astype(F32) + take(k)).astype(BF16)
                emit(part, 8 + k if step == 1 else 16 + k, step, 0)
            @pl.when(r == 2)
            def _():
                arrived(cross2, ex_s.at[0], ex_r.at[9])
                send("i2r", cross2, slot(3), (ex_s, 13), ex_r.at[7], first, lambda: slot(0))

            for i, k in enumerate(Z_ORDER + (0,)):
                total = mine(0, k)[...].astype(F32) + take(8 + k) + take(16 + k)
                if i < NEAR:
                    total = total + take(k)
                if k:
                    sbuf[k, :, pl.ds(0, cw)] = total.astype(BF16)
                    emit(sbuf.at[k, :, pl.ds(0, cw)], 24 + k, 0, k)
            @pl.when(r == 0)
            def _():
                arrived(cross2, ex_s.at[0], ex_r.at[9])
                send("i0", cross2, slot(2), (ex_s, 13), ex_r.at[6], near(ROW), lambda: slot(0))

            @pl.when(((r == 4) | (r == 6)) & last)
            def _():
                arrived(cross2, ex_s.at[0], ex_r.at[9])

            @pl.when((r == 6) & last)
            def _():
                send("i6r", cross2, slot(1), (ex_s, 13), ex_r.at[5], dev(0, 1) - r, lambda: slot(0))

            @pl.when((r == 4) & last)
            def _():
                send("i4r", cross2, slot(3), (ex_s, 13), ex_r.at[7], dev(0, 1) - r + 2, lambda: slot(0))

            @pl.when(early)
            def _():
                arrived(slot(1), ex_s.at[0], ex_r.at[5])
                send("i0e", slot(1), slot(3), (ex_s, 7), ex_r.at[7], near(2), lambda: slot(0))

            for k in Z_ARRIVAL[1:]:
                total = total + take(24 + k)
        else:
            for j in range(NY):
                product(j)
            order = (2, 1, 3, 0)
            for j in order:
                emit(mine(j, 4), 16 + j, 0, -1)
            feature_gradient(2)
            for h in (3, 2, 1):
                s = 3 - h
                for j in order:
                    for sign, base in ((1, 0), (-1, 16)):
                        part = mine(j, sign * h)
                        if s or sign == -1:
                            part[...] = (part[...].astype(F32) + take(base + 4 * s + j)).astype(BF16)
                        emit(part, base + 4 * (s + 1) + j, 0, sign)
            for j in order:
                total = mine(j, 0)[...].astype(F32) + take(12 + j) + take(28 + j)
                if j:
                    sbuf[j, :, pl.ds(0, cw)] = total.astype(BF16)
                    emit(sbuf.at[j, :, pl.ds(0, cw)], 32 + j, j, 0)
            for j in (1, 3, 2):
                total = total + take(32 + j)

        xrow[:, pl.ds(0, cw)] = total
        for k in range(ROW):
            xs[k, :, pl.ds(0, cw)] = xrow[pl.ds(SH * k, SH), pl.ds(0, cw)]
        for k in (4, 3, 5, 2, 6, 1, 7):
            send(
                c, xs.at[lax.rem(r + k, ROW), :, pl.ds(0, cw)], xr.at[r, :, pl.ds(0, cw)],
                (xg_s, k), xg_r.at[k], row_dev(k), lambda: xs.at[0, :, pl.ds(0, cw)],
            )
        xr[r, :, pl.ds(0, cw)] = xs[r, :, pl.ds(0, cw)]

    with jax.named_scope("reduce"):
        @pl.when(core == 0)
        def _():
            reduce_weight(0)

        @pl.when(core == 1)
        def _():
            reduce_weight(1)

    with jax.named_scope("image_wait"):
        @pl.when((core == 0) & ((r != 0) | (z == 0)))
        def _():
            arrived(slot(1), ex_s.at[0], ex_r.at[5])

        @pl.when(core == 0)
        def _():
            send(0, slot(1), slot(2), (ex_s, 8), ex_r.at[6], near(1), lambda: slot(0))
            arrived(slot(2), ex_s.at[0], ex_r.at[6])
            send(0, slot(2), slot(3), (ex_s, 11), ex_r.at[7], near(1), lambda: slot(0))

        @pl.when(core == 1)
        def _():
            arrived(slot(1), ex_s.at[0], ex_r.at[5])
            arrived(slot(2), ex_s.at[0], ex_r.at[6])

        arrived(slot(3), ex_s.at[0], ex_r.at[7])

    with jax.named_scope("text_side"):
        for s in range(S):
            pair[:, pl.ds(s * R, R)] = derivative(dot_nt(tlow[pl.ds(0, R), :], img[pl.ds(s * R, R), :]), s == 0)
        for c0, cw in TILES:
            igrad[:, pl.ds(c0, cw)] = dot(pair[...], img[:, pl.ds(c0, cw)])

        @pl.loop(0, R // 32)
        def _(i):
            rows = pl.ds(pl.multiple_of(i * 32, 32), 32)
            inv = tlen[rows, :]
            gtext[rows, :] = back(igrad[rows, :], traw[rows, :].astype(F32) * inv, inv).astype(BF16)

    with jax.named_scope("final"):
        for k in range(1, ROW):
            source = lax.rem(r + (ROW - k), ROW)

            @pl.when(lax.rem(source, 2) == 1)
            def _():
                arrived(xr.at[source, :, pl.ds(0, COLS[1][1])], xg_s.at[k], xg_r.at[k])

            @pl.when(lax.rem(source, 2) == 0)
            def _():
                arrived(xr.at[source, :, pl.ds(0, COLS[0][1])], xg_s.at[k], xg_r.at[k])

        for c in range(2):
            c0, cw = COLS[c]
            total = xr[c, :, pl.ds(0, cw)]
            for k in range(1, NX):
                total = total + xr[2 * k + c, :, pl.ds(0, cw)]
            gout[:, pl.ds(c0, cw)] = total

    with jax.named_scope("drain"):
        for only, wait in pending:
            if only is None:
                wait()
        groups = {
            0: core == 0, 1: core == 1, "r0": r == 0, "r2": r == 2, "r3": r == 3, "r5": r == 5, "r1z": (r == 1) & (z == 0), "r1n": (r == 1) & (z != 0), "r7": r == ROW - 1, "i0": r == 0,
            "o7": (core == 1) & (r != ROW - 1), "t3": (core == 0) & (r != 0), "t4": (core == 0) & (r > 2),
            "t2": (core == 1) & (r != 1), "i3": i3, "i0e": early, "i7": i7_last, "i6r": (r == 6) & last, "i4r": (r == 4) & last, "i1": (core == 1) & ((r != ROW - 1) | (z != NZ - 1)),
            "i5": r == 5, "i2r": r == 2, "i6": r == ROW - 2,
            "i2": (core == 0) & (r != ROW - 2),
        }
        for group, inside in groups.items():

            @pl.when(inside)
            def _():
                for only, wait in pending:
                    if only == group:
                        wait()


def put_out(gf, gt, gw, gf_out, gt_out, gw_out, sem):
    copies = [pltpu.make_async_copy(a, b, sem.at[i]) for i, (a, b) in enumerate(((gf, gf_out), (gt, gt_out), (gw, gw_out)))]
    for copy in copies:
        copy.start()
    for copy in copies:
        copy.wait()


def on_device(image_features, head_weight, text_embeds, natural_exponent_factor, logit_bias):
    dma = pltpu.SemaphoreType.DMA
    hbm = pl.BlockSpec(memory_space=pltpu.HBM)
    local = pl.BlockSpec(memory_space=pltpu.VMEM)
    scalar = pl.BlockSpec(memory_space=pltpu.SMEM)
    results = pl.pallas_call(
        kernel,
        out_shape=(
            jax.ShapeDtypeStruct((R, D), BF16),
            jax.ShapeDtypeStruct((R, E), BF16),
            jax.ShapeDtypeStruct((SH, E), F32),
        ),
        in_specs=[hbm, hbm, hbm, scalar, scalar],
        out_specs=(local, local, local),
        scratch_shapes=[
            pltpu.VMEM((D, E), BF16),
            pltpu.VMEM((R, D), BF16),
            pltpu.VMEM((R, D), BF16),
            pltpu.VMEM((D, 2 * R), BF16),
            pltpu.VMEM((R, E), F32),
            pltpu.VMEM((R, 1), F32),
            pltpu.VMEM((S * R, E), BF16),
            pltpu.VMEM((R, E), BF16),
            pltpu.VMEM((S * R, E), BF16),
            pltpu.VMEM((R, 1), F32),
            pltpu.VMEM((R, S * R), BF16),
            pltpu.VMEM((2 * R, E), BF16),
            pltpu.VMEM((D, W1), BF16),
            pltpu.VMEM((ROW, SH, E), BF16),
            pltpu.VMEM((BLK, E), F32),
            pltpu.VMEM((36, BLK, W1), BF16),
            pltpu.VMEM((8, BLK, W1), BF16),
            pltpu.VMEM((BLK, W1), F32),
            pltpu.VMEM((ROW, SH, W1), F32),
            pltpu.VMEM((ROW, SH, W1), F32),
            pltpu.VMEM((R, E), F32),
            pltpu.VMEM((R, E), BF16),
            pltpu.VMEM((R, E), BF16),
            dma((3,)),
            dma((ROW,)), dma((ROW,)),
            dma((32,)), dma((32,)),
            dma((32,)), dma((32,)),
            dma((14,)), dma((11,)),
            dma((40,)), dma((36,)),
            dma((ROW,)), dma((ROW,)),
        ],
        compiler_params=pltpu.CompilerParams(
            collective_id=0, has_side_effects=True, vmem_limit_bytes=52 * 1024 * 1024
        ),
    )(image_features, head_weight, text_embeds, natural_exponent_factor, logit_bias)
    return pl.pallas_call(
        put_out,
        out_shape=tuple(jax.ShapeDtypeStruct(a.shape, a.dtype) for a in results),
        in_specs=[local] * 3,
        out_specs=[hbm] * 3,
        scratch_shapes=[dma((3,))],
        compiler_params=pltpu.CompilerParams(vmem_limit_bytes=8 * 1024 * 1024),
    )(*results)


def solution(mesh):
    split = P("blk", None)
    return jax.shard_map(
        on_device,
        mesh=mesh,
        in_specs=(split, split, split, P(), P()),
        out_specs=(split, split, split),
        check_vma=False,
    )
```

```python
import jax
import jax.numpy as jnp
from jax import lax
from jax.experimental import pallas as pl
from jax.experimental.pallas import tpu as pltpu
from jax.sharding import PartitionSpec as P

MESH = pl.DeviceIdType.MESH
D, E, R, S = 1536, 1152, 256, 4
NY, NZ, NX = 4, 8, 4
N = NY * NZ * NX * 2
ROW = NX * 2
SH = D // N
BLK = SH * ROW
YROWS = BLK * NZ
W1 = 640
COLS = ((0, W1), (W1, E - W1))
FAR, NEAR = 5, 0
W2 = 768
RCOLS = ((0, W2), (W2, E - W2))
Y_CORE = 0
EPS = 1e-06
TILES = ((0, 512), (512, 512), (1024, 128))
F32, BF16 = jnp.float32, jnp.bfloat16
Z_ORDER = (4, 3, 5, 2, 6, 1, 7)
Z_ARRIVAL = (0, 1, 7, 2, 6, 3, 5, 4)
ORDER_NT = (((1,), (1,)), ((), ()))


def dot(a, b):
    return jnp.dot(a, b, preferred_element_type=F32)


def dot_nt(a, b):
    return lax.dot_general(a, b, ORDER_NT, preferred_element_type=F32)


def kernel(
    feat_hbm, w_hbm, text_hbm, nef_ref, bias_ref,
    gfeat, gtext, gout,
    w_ref, feat, feat2, feat_t, unit, length, img, traw, tlow, tlen, pair, eg,
    gpart, xbuf, wrow, rbuf, sbuf, xrow, xs, xr, igrad, cross, cross2,
    in_sem, xw_s, xw_r, ag_s, ag_r, dd_s, dd_r, ex_s, ex_r, rs_s, rs_r, xg_s, xg_r,
):
    me = lax.axis_index("blk")
    core = lax.rem(me, 2)
    r = lax.rem(me, ROW)
    z = lax.rem(lax.div(me, ROW), NZ)
    y = lax.div(me, ROW * NZ)
    pending = []

    row_y = [lax.rem(y + j, NY) for j in range(NY)]
    row_z = [lax.rem(z + k, NZ) for k in range(NZ)]
    dev_y = [v * (NZ * ROW) for v in row_y]
    dev_z = [v * ROW + r for v in row_z]
    at_y = [v * YROWS for v in row_y]
    at_z = [v * BLK for v in row_z]

    def dev(dy=0, dz=0):
        return dev_y[dy % NY] + dev_z[dz % NZ]

    wrap = 1 - lax.div(z + (NZ - 1), NZ)
    first = me - r
    pre_row = first + wrap * (dev_y[NY - 1] - dev_y[0])
    below_row = dev(0, -1) - r

    def row_dev(k):
        return me - r + lax.rem(r + k, ROW)

    def near(k):
        return lax.rem(me + (k + N), N)

    def remote(src, dst, ss, rs, to):
        return pltpu.make_async_remote_copy(
            src_ref=src, dst_ref=dst, send_sem=ss, recv_sem=rs, device_id=(to,), device_id_type=MESH
        )

    def send(only, src, dst, ss, rs, to, like=None):
        sems, i = ss
        remote(src, dst, sems.at[i], rs, to).start()

        def wait():
            ref = src if like is None else like()
            remote(ref, ref, sems.at[i], sems.at[i], near(1)).wait_send()

        pending.append((only, wait))

    def arrived(dst, ss, rs):
        remote(dst, dst, ss, rs, near(1)).wait_recv()

    def wblock(ref, dy, dz, c0, cw):
        start = pl.multiple_of(at_y[dy % NY] + at_z[dz % NZ], 8)
        return ref.at[pl.ds(start, BLK), pl.ds(c0, cw)]

    def transpose(src, col):
        if col:
            arrived(feat2, ex_s.at[12], ex_r.at[0])

        @pl.loop(0, D // 256)
        def _(i):
            cols = pl.ds(pl.multiple_of(i * 256, 256), 256)
            feat_t[cols, pl.ds(col, R)] = jnp.transpose(src[:, cols])

    def tslot(k):
        return tlow.at[pl.ds(k * R, R), :]

    def slot(k):
        return img.at[pl.ds(k * R, R), :]

    cp_w = pltpu.make_async_copy(w_hbm, xbuf.at[r], in_sem.at[0])
    cp_t = pltpu.make_async_copy(text_hbm, traw, in_sem.at[1])
    cp_f = pltpu.make_async_copy(feat_hbm, feat, in_sem.at[2])
    cp_w.start()
    cp_t.start()
    cp_f.start()

    with jax.named_scope("barrier"):
        barrier = pltpu.get_barrier_semaphore()
        peers = [row_dev(k) for k in range(1, ROW)] + [dev(dz=k) for k in range(1, NZ)]
        peers += [dev(d) - r + lax.rem(r + d * -k + ROW, ROW) for d in (-1, 1) for k in (1, 3, 7)]
        peers += [dev(0, d) - r + lax.rem(r + d * -k + ROW, ROW) for d in (-1, 1) for k in (2, 6)]
        peers += [dev(dy=k) for k in range(1, NY)] + [near(k) for k in (-ROW, -5, -3, -2, -1, 1, 2, 3, 5, ROW)]
        for peer in peers:
            pl.semaphore_signal(barrier, inc=1, device_id=(peer,), device_id_type=MESH)
        pl.semaphore_wait(barrier, len(peers))

    with jax.named_scope("w_row_send"):
        cp_w.wait()
        for k in (4, 3, 5, 2, 6, 1, 7):
            send(None, xbuf.at[r], xbuf.at[r], (xw_s, k), xw_r.at[k], row_dev(k), lambda: xbuf.at[0])

    with jax.named_scope("own_text"):
        cp_t.wait()

        @pl.loop(0, R // 32, unroll=2)
        def _(i):
            rows = pl.ds(pl.multiple_of(i * 32, 32), 32)
            t = traw[rows, :].astype(F32)
            inv = 1.0 / jnp.sqrt(jnp.sum(t * t, axis=1, keepdims=True) + EPS)
            tlow[rows, :] = (t * inv).astype(BF16)
            tlen[rows, :] = inv

        cp_f.wait()
        send(None, feat, feat2, (ex_s, 12), ex_r.at[0], me + 1 - 2 * core)
        transpose(feat, 0)

    with jax.named_scope("w_row"):
        for k in range(1, ROW):
            arrived(xbuf.at[lax.rem(r + (ROW - k), ROW)], xw_s.at[k], xw_r.at[k])
        for k in range(ROW):
            wrow[pl.ds(SH * k, SH), :] = xbuf[k].astype(F32)
        own = pl.multiple_of(y * YROWS + z * BLK, 8)
        w_ref[pl.ds(own, BLK), :] = wrow[...].astype(BF16)

    with jax.named_scope("text_send"):
        @pl.when((core == 0) & (r != 0))
        def _():
            send("t3", tslot(0), tslot(1), (ex_s, 0), ex_r.at[1], near(-1), lambda: tslot(0))

        @pl.when((core == 0) & (r > 2))
        def _():
            send("t4", tslot(0), tslot(3), (ex_s, 1), ex_r.at[3], near(-3), lambda: tslot(0))

        @pl.when(core == 1)
        def _():
            send(1, tslot(0), tslot(1), (ex_s, 0), ex_r.at[1], near(-1), lambda: tslot(0))

        @pl.when((core == 1) & (r != 1))
        def _():
            send("t2", tslot(0), tslot(2), (ex_s, 1), ex_r.at[2], near(-2), lambda: tslot(0))

        @pl.when(r == 0)
        def _():
            send("r0", tslot(0), cross, (ex_s, 0), ex_r.at[8], pre_row + 7, lambda: tslot(0))
            send("r0", tslot(0), cross, (ex_s, 1), ex_r.at[8], pre_row + 3, lambda: tslot(0))

        @pl.when(r == 2)
        def _():
            send("r2", tslot(0), cross, (ex_s, 1), ex_r.at[8], pre_row + 5, lambda: tslot(0))


    def gather(c):
        c0, cw = COLS[c]
        sibling = me + (1 - 2 * c)
        count = [0]
        like = lambda: w_ref.at[pl.ds(0, BLK), pl.ds(c0, cw)]

        def put(j, k, dy, dz):
            part = wblock(w_ref, -j, -k, c0, cw)
            idx = ((j + dy) % NY) * NZ + (k + dz) % NZ
            send(c, part, part, (ag_s, count[0]), ag_r.at[idx], dev(dy, dz), like)
            count[0] += 1

        def share(j, k):
            part = wblock(w_ref, -j, -k, c0, cw)
            send(c, part, part, (dd_s, j * NZ + k), dd_r.at[j * NZ + k], sibling, like)

        def got(j, k):
            part = wblock(w_ref, -j, -k, c0, cw)
            arrived(part, ag_s.at[0], ag_r.at[j * NZ + k])
            return part

        if c == Y_CORE:
            for k in Z_ARRIVAL[1:]:
                put(0, 0, 0, k)
            transpose(feat2, R)

            def stage1(i):
                k = Z_ARRIVAL[i]
                if k:
                    got(0, k)
                put(0, k, 1, 0)
                put(0, k, -1, 0)
                if i >= FAR:
                    put(0, k, 2, 0)
                if k:
                    share(0, k)

            def stage2(i):
                k = Z_ARRIVAL[i]
                got(1, k)
                if i < FAR and i % 2 == 0:
                    put(1, k, 1, 0)
                share(1, k)
                got(3, k)
                if i < FAR and i % 2 == 1:
                    put(3, k, -1, 0)
                share(3, k)

            def stage3(i):
                k = Z_ARRIVAL[i]
                got(2, k)
                share(2, k)

            for i in range(NZ + 4):
                if i < NZ:
                    stage1(i)
                if 2 <= i < NZ + 2:
                    stage2(i - 2)
                if 4 <= i:
                    stage3(i - 4)
        else:
            for j in (1, 3, 2):
                put(0, 0, j, 0)

            @pl.when((r == 1) & (z == 0))
            def _():
                send("r1z", tslot(0), cross, (ex_s, 1), ex_r.at[8], pre_row + 1, lambda: tslot(0))

            for j in (0, 1, 3, 2):
                if j:
                    got(j, 0)
                put(j, 0, 0, 1)
                put(j, 0, 0, -1)
                if j == 0:
                    transpose(feat2, R)
                if j:
                    share(j, 0)
            for h in (1, 2, 3):
                for j in (0, 1, 3, 2):
                    got(j, h)
                    put(j, h, 0, 1)
                    share(j, h)
                    got(j, NZ - h)
                    if h < 3:
                        put(j, NZ - h, 0, -1)
                    share(j, NZ - h)
                if h == 3:

                    @pl.when((r > 1) | (z == 0))
                    def _():
                        arrived(cross, ex_s.at[0], ex_r.at[8])

                    @pl.when((r == 1) & (z == 0))
                    def _():
                        send("r1z", cross, tslot(2), (ex_s, 2), ex_r.at[2], below_row + 7, lambda: tslot(0))

                    @pl.when((r == 1) & (z != 0))
                    def _():
                        send("r1n", tslot(0), tslot(2), (ex_s, 1), ex_r.at[2], below_row + 7, lambda: tslot(0))

                    @pl.when(r == 3)
                    def _():
                        send("r3", cross, tslot(3), (ex_s, 2), ex_r.at[3], below_row + 5, lambda: tslot(0))

                    @pl.when(r == 5)
                    def _():
                        send("r5", cross, tslot(3), (ex_s, 2), ex_r.at[3], below_row + 7, lambda: tslot(0))

                    @pl.when(r == 7)
                    def _():
                        send("r7", cross, tslot(1), (ex_s, 2), ex_r.at[1], below_row + 7, lambda: tslot(0))

            for j in (0, 1, 3, 2):
                got(j, 4)
                share(j, 4)
            @pl.when(r != ROW - 1)
            def _():
                arrived(tslot(1), ex_s.at[0], ex_r.at[1])
                send("o7", tslot(1), tslot(2), (ex_s, 3), ex_r.at[2], near(-1), lambda: tslot(0))
                arrived(tslot(2), ex_s.at[0], ex_r.at[2])
                send("o7", tslot(2), tslot(3), (ex_s, 10), ex_r.at[3], near(-1), lambda: tslot(0))

        o0, ow = COLS[1 - c]
        for j in range(NY):
            for k in range(NZ):
                if j or k:
                    part = wblock(w_ref, -j, -k, o0, ow)
                    arrived(part, dd_s.at[0], dd_r.at[j * NZ + k])

    with jax.named_scope("gather"):
        @pl.when(core == 0)
        def _():
            gather(0)

        @pl.when(core == 1)
        def _():
            gather(1)

    with jax.named_scope("embed"):
        for c0, cw in TILES:
            unit[:, pl.ds(c0, cw)] = dot(feat[...], w_ref[:, pl.ds(c0, cw)])

        @pl.loop(0, R // 32, unroll=2)
        def _(i):
            rows = pl.ds(pl.multiple_of(i * 32, 32), 32)
            e = unit[rows, :]
            inv = 1.0 / jnp.sqrt(jnp.sum(e * e, axis=1, keepdims=True) + EPS)
            u = e * inv
            unit[rows, :] = u
            length[rows, :] = inv
            img[rows, :] = u.astype(BF16)

    @pl.when(r == ROW - 1)
    def _():
        arrived(tslot(1), ex_s.at[0], ex_r.at[1])
        send("r7", tslot(1), tslot(2), (ex_s, 3), ex_r.at[2], near(-1), lambda: tslot(0))
        arrived(tslot(2), ex_s.at[0], ex_r.at[2])
        send("r7", tslot(2), tslot(3), (ex_s, 10), ex_r.at[3], near(-1), lambda: tslot(0))

    with jax.named_scope("image_send"):
        i3 = (core == 1) & (r != ROW - 1) & (r != 5)
        last = z == NZ - 1
        i7_last = (r == ROW - 1) & last

        @pl.when(i7_last)
        def _():
            send("i7", slot(0), cross2, (ex_s, 5), ex_r.at[9], dev(1) - 1, lambda: slot(0))
            send("i7", slot(0), cross2, (ex_s, 6), ex_r.at[9], dev(1) - 3, lambda: slot(0))

        early = (r == 0) & (z != 0)

        @pl.when(r == 5)
        def _():
            send("i5", slot(0), cross2, (ex_s, 6), ex_r.at[9], near(5), lambda: slot(0))

        i5_early = (core == 1) & (r != ROW - 1) & ((r != 5) | (z != NZ - 1))

        @pl.when((core == 1) & ((r != ROW - 1) | (z != NZ - 1)))
        def _():
            send("i1", slot(0), slot(1), (ex_s, 5), ex_r.at[5], near(1), lambda: slot(0))

        @pl.when(i3)
        def _():
            send("i3", slot(0), slot(3), (ex_s, 6), ex_r.at[7], near(3), lambda: slot(0))

        @pl.when(core == 0)
        def _():
            send(0, slot(0), slot(1), (ex_s, 5), ex_r.at[5], near(1), lambda: slot(0))

        @pl.when((core == 0) & (r != ROW - 2))
        def _():
            send("i2", slot(0), slot(2), (ex_s, 6), ex_r.at[6], near(2), lambda: slot(0))

    factor = jnp.exp(jnp.full((1, R), nef_ref[0], F32))
    bias = bias_ref[0]

    def derivative(logit_dot, diagonal):
        logits = factor * logit_dot + bias
        if diagonal:
            same = lax.broadcasted_iota(jnp.int32, (R, R), 0) == lax.broadcasted_iota(jnp.int32, (R, R), 1)
            label = jnp.where(same, 1.0, -1.0).astype(F32)
            g = -factor * label / (1.0 + jnp.exp(label * logits))
        else:
            g = factor / (1.0 + jnp.exp(-logits))
        return g.astype(BF16)

    def back(grad, u, inv):
        return (grad - u * jnp.sum(u * grad, axis=1, keepdims=True)) * inv

    with jax.named_scope("image_side"):
        for s in range(S):
            if s == 1:

                @pl.when(core == 0)
                def _():
                    arrived(tslot(1), ex_s.at[0], ex_r.at[1])
                    arrived(tslot(2), ex_s.at[0], ex_r.at[2])

            if s == 3:
                with jax.named_scope("text_wait"):
                    arrived(tslot(3), ex_s.at[0], ex_r.at[3])
            pair[:, pl.ds(s * R, R)] = derivative(dot_nt(img[pl.ds(0, R), :], tlow[pl.ds(s * R, R), :]), s == 0)
        for c0, cw in TILES:
            igrad[:, pl.ds(c0, cw)] = dot(pair[...], tlow[:, pl.ds(c0, cw)])

        @pl.loop(0, R // 32, unroll=2)
        def _(i):
            rows = pl.ds(pl.multiple_of(i * 32, 32), 32)
            eg[rows, :] = back(igrad[rows, :], unit[rows, :], length[rows, :]).astype(BF16)

    with jax.named_scope("eg_send"):
        @pl.when(core == 0)
        def _():
            part = pl.ds(RCOLS[1][0], RCOLS[1][1])
            send(0, eg.at[pl.ds(0, R), part], eg.at[pl.ds(R, R), part], (ex_s, 9), ex_r.at[10], me + 1, lambda: eg.at[pl.ds(0, R), pl.ds(RCOLS[1][0], RCOLS[1][1])])

        @pl.when(core == 1)
        def _():
            part = pl.ds(RCOLS[0][0], RCOLS[0][1])
            send(1, eg.at[pl.ds(0, R), part], eg.at[pl.ds(R, R), part], (ex_s, 9), ex_r.at[10], me - 1, lambda: eg.at[pl.ds(0, R), pl.ds(RCOLS[0][0], RCOLS[0][1])])

    def feature_gradient(i):
        cols = pl.ds(i * 512, 512)
        gfeat[:, cols] = dot_nt(eg[pl.ds(0, R), :], w_ref[cols, :]).astype(BF16)

    with jax.named_scope("feat_grad"):
        feature_gradient(0)
        feature_gradient(1)

    def reduce_weight(c):
        c0, cw = RCOLS[c]
        count = [0]
        arrived(eg.at[pl.ds(R, R), pl.ds(c0, cw)], ex_s.at[0], ex_r.at[10])

        def product(j):
            rows = pl.ds(pl.multiple_of(at_y[j], 8), YROWS)
            gpart[rows, pl.ds(0, cw)] = dot(feat_t[rows, :], eg[:, pl.ds(c0, cw)]).astype(BF16)

        def mine(dy, dz):
            return wblock(gpart, dy, dz, 0, cw)

        def buf(i):
            return rbuf.at[i, :, pl.ds(0, cw)]

        def emit(src, i, dy, dz):
            send(c, src, buf(i), (rs_s, count[0]), rs_r.at[i], dev(dy, dz), lambda: buf(0))
            count[0] += 1

        def take(i):
            arrived(buf(i), rs_s.at[0], rs_r.at[i])
            return buf(i)[...].astype(F32)

        if c == Y_CORE:
            product(2)

            @pl.when(r == ROW - 2)
            def _():
                send("i6", slot(0), cross2, (ex_s, 6), ex_r.at[9], first, lambda: slot(0))

            for i, k in enumerate(Z_ORDER + (0,)):
                emit(mine(2, k), k, 2 if i < NEAR else 1 if i % 2 == 0 else -1, 0)
            product(1)
            product(3)
            product(0)
            feature_gradient(2)
            for i, k in enumerate(Z_ORDER + (0,)):
                step = 1 if i % 2 == 0 else -1
                part = mine(step, k)
                other = mine(-step, k)
                emit(other, 8 + k if step == -1 else 16 + k, -step, 0)
                if i >= NEAR:
                    part[...] = (part[...].astype(F32) + take(k)).astype(BF16)
                emit(part, 8 + k if step == 1 else 16 + k, step, 0)
            @pl.when(r == 2)
            def _():
                arrived(cross2, ex_s.at[0], ex_r.at[9])
                send("i2r", cross2, slot(3), (ex_s, 13), ex_r.at[7], first, lambda: slot(0))

            for i, k in enumerate(Z_ORDER + (0,)):
                total = mine(0, k)[...].astype(F32) + take(8 + k) + take(16 + k)
                if i < NEAR:
                    total = total + take(k)
                if k:
                    sbuf[k, :, pl.ds(0, cw)] = total.astype(BF16)
                    emit(sbuf.at[k, :, pl.ds(0, cw)], 24 + k, 0, k)
            @pl.when(r == 0)
            def _():
                arrived(cross2, ex_s.at[0], ex_r.at[9])
                send("i0", cross2, slot(2), (ex_s, 13), ex_r.at[6], near(ROW), lambda: slot(0))

            @pl.when(((r == 4) | (r == 6)) & last)
            def _():
                arrived(cross2, ex_s.at[0], ex_r.at[9])

            @pl.when((r == 6) & last)
            def _():
                send("i6r", cross2, slot(1), (ex_s, 13), ex_r.at[5], dev(0, 1) - r, lambda: slot(0))

            @pl.when((r == 4) & last)
            def _():
                send("i4r", cross2, slot(3), (ex_s, 13), ex_r.at[7], dev(0, 1) - r + 2, lambda: slot(0))

            @pl.when(early)
            def _():
                arrived(slot(1), ex_s.at[0], ex_r.at[5])
                send("i0e", slot(1), slot(3), (ex_s, 7), ex_r.at[7], near(2), lambda: slot(0))

            for k in Z_ARRIVAL[1:]:
                total = total + take(24 + k)
        else:
            for j in range(NY):
                product(j)
            order = (2, 1, 3, 0)
            for j in order:
                emit(mine(j, 4), 16 + j, 0, -1)
            feature_gradient(2)
            for h in (3, 2, 1):
                s = 3 - h
                for j in order:
                    for sign, base in ((1, 0), (-1, 16)):
                        part = mine(j, sign * h)
                        if s or sign == -1:
                            part[...] = (part[...].astype(F32) + take(base + 4 * s + j)).astype(BF16)
                        emit(part, base + 4 * (s + 1) + j, 0, sign)
            for j in order:
                total = mine(j, 0)[...].astype(F32) + take(12 + j) + take(28 + j)
                if j:
                    sbuf[j, :, pl.ds(0, cw)] = total.astype(BF16)
                    emit(sbuf.at[j, :, pl.ds(0, cw)], 32 + j, j, 0)
            for j in (1, 3, 2):
                total = total + take(32 + j)

        xrow[:, pl.ds(0, cw)] = total
        for k in range(ROW):
            xs[k, :, pl.ds(0, cw)] = xrow[pl.ds(SH * k, SH), pl.ds(0, cw)]
        for k in (4, 3, 5, 2, 6, 1, 7):
            send(
                c, xs.at[lax.rem(r + k, ROW), :, pl.ds(0, cw)], xr.at[r, :, pl.ds(0, cw)],
                (xg_s, k), xg_r.at[k], row_dev(k), lambda: xs.at[0, :, pl.ds(0, cw)],
            )
        xr[r, :, pl.ds(0, cw)] = xs[r, :, pl.ds(0, cw)]

    with jax.named_scope("reduce"):
        @pl.when(core == 0)
        def _():
            reduce_weight(0)

        @pl.when(core == 1)
        def _():
            reduce_weight(1)

    def similarities(s):
        pair[:, pl.ds(s * R, R)] = derivative(dot_nt(tlow[pl.ds(0, R), :], img[pl.ds(s * R, R), :]), s == 0)

    with jax.named_scope("image_wait"):
        @pl.when((core == 0) & ((r != 0) | (z == 0)))
        def _():
            arrived(slot(1), ex_s.at[0], ex_r.at[5])

        @pl.when(core == 0)
        def _():
            send(0, slot(1), slot(2), (ex_s, 8), ex_r.at[6], near(1), lambda: slot(0))

        @pl.when((core == 0) & (r != 0))
        def _():
            arrived(slot(2), ex_s.at[0], ex_r.at[6])
            send("s2", slot(2), slot(3), (ex_s, 11), ex_r.at[7], near(1), lambda: slot(0))

        @pl.when(core == 1)
        def _():
            arrived(slot(1), ex_s.at[0], ex_r.at[5])

        for s in range(2):
            similarities(s)
        for c0, cw in TILES:
            igrad[:, pl.ds(c0, cw)] = dot(pair[:, pl.ds(0, 2 * R)], img[pl.ds(0, 2 * R), pl.ds(c0, cw)])

        @pl.when(r == 0)
        def _():
            arrived(slot(2), ex_s.at[0], ex_r.at[6])
            send("s0", slot(2), slot(3), (ex_s, 11), ex_r.at[7], near(1), lambda: slot(0))

        @pl.when(core == 1)
        def _():
            arrived(slot(2), ex_s.at[0], ex_r.at[6])

        similarities(2)
        arrived(slot(3), ex_s.at[0], ex_r.at[7])

    with jax.named_scope("text_side"):
        similarities(3)
        for c0, cw in TILES:
            igrad[:, pl.ds(c0, cw)] += dot(pair[:, pl.ds(2 * R, 2 * R)], img[pl.ds(2 * R, 2 * R), pl.ds(c0, cw)])

        @pl.loop(0, R // 32, unroll=2)
        def _(i):
            rows = pl.ds(pl.multiple_of(i * 32, 32), 32)
            inv = tlen[rows, :]
            gtext[rows, :] = back(igrad[rows, :], traw[rows, :].astype(F32) * inv, inv).astype(BF16)

    with jax.named_scope("final"):
        for k in range(1, ROW):
            source = lax.rem(r + (ROW - k), ROW)

            @pl.when(lax.rem(source, 2) == 1)
            def _():
                arrived(xr.at[source, :, pl.ds(0, RCOLS[1][1])], xg_s.at[k], xg_r.at[k])

            @pl.when(lax.rem(source, 2) == 0)
            def _():
                arrived(xr.at[source, :, pl.ds(0, RCOLS[0][1])], xg_s.at[k], xg_r.at[k])

        for c in range(2):
            c0, cw = RCOLS[c]
            total = xr[c, :, pl.ds(0, cw)]
            for k in range(1, NX):
                total = total + xr[2 * k + c, :, pl.ds(0, cw)]
            gout[:, pl.ds(c0, cw)] = total

    with jax.named_scope("drain"):
        for only, wait in pending:
            if only is None:
                wait()
        groups = {
            0: core == 0, 1: core == 1, "r0": r == 0, "r2": r == 2, "r3": r == 3, "r5": r == 5, "r1z": (r == 1) & (z == 0), "r1n": (r == 1) & (z != 0), "r7": r == ROW - 1, "i0": r == 0,
            "o7": (core == 1) & (r != ROW - 1), "t3": (core == 0) & (r != 0), "t4": (core == 0) & (r > 2),
            "t2": (core == 1) & (r != 1), "i3": i3, "s0": r == 0, "s2": (core == 0) & (r != 0), "i0e": early, "i7": i7_last, "i6r": (r == 6) & last, "i4r": (r == 4) & last, "i1": (core == 1) & ((r != ROW - 1) | (z != NZ - 1)),
            "i5": r == 5, "i2r": r == 2, "i6": r == ROW - 2,
            "i2": (core == 0) & (r != ROW - 2),
        }
        for group, inside in groups.items():

            @pl.when(inside)
            def _():
                for only, wait in pending:
                    if only == group:
                        wait()


def put_out(gf, gt, gw, gf_out, gt_out, gw_out, sem):
    copies = [pltpu.make_async_copy(a, b, sem.at[i]) for i, (a, b) in enumerate(((gf, gf_out), (gt, gt_out), (gw, gw_out)))]
    for copy in copies:
        copy.start()
    for copy in copies:
        copy.wait()


def on_device(image_features, head_weight, text_embeds, natural_exponent_factor, logit_bias):
    dma = pltpu.SemaphoreType.DMA
    hbm = pl.BlockSpec(memory_space=pltpu.HBM)
    local = pl.BlockSpec(memory_space=pltpu.VMEM)
    scalar = pl.BlockSpec(memory_space=pltpu.SMEM)
    results = pl.pallas_call(
        kernel,
        out_shape=(
            jax.ShapeDtypeStruct((R, D), BF16),
            jax.ShapeDtypeStruct((R, E), BF16),
            jax.ShapeDtypeStruct((SH, E), F32),
        ),
        in_specs=[hbm, hbm, hbm, scalar, scalar],
        out_specs=(local, local, local),
        scratch_shapes=[
            pltpu.VMEM((D, E), BF16),
            pltpu.VMEM((R, D), BF16),
            pltpu.VMEM((R, D), BF16),
            pltpu.VMEM((D, 2 * R), BF16),
            pltpu.VMEM((R, E), F32),
            pltpu.VMEM((R, 1), F32),
            pltpu.VMEM((S * R, E), BF16),
            pltpu.VMEM((R, E), BF16),
            pltpu.VMEM((S * R, E), BF16),
            pltpu.VMEM((R, 1), F32),
            pltpu.VMEM((R, S * R), BF16),
            pltpu.VMEM((2 * R, E), BF16),
            pltpu.VMEM((D, W2), BF16),
            pltpu.VMEM((ROW, SH, E), BF16),
            pltpu.VMEM((BLK, E), F32),
            pltpu.VMEM((36, BLK, W2), BF16),
            pltpu.VMEM((8, BLK, W2), BF16),
            pltpu.VMEM((BLK, W2), F32),
            pltpu.VMEM((ROW, SH, W2), F32),
            pltpu.VMEM((ROW, SH, W2), F32),
            pltpu.VMEM((R, E), F32),
            pltpu.VMEM((R, E), BF16),
            pltpu.VMEM((R, E), BF16),
            dma((3,)),
            dma((ROW,)), dma((ROW,)),
            dma((32,)), dma((32,)),
            dma((32,)), dma((32,)),
            dma((14,)), dma((11,)),
            dma((40,)), dma((36,)),
            dma((ROW,)), dma((ROW,)),
        ],
        compiler_params=pltpu.CompilerParams(
            collective_id=0, has_side_effects=True, vmem_limit_bytes=52 * 1024 * 1024
        ),
    )(image_features, head_weight, text_embeds, natural_exponent_factor, logit_bias)
    return pl.pallas_call(
        put_out,
        out_shape=tuple(jax.ShapeDtypeStruct(a.shape, a.dtype) for a in results),
        in_specs=[local] * 3,
        out_specs=[hbm] * 3,
        scratch_shapes=[dma((3,))],
        compiler_params=pltpu.CompilerParams(vmem_limit_bytes=8 * 1024 * 1024),
    )(*results)


def solution(mesh):
    split = P("blk", None)
    return jax.shard_map(
        on_device,
        mesh=mesh,
        in_specs=(split, split, split, P(), P()),
        out_specs=(split, split, split),
        check_vma=False,
    )
```

```python
import jax
import jax.numpy as jnp
from jax import lax
from jax.experimental import pallas as pl
from jax.experimental.pallas import tpu as pltpu
from jax.sharding import PartitionSpec as P

MESH = pl.DeviceIdType.MESH
D, E, R, S = 1536, 1152, 256, 4
NY, NZ, NX = 4, 8, 4
N = NY * NZ * NX * 2
ROW = NX * 2
SH = D // N
BLK = SH * ROW
YROWS = BLK * NZ
W1 = 640
COLS = ((0, W1), (W1, E - W1))
FAR, NEAR = 5, 0
W2 = 768
RCOLS = ((0, W2), (W2, E - W2))
Y_CORE = 0
EPS = 1e-06
TILES = ((0, 512), (512, 512), (1024, 128))
F32, BF16 = jnp.float32, jnp.bfloat16
Z_ORDER = (4, 3, 5, 2, 6, 1, 7)
Z_ARRIVAL = (0, 1, 7, 2, 6, 3, 5, 4)
ORDER_NT = (((1,), (1,)), ((), ()))


def dot(a, b):
    return jnp.dot(a, b, preferred_element_type=F32)


def dot_nt(a, b):
    return lax.dot_general(a, b, ORDER_NT, preferred_element_type=F32)


def kernel(
    feat_hbm, w_hbm, text_hbm, nef_ref, bias_ref,
    gfeat, gtext, gout,
    w_ref, feat, feat2, feat_t, unit, length, img, traw, tlow, tlen, pair, eg,
    gpart, xbuf, wrow, rbuf, sbuf, xrow, xs, xr, igrad, cross, cross2,
    in_sem, xw_s, xw_r, ag_s, ag_r, dd_s, dd_r, ex_s, ex_r, rs_s, rs_r, xg_s, xg_r,
):
    me = lax.axis_index("blk")
    core = lax.rem(me, 2)
    r = lax.rem(me, ROW)
    z = lax.rem(lax.div(me, ROW), NZ)
    y = lax.div(me, ROW * NZ)
    pending = []

    row_y = [lax.rem(y + j, NY) for j in range(NY)]
    row_z = [lax.rem(z + k, NZ) for k in range(NZ)]
    dev_y = [v * (NZ * ROW) for v in row_y]
    dev_z = [v * ROW + r for v in row_z]
    at_y = [v * YROWS for v in row_y]
    at_z = [v * BLK for v in row_z]

    def dev(dy=0, dz=0):
        return dev_y[dy % NY] + dev_z[dz % NZ]

    wrap = 1 - lax.div(z + (NZ - 1), NZ)
    first = me - r
    pre_row = first + wrap * (dev_y[NY - 1] - dev_y[0])
    below_row = dev(0, -1) - r

    def row_dev(k):
        return me - r + lax.rem(r + k, ROW)

    def near(k):
        return lax.rem(me + (k + N), N)

    def remote(src, dst, ss, rs, to):
        return pltpu.make_async_remote_copy(
            src_ref=src, dst_ref=dst, send_sem=ss, recv_sem=rs, device_id=(to,), device_id_type=MESH
        )

    def send(only, src, dst, ss, rs, to, like=None):
        sems, i = ss
        remote(src, dst, sems.at[i], rs, to).start()

        def wait():
            ref = src if like is None else like()
            remote(ref, ref, sems.at[i], sems.at[i], near(1)).wait_send()

        pending.append((only, wait))

    def arrived(dst, ss, rs):
        remote(dst, dst, ss, rs, near(1)).wait_recv()

    def wblock(ref, dy, dz, c0, cw):
        start = pl.multiple_of(at_y[dy % NY] + at_z[dz % NZ], 8)
        return ref.at[pl.ds(start, BLK), pl.ds(c0, cw)]

    def transpose(src, col):
        if col:
            arrived(feat2, ex_s.at[12], ex_r.at[0])

        @pl.loop(0, D // 256)
        def _(i):
            cols = pl.ds(pl.multiple_of(i * 256, 256), 256)
            feat_t[cols, pl.ds(col, R)] = jnp.transpose(src[:, cols])

    def tslot(k):
        return tlow.at[pl.ds(k * R, R), :]

    def slot(k):
        return img.at[pl.ds(k * R, R), :]

    cp_w = pltpu.make_async_copy(w_hbm, xbuf.at[r], in_sem.at[0])
    cp_t = pltpu.make_async_copy(text_hbm, traw, in_sem.at[1])
    cp_f = pltpu.make_async_copy(feat_hbm, feat, in_sem.at[2])
    cp_w.start()
    cp_t.start()
    cp_f.start()

    with jax.named_scope("barrier"):
        barrier = pltpu.get_barrier_semaphore()
        peers = [row_dev(k) for k in range(1, ROW)] + [dev(dz=k) for k in range(1, NZ)]
        peers += [dev(d) - r + lax.rem(r + d * -k + ROW, ROW) for d in (-1, 1) for k in (1, 3, 7)]
        peers += [dev(0, d) - r + lax.rem(r + d * -k + ROW, ROW) for d in (-1, 1) for k in (2, 6)]
        peers += [dev(dy=k) for k in range(1, NY)] + [near(k) for k in (-ROW, -5, -3, -2, -1, 1, 2, 3, 5, ROW)]
        for peer in peers:
            pl.semaphore_signal(barrier, inc=1, device_id=(peer,), device_id_type=MESH)
        pl.semaphore_wait(barrier, len(peers))

    with jax.named_scope("w_row_send"):
        cp_w.wait()
        for k in (4, 3, 5, 2, 6, 1, 7):
            send(None, xbuf.at[r], xbuf.at[r], (xw_s, k), xw_r.at[k], row_dev(k), lambda: xbuf.at[0])

    with jax.named_scope("own_text"):
        cp_t.wait()

        @pl.loop(0, R // 32, unroll=2)
        def _(i):
            rows = pl.ds(pl.multiple_of(i * 32, 32), 32)
            t = traw[rows, :].astype(F32)
            inv = 1.0 / jnp.sqrt(jnp.sum(t * t, axis=1, keepdims=True) + EPS)
            tlow[rows, :] = (t * inv).astype(BF16)
            tlen[rows, :] = inv

        cp_f.wait()
        send(None, feat, feat2, (ex_s, 12), ex_r.at[0], me + 1 - 2 * core)
        transpose(feat, 0)

    with jax.named_scope("w_row"):
        for k in range(1, ROW):
            arrived(xbuf.at[lax.rem(r + (ROW - k), ROW)], xw_s.at[k], xw_r.at[k])
        for k in range(ROW):
            wrow[pl.ds(SH * k, SH), :] = xbuf[k].astype(F32)
        own = pl.multiple_of(y * YROWS + z * BLK, 8)
        w_ref[pl.ds(own, BLK), :] = wrow[...].astype(BF16)

    with jax.named_scope("text_send"):
        @pl.when((core == 0) & (r != 0))
        def _():
            send("t3", tslot(0), tslot(1), (ex_s, 0), ex_r.at[1], near(-1), lambda: tslot(0))

        @pl.when((core == 0) & (r > 2))
        def _():
            send("t4", tslot(0), tslot(3), (ex_s, 1), ex_r.at[3], near(-3), lambda: tslot(0))

        @pl.when(core == 1)
        def _():
            send(1, tslot(0), tslot(1), (ex_s, 0), ex_r.at[1], near(-1), lambda: tslot(0))

        @pl.when((core == 1) & (r != 1))
        def _():
            send("t2", tslot(0), tslot(2), (ex_s, 1), ex_r.at[2], near(-2), lambda: tslot(0))

        @pl.when(r == 0)
        def _():
            send("r0", tslot(0), cross, (ex_s, 0), ex_r.at[8], pre_row + 7, lambda: tslot(0))
            send("r0", tslot(0), cross, (ex_s, 1), ex_r.at[8], pre_row + 3, lambda: tslot(0))

        @pl.when(r == 2)
        def _():
            send("r2", tslot(0), cross, (ex_s, 1), ex_r.at[8], pre_row + 5, lambda: tslot(0))


    def gather(c):
        c0, cw = COLS[c]
        sibling = me + (1 - 2 * c)
        count = [0]
        like = lambda: w_ref.at[pl.ds(0, BLK), pl.ds(c0, cw)]

        def put(j, k, dy, dz):
            part = wblock(w_ref, -j, -k, c0, cw)
            idx = ((j + dy) % NY) * NZ + (k + dz) % NZ
            send(c, part, part, (ag_s, count[0]), ag_r.at[idx], dev(dy, dz), like)
            count[0] += 1

        def share(j, k):
            part = wblock(w_ref, -j, -k, c0, cw)
            send(c, part, part, (dd_s, j * NZ + k), dd_r.at[j * NZ + k], sibling, like)

        def got(j, k):
            part = wblock(w_ref, -j, -k, c0, cw)
            arrived(part, ag_s.at[0], ag_r.at[j * NZ + k])
            return part

        if c == Y_CORE:
            for k in Z_ARRIVAL[1:]:
                put(0, 0, 0, k)
            transpose(feat2, R)

            def stage1(i):
                k = Z_ARRIVAL[i]
                if k:
                    got(0, k)
                put(0, k, 1, 0)
                put(0, k, -1, 0)
                if i >= FAR:
                    put(0, k, 2, 0)
                if k:
                    share(0, k)

            def stage2(i):
                k = Z_ARRIVAL[i]
                got(1, k)
                if i < FAR and i % 2 == 0:
                    put(1, k, 1, 0)
                share(1, k)
                got(3, k)
                if i < FAR and i % 2 == 1:
                    put(3, k, -1, 0)
                share(3, k)

            def stage3(i):
                k = Z_ARRIVAL[i]
                got(2, k)
                share(2, k)

            for i in range(NZ + 4):
                if i < NZ:
                    stage1(i)
                if 2 <= i < NZ + 2:
                    stage2(i - 2)
                if 4 <= i:
                    stage3(i - 4)
        else:
            for j in (1, 3, 2):
                put(0, 0, j, 0)

            @pl.when((r == 1) & (z == 0))
            def _():
                send("r1z", tslot(0), cross, (ex_s, 1), ex_r.at[8], pre_row + 1, lambda: tslot(0))

            for j in (0, 1, 3, 2):
                if j:
                    got(j, 0)
                put(j, 0, 0, 1)
                put(j, 0, 0, -1)
                if j == 0:
                    transpose(feat2, R)
                if j:
                    share(j, 0)
            for h in (1, 2, 3):
                for j in (0, 1, 3, 2):
                    got(j, h)
                    put(j, h, 0, 1)
                    share(j, h)
                    got(j, NZ - h)
                    if h < 3:
                        put(j, NZ - h, 0, -1)
                    share(j, NZ - h)
                if h == 3:

                    @pl.when((r > 1) | (z == 0))
                    def _():
                        arrived(cross, ex_s.at[0], ex_r.at[8])

                    @pl.when((r == 1) & (z == 0))
                    def _():
                        send("r1z", cross, tslot(2), (ex_s, 2), ex_r.at[2], below_row + 7, lambda: tslot(0))

                    @pl.when((r == 1) & (z != 0))
                    def _():
                        send("r1n", tslot(0), tslot(2), (ex_s, 1), ex_r.at[2], below_row + 7, lambda: tslot(0))

                    @pl.when(r == 3)
                    def _():
                        send("r3", cross, tslot(3), (ex_s, 2), ex_r.at[3], below_row + 5, lambda: tslot(0))

                    @pl.when(r == 5)
                    def _():
                        send("r5", cross, tslot(3), (ex_s, 2), ex_r.at[3], below_row + 7, lambda: tslot(0))

                    @pl.when(r == 7)
                    def _():
                        send("r7", cross, tslot(1), (ex_s, 2), ex_r.at[1], below_row + 7, lambda: tslot(0))

            for j in (0, 1, 3, 2):
                got(j, 4)
                share(j, 4)
            @pl.when(r != ROW - 1)
            def _():
                arrived(tslot(1), ex_s.at[0], ex_r.at[1])
                send("o7", tslot(1), tslot(2), (ex_s, 3), ex_r.at[2], near(-1), lambda: tslot(0))
                arrived(tslot(2), ex_s.at[0], ex_r.at[2])
                send("o7", tslot(2), tslot(3), (ex_s, 10), ex_r.at[3], near(-1), lambda: tslot(0))

        o0, ow = COLS[1 - c]
        for j in range(NY):
            for k in range(NZ):
                if j or k:
                    part = wblock(w_ref, -j, -k, o0, ow)
                    arrived(part, dd_s.at[0], dd_r.at[j * NZ + k])

    with jax.named_scope("gather"):
        @pl.when(core == 0)
        def _():
            gather(0)

        @pl.when(core == 1)
        def _():
            gather(1)

    with jax.named_scope("embed"):
        for c0, cw in TILES:
            unit[:, pl.ds(c0, cw)] = dot(feat[...], w_ref[:, pl.ds(c0, cw)])

        @pl.loop(0, R // 32, unroll=2)
        def _(i):
            rows = pl.ds(pl.multiple_of(i * 32, 32), 32)
            e = unit[rows, :]
            inv = 1.0 / jnp.sqrt(jnp.sum(e * e, axis=1, keepdims=True) + EPS)
            u = e * inv
            unit[rows, :] = u
            length[rows, :] = inv
            img[rows, :] = u.astype(BF16)

    @pl.when(r == ROW - 1)
    def _():
        arrived(tslot(1), ex_s.at[0], ex_r.at[1])
        send("r7", tslot(1), tslot(2), (ex_s, 3), ex_r.at[2], near(-1), lambda: tslot(0))
        arrived(tslot(2), ex_s.at[0], ex_r.at[2])
        send("r7", tslot(2), tslot(3), (ex_s, 10), ex_r.at[3], near(-1), lambda: tslot(0))

    with jax.named_scope("image_send"):
        i3 = (core == 1) & (r != ROW - 1) & (r != 5)
        last = z == NZ - 1
        i7_last = (r == ROW - 1) & last

        @pl.when(i7_last)
        def _():
            send("i7", slot(0), cross2, (ex_s, 5), ex_r.at[9], dev(1) - 1, lambda: slot(0))
            send("i7", slot(0), cross2, (ex_s, 6), ex_r.at[9], dev(1) - 3, lambda: slot(0))

        early = (r == 0) & (z != 0)

        @pl.when(r == 5)
        def _():
            send("i5", slot(0), cross2, (ex_s, 6), ex_r.at[9], near(5), lambda: slot(0))

        i5_early = (core == 1) & (r != ROW - 1) & ((r != 5) | (z != NZ - 1))

        @pl.when((core == 1) & ((r != ROW - 1) | (z != NZ - 1)))
        def _():
            send("i1", slot(0), slot(1), (ex_s, 5), ex_r.at[5], near(1), lambda: slot(0))

        @pl.when(i3)
        def _():
            send("i3", slot(0), slot(3), (ex_s, 6), ex_r.at[7], near(3), lambda: slot(0))

        @pl.when(core == 0)
        def _():
            send(0, slot(0), slot(1), (ex_s, 5), ex_r.at[5], near(1), lambda: slot(0))

        @pl.when((core == 0) & (r != ROW - 2))
        def _():
            send("i2", slot(0), slot(2), (ex_s, 6), ex_r.at[6], near(2), lambda: slot(0))

    factor = jnp.exp(jnp.full((1, R), nef_ref[0], F32))
    bias = bias_ref[0]

    def derivative(logit_dot, diagonal):
        logits = factor * logit_dot + bias
        if diagonal:
            same = lax.broadcasted_iota(jnp.int32, (R, R), 0) == lax.broadcasted_iota(jnp.int32, (R, R), 1)
            label = jnp.where(same, 1.0, -1.0).astype(F32)
            g = -factor * label / (1.0 + jnp.exp(label * logits))
        else:
            g = factor / (1.0 + jnp.exp(-logits))
        return g.astype(BF16)

    def back(grad, u, inv):
        return (grad - u * jnp.sum(u * grad, axis=1, keepdims=True)) * inv

    with jax.named_scope("image_side"):
        for s in range(S):
            if s == 1:

                @pl.when(core == 0)
                def _():
                    arrived(tslot(1), ex_s.at[0], ex_r.at[1])
                    arrived(tslot(2), ex_s.at[0], ex_r.at[2])

            if s == 3:
                with jax.named_scope("text_wait"):
                    arrived(tslot(3), ex_s.at[0], ex_r.at[3])
            pair[:, pl.ds(s * R, R)] = derivative(dot_nt(img[pl.ds(0, R), :], tlow[pl.ds(s * R, R), :]), s == 0)
        for c0, cw in TILES:
            igrad[:, pl.ds(c0, cw)] = dot(pair[...], tlow[:, pl.ds(c0, cw)])

        @pl.loop(0, R // 32, unroll=2)
        def _(i):
            rows = pl.ds(pl.multiple_of(i * 32, 32), 32)
            eg[rows, :] = back(igrad[rows, :], unit[rows, :], length[rows, :]).astype(BF16)

    with jax.named_scope("eg_send"):
        @pl.when(core == 0)
        def _():
            part = pl.ds(RCOLS[1][0], RCOLS[1][1])
            send(0, eg.at[pl.ds(0, R), part], eg.at[pl.ds(R, R), part], (ex_s, 9), ex_r.at[10], me + 1, lambda: eg.at[pl.ds(0, R), pl.ds(RCOLS[1][0], RCOLS[1][1])])

        @pl.when(core == 1)
        def _():
            part = pl.ds(RCOLS[0][0], RCOLS[0][1])
            send(1, eg.at[pl.ds(0, R), part], eg.at[pl.ds(R, R), part], (ex_s, 9), ex_r.at[10], me - 1, lambda: eg.at[pl.ds(0, R), pl.ds(RCOLS[0][0], RCOLS[0][1])])

    def feature_gradient(i):
        cols = pl.ds(i * 512, 512)
        gfeat[:, cols] = dot_nt(eg[pl.ds(0, R), :], w_ref[cols, :]).astype(BF16)

    with jax.named_scope("feat_grad"):
        feature_gradient(0)
        feature_gradient(1)

    def reduce_weight(c):
        c0, cw = RCOLS[c]
        count = [0]
        arrived(eg.at[pl.ds(R, R), pl.ds(c0, cw)], ex_s.at[0], ex_r.at[10])

        def product(j):
            rows = pl.ds(pl.multiple_of(at_y[j], 8), YROWS)
            gpart[rows, pl.ds(0, cw)] = dot(feat_t[rows, :], eg[:, pl.ds(c0, cw)]).astype(BF16)

        def mine(dy, dz):
            return wblock(gpart, dy, dz, 0, cw)

        def buf(i):
            return rbuf.at[i, :, pl.ds(0, cw)]

        def emit(src, i, dy, dz):
            send(c, src, buf(i), (rs_s, count[0]), rs_r.at[i], dev(dy, dz), lambda: buf(0))
            count[0] += 1

        def take(i):
            arrived(buf(i), rs_s.at[0], rs_r.at[i])
            return buf(i)[...].astype(F32)

        if c == Y_CORE:
            product(2)

            @pl.when(r == ROW - 2)
            def _():
                send("i6", slot(0), cross2, (ex_s, 6), ex_r.at[9], first, lambda: slot(0))

            for i, k in enumerate(Z_ORDER + (0,)):
                emit(mine(2, k), k, 2 if i < NEAR else 1 if i % 2 == 0 else -1, 0)
            product(1)
            product(3)
            product(0)
            feature_gradient(2)
            for i, k in enumerate(Z_ORDER + (0,)):
                step = 1 if i % 2 == 0 else -1
                part = mine(step, k)
                other = mine(-step, k)
                emit(other, 8 + k if step == -1 else 16 + k, -step, 0)
                if i >= NEAR:
                    part[...] = (part[...].astype(F32) + take(k)).astype(BF16)
                emit(part, 8 + k if step == 1 else 16 + k, step, 0)
            @pl.when(r == 2)
            def _():
                arrived(cross2, ex_s.at[0], ex_r.at[9])
                send("i2r", cross2, slot(3), (ex_s, 13), ex_r.at[7], first, lambda: slot(0))

            for i, k in enumerate(Z_ORDER + (0,)):
                total = mine(0, k)[...].astype(F32) + take(8 + k) + take(16 + k)
                if i < NEAR:
                    total = total + take(k)
                if k:
                    sbuf[k, :, pl.ds(0, cw)] = total.astype(BF16)
                    emit(sbuf.at[k, :, pl.ds(0, cw)], 24 + k, 0, k)
            @pl.when(r == 0)
            def _():
                arrived(cross2, ex_s.at[0], ex_r.at[9])
                send("i0", cross2, slot(2), (ex_s, 13), ex_r.at[6], near(ROW), lambda: slot(0))

            @pl.when(((r == 4) | (r == 6)) & last)
            def _():
                arrived(cross2, ex_s.at[0], ex_r.at[9])

            @pl.when((r == 6) & last)
            def _():
                send("i6r", cross2, slot(1), (ex_s, 13), ex_r.at[5], dev(0, 1) - r, lambda: slot(0))

            @pl.when((r == 4) & last)
            def _():
                send("i4r", cross2, slot(3), (ex_s, 13), ex_r.at[7], dev(0, 1) - r + 2, lambda: slot(0))

            @pl.when(early)
            def _():
                arrived(slot(1), ex_s.at[0], ex_r.at[5])
                send("i0e", slot(1), slot(3), (ex_s, 7), ex_r.at[7], near(2), lambda: slot(0))

            for k in Z_ARRIVAL[1:]:
                total = total + take(24 + k)
        else:
            for j in range(NY):
                product(j)
            order = (2, 1, 3, 0)
            for j in order:
                emit(mine(j, 4), 16 + j, 0, -1)
            feature_gradient(2)
            for h in (3, 2, 1):
                s = 3 - h
                for j in order:
                    for sign, base in ((1, 0), (-1, 16)):
                        part = mine(j, sign * h)
                        if s or sign == -1:
                            part[...] = (part[...].astype(F32) + take(base + 4 * s + j)).astype(BF16)
                        emit(part, base + 4 * (s + 1) + j, 0, sign)
            for j in order:
                total = mine(j, 0)[...].astype(F32) + take(12 + j) + take(28 + j)
                if j:
                    sbuf[j, :, pl.ds(0, cw)] = total.astype(BF16)
                    emit(sbuf.at[j, :, pl.ds(0, cw)], 32 + j, j, 0)
            for j in (1, 3, 2):
                total = total + take(32 + j)

        xrow[:, pl.ds(0, cw)] = total
        for k in range(ROW):
            xs[k, :, pl.ds(0, cw)] = xrow[pl.ds(SH * k, SH), pl.ds(0, cw)]
        for k in (4, 3, 5, 2, 6, 1, 7):
            send(
                c, xs.at[lax.rem(r + k, ROW), :, pl.ds(0, cw)], xr.at[r, :, pl.ds(0, cw)],
                (xg_s, k), xg_r.at[k], row_dev(k), lambda: xs.at[0, :, pl.ds(0, cw)],
            )
        xr[r, :, pl.ds(0, cw)] = xs[r, :, pl.ds(0, cw)]

    with jax.named_scope("reduce"):
        @pl.when(core == 0)
        def _():
            reduce_weight(0)

        @pl.when(core == 1)
        def _():
            reduce_weight(1)

    def similarities(s):
        pair[:, pl.ds(s * R, R)] = derivative(dot_nt(tlow[pl.ds(0, R), :], img[pl.ds(s * R, R), :]), s == 0)

    with jax.named_scope("image_wait"):
        @pl.when((core == 0) & ((r != 0) | (z == 0)))
        def _():
            arrived(slot(1), ex_s.at[0], ex_r.at[5])

        @pl.when(core == 0)
        def _():
            send(0, slot(1), slot(2), (ex_s, 8), ex_r.at[6], near(1), lambda: slot(0))

        @pl.when((core == 0) & (r != 0))
        def _():
            arrived(slot(2), ex_s.at[0], ex_r.at[6])
            send("s2", slot(2), slot(3), (ex_s, 11), ex_r.at[7], near(1), lambda: slot(0))

        @pl.when(core == 1)
        def _():
            arrived(slot(1), ex_s.at[0], ex_r.at[5])

        for s in range(2):
            similarities(s)
        for c0, cw in TILES:
            igrad[:, pl.ds(c0, cw)] = dot(pair[:, pl.ds(0, 2 * R)], img[pl.ds(0, 2 * R), pl.ds(c0, cw)])

        @pl.when(r == 0)
        def _():
            arrived(slot(2), ex_s.at[0], ex_r.at[6])
            send("s0", slot(2), slot(3), (ex_s, 11), ex_r.at[7], near(1), lambda: slot(0))

        @pl.when(core == 1)
        def _():
            arrived(slot(2), ex_s.at[0], ex_r.at[6])

        similarities(2)
        arrived(slot(3), ex_s.at[0], ex_r.at[7])

    with jax.named_scope("text_side"):
        similarities(3)
        for c0, cw in TILES:
            igrad[:, pl.ds(c0, cw)] += dot(pair[:, pl.ds(2 * R, 2 * R)], img[pl.ds(2 * R, 2 * R), pl.ds(c0, cw)])

        @pl.loop(0, R // 32, unroll=2)
        def _(i):
            rows = pl.ds(pl.multiple_of(i * 32, 32), 32)
            inv = tlen[rows, :]
            gtext[rows, :] = back(igrad[rows, :], traw[rows, :].astype(F32) * inv, inv).astype(BF16)

    with jax.named_scope("final"):
        for k in range(1, ROW):
            source = lax.rem(r + (ROW - k), ROW)

            @pl.when(lax.rem(source, 2) == 1)
            def _():
                arrived(xr.at[source, :, pl.ds(0, RCOLS[1][1])], xg_s.at[k], xg_r.at[k])

            @pl.when(lax.rem(source, 2) == 0)
            def _():
                arrived(xr.at[source, :, pl.ds(0, RCOLS[0][1])], xg_s.at[k], xg_r.at[k])

        for c in range(2):
            c0, cw = RCOLS[c]
            total = xr[c, :, pl.ds(0, cw)]
            for k in range(1, NX):
                total = total + xr[2 * k + c, :, pl.ds(0, cw)]
            gout[:, pl.ds(c0, cw)] = total

    with jax.named_scope("drain"):
        for only, wait in pending:
            if only is None:
                wait()
        groups = {
            0: core == 0, 1: core == 1, "r0": r == 0, "r2": r == 2, "r3": r == 3, "r5": r == 5, "r1z": (r == 1) & (z == 0), "r1n": (r == 1) & (z != 0), "r7": r == ROW - 1, "i0": r == 0,
            "o7": (core == 1) & (r != ROW - 1), "t3": (core == 0) & (r != 0), "t4": (core == 0) & (r > 2),
            "t2": (core == 1) & (r != 1), "i3": i3, "s0": r == 0, "s2": (core == 0) & (r != 0), "i0e": early, "i7": i7_last, "i6r": (r == 6) & last, "i4r": (r == 4) & last, "i1": (core == 1) & ((r != ROW - 1) | (z != NZ - 1)),
            "i5": r == 5, "i2r": r == 2, "i6": r == ROW - 2,
            "i2": (core == 0) & (r != ROW - 2),
        }
        for group, inside in groups.items():

            @pl.when(inside)
            def _():
                for only, wait in pending:
                    if only == group:
                        wait()


def put_out(gf, gt, gw, gf_out, gt_out, gw_out, sem):
    copies = [pltpu.make_async_copy(a, b, sem.at[i]) for i, (a, b) in enumerate(((gf, gf_out), (gt, gt_out), (gw, gw_out)))]
    for copy in copies:
        copy.start()
    for copy in copies:
        copy.wait()


def on_device(image_features, head_weight, text_embeds, natural_exponent_factor, logit_bias):
    dma = pltpu.SemaphoreType.DMA
    hbm = pl.BlockSpec(memory_space=pltpu.HBM)
    local = pl.BlockSpec(memory_space=pltpu.VMEM)
    scalar = pl.BlockSpec(memory_space=pltpu.SMEM)
    results = pl.pallas_call(
        kernel,
        out_shape=(
            jax.ShapeDtypeStruct((R, D), BF16),
            jax.ShapeDtypeStruct((R, E), BF16),
            jax.ShapeDtypeStruct((SH, E), F32),
        ),
        in_specs=[hbm, hbm, hbm, scalar, scalar],
        out_specs=(local, local, local),
        scratch_shapes=[
            pltpu.VMEM((D, E), BF16),
            pltpu.VMEM((R, D), BF16),
            pltpu.VMEM((R, D), BF16),
            pltpu.VMEM((D, 2 * R), BF16),
            pltpu.VMEM((R, E), F32),
            pltpu.VMEM((R, 1), F32),
            pltpu.VMEM((S * R, E), BF16),
            pltpu.VMEM((R, E), BF16),
            pltpu.VMEM((S * R, E), BF16),
            pltpu.VMEM((R, 1), F32),
            pltpu.VMEM((R, S * R), BF16),
            pltpu.VMEM((2 * R, E), BF16),
            pltpu.VMEM((D, W2), BF16),
            pltpu.VMEM((ROW, SH, E), BF16),
            pltpu.VMEM((BLK, E), F32),
            pltpu.VMEM((36, BLK, W2), BF16),
            pltpu.VMEM((8, BLK, W2), BF16),
            pltpu.VMEM((BLK, W2), F32),
            pltpu.VMEM((ROW, SH, W2), F32),
            pltpu.VMEM((ROW, SH, W2), F32),
            pltpu.VMEM((R, E), F32),
            pltpu.VMEM((R, E), BF16),
            pltpu.VMEM((R, E), BF16),
            dma((3,)),
            dma((ROW,)), dma((ROW,)),
            dma((32,)), dma((32,)),
            dma((32,)), dma((32,)),
            dma((14,)), dma((11,)),
            dma((40,)), dma((36,)),
            dma((ROW,)), dma((ROW,)),
        ],
        compiler_params=pltpu.CompilerParams(
            collective_id=0, has_side_effects=True, vmem_limit_bytes=52 * 1024 * 1024
        ),
    )(*(pltpu.with_memory_space_constraint(a, pltpu.HBM) for a in (image_features, head_weight, text_embeds)), natural_exponent_factor, logit_bias)
    return pl.pallas_call(
        put_out,
        out_shape=tuple(jax.ShapeDtypeStruct(a.shape, a.dtype) for a in results),
        in_specs=[local] * 3,
        out_specs=[hbm] * 3,
        scratch_shapes=[dma((3,))],
        compiler_params=pltpu.CompilerParams(vmem_limit_bytes=8 * 1024 * 1024),
    )(*results)


def solution(mesh):
    split = P("blk", None)
    return jax.shard_map(
        on_device,
        mesh=mesh,
        in_specs=(split, split, split, P(), P()),
        out_specs=(split, split, split),
        check_vma=False,
    )
```

```python
import jax
import jax.numpy as jnp
from jax import lax
from jax.experimental import pallas as pl
from jax.experimental.pallas import tpu as pltpu
from jax.sharding import PartitionSpec as P

MESH = pl.DeviceIdType.MESH
D, E, R, S = 1536, 1152, 256, 4
NY, NZ, NX = 4, 8, 4
N = NY * NZ * NX * 2
ROW = NX * 2
SH = D // N
BLK = SH * ROW
YROWS = BLK * NZ
W1 = 640
COLS = ((0, W1), (W1, E - W1))
FAR, NEAR = 5, 0
W2 = 768
RCOLS = ((0, W2), (W2, E - W2))
Y_CORE = 0
EPS = 1e-06
TILES = ((0, 512), (512, 512), (1024, 128))
F32, BF16 = jnp.float32, jnp.bfloat16
Z_ORDER = (4, 3, 5, 2, 6, 1, 7)
Z_ARRIVAL = (0, 1, 7, 2, 6, 3, 5, 4)
ORDER_NT = (((1,), (1,)), ((), ()))


def dot(a, b):
    return jnp.dot(a, b, preferred_element_type=F32)


def dot_nt(a, b):
    return lax.dot_general(a, b, ORDER_NT, preferred_element_type=F32)


def kernel(
    feat_hbm, w_hbm, text_hbm, nef_ref, bias_ref,
    gfeat, gtext, gout,
    w_ref, feat, feat2, feat_t, unit, length, img, traw, tlow, tlen, pair, eg,
    gpart, xbuf, wrow, rbuf, sbuf, xrow, xs, xr, igrad, cross, cross2,
    in_sem, xw_s, xw_r, ag_s, ag_r, dd_s, dd_r, ex_s, ex_r, rs_s, rs_r, xg_s, xg_r,
):
    me = lax.axis_index("blk")
    core = lax.rem(me, 2)
    r = lax.rem(me, ROW)
    z = lax.rem(lax.div(me, ROW), NZ)
    y = lax.div(me, ROW * NZ)
    pending = []

    row_y = [lax.rem(y + j, NY) for j in range(NY)]
    row_z = [lax.rem(z + k, NZ) for k in range(NZ)]
    dev_y = [v * (NZ * ROW) for v in row_y]
    dev_z = [v * ROW + r for v in row_z]
    at_y = [v * YROWS for v in row_y]
    at_z = [v * BLK for v in row_z]

    def dev(dy=0, dz=0):
        return dev_y[dy % NY] + dev_z[dz % NZ]

    wrap = 1 - lax.div(z + (NZ - 1), NZ)
    first = me - r
    pre_row = first + wrap * (dev_y[NY - 1] - dev_y[0])
    below_row = dev(0, -1) - r

    def row_dev(k):
        return me - r + lax.rem(r + k, ROW)

    def near(k):
        return lax.rem(me + (k + N), N)

    def remote(src, dst, ss, rs, to):
        return pltpu.make_async_remote_copy(
            src_ref=src, dst_ref=dst, send_sem=ss, recv_sem=rs, device_id=(to,), device_id_type=MESH
        )

    def send(only, src, dst, ss, rs, to, like=None):
        sems, i = ss
        remote(src, dst, sems.at[i], rs, to).start()

        def wait():
            ref = src if like is None else like()
            remote(ref, ref, sems.at[i], sems.at[i], near(1)).wait_send()

        pending.append((only, wait))

    def arrived(dst, ss, rs):
        remote(dst, dst, ss, rs, near(1)).wait_recv()

    def wblock(ref, dy, dz, c0, cw):
        start = pl.multiple_of(at_y[dy % NY] + at_z[dz % NZ], 8)
        return ref.at[pl.ds(start, BLK), pl.ds(c0, cw)]

    def transpose(src, col):
        if col:
            arrived(feat2, ex_s.at[12], ex_r.at[0])

        @pl.loop(0, D // 256)
        def _(i):
            cols = pl.ds(pl.multiple_of(i * 256, 256), 256)
            feat_t[cols, pl.ds(col, R)] = jnp.transpose(src[:, cols])

    def tslot(k):
        return tlow.at[pl.ds(k * R, R), :]

    def slot(k):
        return img.at[pl.ds(k * R, R), :]

    cp_w = pltpu.make_async_copy(w_hbm, xbuf.at[r], in_sem.at[0])
    cp_t = pltpu.make_async_copy(text_hbm, traw, in_sem.at[1])
    cp_f = pltpu.make_async_copy(feat_hbm, feat, in_sem.at[2])
    cp_w.start()
    cp_t.start()
    cp_f.start()

    with jax.named_scope("barrier"):
        barrier = pltpu.get_barrier_semaphore()
        peers = [row_dev(k) for k in range(1, ROW)] + [dev(dz=k) for k in range(1, NZ)]
        peers += [dev(d) - r + lax.rem(r + d * -k + ROW, ROW) for d in (-1, 1) for k in (1, 3, 7)]
        peers += [dev(0, d) - r + lax.rem(r + d * -k + ROW, ROW) for d in (-1, 1) for k in (2, 6)]
        peers += [dev(dy=k) for k in range(1, NY)] + [near(k) for k in (-ROW, -5, -3, -2, -1, 1, 2, 3, 5, ROW)]
        for peer in peers:
            pl.semaphore_signal(barrier, inc=1, device_id=(peer,), device_id_type=MESH)
        pl.semaphore_wait(barrier, len(peers))

    with jax.named_scope("w_row_send"):
        cp_w.wait()
        for k in (4, 3, 5, 2, 6, 1, 7):
            send(None, xbuf.at[r], xbuf.at[r], (xw_s, k), xw_r.at[k], row_dev(k), lambda: xbuf.at[0])

    with jax.named_scope("own_text"):
        cp_t.wait()

        @pl.loop(0, R // 32, unroll=2)
        def _(i):
            rows = pl.ds(pl.multiple_of(i * 32, 32), 32)
            t = traw[rows, :].astype(F32)
            inv = 1.0 / jnp.sqrt(jnp.sum(t * t, axis=1, keepdims=True) + EPS)
            tlow[rows, :] = (t * inv).astype(BF16)
            tlen[rows, :] = inv

        cp_f.wait()
        send(None, feat, feat2, (ex_s, 12), ex_r.at[0], me + 1 - 2 * core)
        transpose(feat, 0)

    with jax.named_scope("w_row"):
        for k in range(1, ROW):
            arrived(xbuf.at[lax.rem(r + (ROW - k), ROW)], xw_s.at[k], xw_r.at[k])
        for k in range(ROW):
            wrow[pl.ds(SH * k, SH), :] = xbuf[k].astype(F32)
        own = pl.multiple_of(y * YROWS + z * BLK, 8)
        w_ref[pl.ds(own, BLK), :] = wrow[...].astype(BF16)

    with jax.named_scope("text_send"):
        @pl.when((core == 0) & (r != 0))
        def _():
            send("t3", tslot(0), tslot(1), (ex_s, 0), ex_r.at[1], near(-1), lambda: tslot(0))

        @pl.when((core == 0) & (r > 2))
        def _():
            send("t4", tslot(0), tslot(3), (ex_s, 1), ex_r.at[3], near(-3), lambda: tslot(0))

        @pl.when(core == 1)
        def _():
            send(1, tslot(0), tslot(1), (ex_s, 0), ex_r.at[1], near(-1), lambda: tslot(0))

        @pl.when((core == 1) & (r != 1))
        def _():
            send("t2", tslot(0), tslot(2), (ex_s, 1), ex_r.at[2], near(-2), lambda: tslot(0))

        @pl.when(r == 0)
        def _():
            send("r0", tslot(0), cross, (ex_s, 0), ex_r.at[8], pre_row + 7, lambda: tslot(0))
            send("r0", tslot(0), cross, (ex_s, 1), ex_r.at[8], pre_row + 3, lambda: tslot(0))

        @pl.when(r == 2)
        def _():
            send("r2", tslot(0), cross, (ex_s, 1), ex_r.at[8], pre_row + 5, lambda: tslot(0))


    def gather(c):
        c0, cw = COLS[c]
        sibling = me + (1 - 2 * c)
        count = [0]
        like = lambda: w_ref.at[pl.ds(0, BLK), pl.ds(c0, cw)]

        def put(j, k, dy, dz):
            part = wblock(w_ref, -j, -k, c0, cw)
            idx = ((j + dy) % NY) * NZ + (k + dz) % NZ
            send(c, part, part, (ag_s, count[0]), ag_r.at[idx], dev(dy, dz), like)
            count[0] += 1

        def share(j, k):
            part = wblock(w_ref, -j, -k, c0, cw)
            send(c, part, part, (dd_s, j * NZ + k), dd_r.at[j * NZ + k], sibling, like)

        def got(j, k):
            part = wblock(w_ref, -j, -k, c0, cw)
            arrived(part, ag_s.at[0], ag_r.at[j * NZ + k])
            return part

        if c == Y_CORE:
            for k in Z_ARRIVAL[1:]:
                put(0, 0, 0, k)
            transpose(feat2, R)

            def stage1(i):
                k = Z_ARRIVAL[i]
                if k:
                    got(0, k)
                put(0, k, 1, 0)
                put(0, k, -1, 0)
                if i >= FAR:
                    put(0, k, 2, 0)
                if k:
                    share(0, k)

            def stage2(i):
                k = Z_ARRIVAL[i]
                got(1, k)
                if i < FAR and i % 2 == 0:
                    put(1, k, 1, 0)
                share(1, k)
                got(3, k)
                if i < FAR and i % 2 == 1:
                    put(3, k, -1, 0)
                share(3, k)

            def stage3(i):
                k = Z_ARRIVAL[i]
                got(2, k)
                share(2, k)

            for i in range(NZ + 4):
                if i < NZ:
                    stage1(i)
                if 2 <= i < NZ + 2:
                    stage2(i - 2)
                if 4 <= i:
                    stage3(i - 4)
        else:
            for j in (1, 3, 2):
                put(0, 0, j, 0)

            @pl.when((r == 1) & (z == 0))
            def _():
                send("r1z", tslot(0), cross, (ex_s, 1), ex_r.at[8], pre_row + 1, lambda: tslot(0))

            for j in (0, 1, 3, 2):
                if j:
                    got(j, 0)
                put(j, 0, 0, 1)
                put(j, 0, 0, -1)
                if j == 0:
                    transpose(feat2, R)
                if j:
                    share(j, 0)
            for h in (1, 2, 3):
                for j in (0, 1, 3, 2):
                    got(j, h)
                    put(j, h, 0, 1)
                    share(j, h)
                    got(j, NZ - h)
                    if h < 3:
                        put(j, NZ - h, 0, -1)
                    share(j, NZ - h)
                if h == 3:

                    @pl.when((r > 1) | (z == 0))
                    def _():
                        arrived(cross, ex_s.at[0], ex_r.at[8])

                    @pl.when((r == 1) & (z == 0))
                    def _():
                        send("r1z", cross, tslot(2), (ex_s, 2), ex_r.at[2], below_row + 7, lambda: tslot(0))

                    @pl.when((r == 1) & (z != 0))
                    def _():
                        send("r1n", tslot(0), tslot(2), (ex_s, 1), ex_r.at[2], below_row + 7, lambda: tslot(0))

                    @pl.when(r == 3)
                    def _():
                        send("r3", cross, tslot(3), (ex_s, 2), ex_r.at[3], below_row + 5, lambda: tslot(0))

                    @pl.when(r == 5)
                    def _():
                        send("r5", cross, tslot(3), (ex_s, 2), ex_r.at[3], below_row + 7, lambda: tslot(0))

                    @pl.when(r == 7)
                    def _():
                        send("r7", cross, tslot(1), (ex_s, 2), ex_r.at[1], below_row + 7, lambda: tslot(0))

            for j in (0, 1, 3, 2):
                got(j, 4)
                share(j, 4)
            @pl.when(r != ROW - 1)
            def _():
                arrived(tslot(1), ex_s.at[0], ex_r.at[1])
                send("o7", tslot(1), tslot(2), (ex_s, 3), ex_r.at[2], near(-1), lambda: tslot(0))
                arrived(tslot(2), ex_s.at[0], ex_r.at[2])
                send("o7", tslot(2), tslot(3), (ex_s, 10), ex_r.at[3], near(-1), lambda: tslot(0))

        o0, ow = COLS[1 - c]
        for j in range(NY):
            for k in range(NZ):
                if j or k:
                    part = wblock(w_ref, -j, -k, o0, ow)
                    arrived(part, dd_s.at[0], dd_r.at[j * NZ + k])

    with jax.named_scope("gather"):
        @pl.when(core == 0)
        def _():
            gather(0)

        @pl.when(core == 1)
        def _():
            gather(1)

    with jax.named_scope("embed"):
        for c0, cw in TILES:
            unit[:, pl.ds(c0, cw)] = dot(feat[...], w_ref[:, pl.ds(c0, cw)])

        @pl.loop(0, R // 32, unroll=2)
        def _(i):
            rows = pl.ds(pl.multiple_of(i * 32, 32), 32)
            e = unit[rows, :]
            inv = 1.0 / jnp.sqrt(jnp.sum(e * e, axis=1, keepdims=True) + EPS)
            u = e * inv
            unit[rows, :] = u
            length[rows, :] = inv
            img[rows, :] = u.astype(BF16)

    @pl.when(r == ROW - 1)
    def _():
        arrived(tslot(1), ex_s.at[0], ex_r.at[1])
        send("r7", tslot(1), tslot(2), (ex_s, 3), ex_r.at[2], near(-1), lambda: tslot(0))
        arrived(tslot(2), ex_s.at[0], ex_r.at[2])
        send("r7", tslot(2), tslot(3), (ex_s, 10), ex_r.at[3], near(-1), lambda: tslot(0))

    with jax.named_scope("image_send"):
        i3 = (core == 1) & (r != ROW - 1) & (r != 5)
        last = z == NZ - 1
        i7_last = (r == ROW - 1) & last

        @pl.when(i7_last)
        def _():
            send("i7", slot(0), cross2, (ex_s, 5), ex_r.at[9], dev(1) - 1, lambda: slot(0))
            send("i7", slot(0), cross2, (ex_s, 6), ex_r.at[9], dev(1) - 3, lambda: slot(0))

        early = (r == 0) & (z != 0)

        @pl.when(r == 5)
        def _():
            send("i5", slot(0), cross2, (ex_s, 6), ex_r.at[9], near(5), lambda: slot(0))

        i5_early = (core == 1) & (r != ROW - 1) & ((r != 5) | (z != NZ - 1))

        @pl.when((core == 1) & ((r != ROW - 1) | (z != NZ - 1)))
        def _():
            send("i1", slot(0), slot(1), (ex_s, 5), ex_r.at[5], near(1), lambda: slot(0))

        @pl.when(i3)
        def _():
            send("i3", slot(0), slot(3), (ex_s, 6), ex_r.at[7], near(3), lambda: slot(0))

        @pl.when(core == 0)
        def _():
            send(0, slot(0), slot(1), (ex_s, 5), ex_r.at[5], near(1), lambda: slot(0))

        @pl.when((core == 0) & (r != ROW - 2))
        def _():
            send("i2", slot(0), slot(2), (ex_s, 6), ex_r.at[6], near(2), lambda: slot(0))

    factor = jnp.exp(jnp.full((1, R), nef_ref[0], F32))
    bias = bias_ref[0]

    def derivative(logit_dot, diagonal):
        logits = factor * logit_dot + bias
        if diagonal:
            same = lax.broadcasted_iota(jnp.int32, (R, R), 0) == lax.broadcasted_iota(jnp.int32, (R, R), 1)
            label = jnp.where(same, 1.0, -1.0).astype(F32)
            g = -factor * label / (1.0 + jnp.exp(label * logits))
        else:
            g = factor / (1.0 + jnp.exp(-logits))
        return g.astype(BF16)

    def back(grad, u, inv):
        return (grad - u * jnp.sum(u * grad, axis=1, keepdims=True)) * inv

    with jax.named_scope("image_side"):
        for s in range(S):
            if s == 1:

                @pl.when(core == 0)
                def _():
                    arrived(tslot(1), ex_s.at[0], ex_r.at[1])
                    arrived(tslot(2), ex_s.at[0], ex_r.at[2])

            if s == 3:
                with jax.named_scope("text_wait"):
                    arrived(tslot(3), ex_s.at[0], ex_r.at[3])
            pair[:, pl.ds(s * R, R)] = derivative(dot_nt(img[pl.ds(0, R), :], tlow[pl.ds(s * R, R), :]), s == 0)
        for c0, cw in TILES:
            igrad[:, pl.ds(c0, cw)] = dot(pair[...], tlow[:, pl.ds(c0, cw)])

        @pl.loop(0, R // 32, unroll=2)
        def _(i):
            rows = pl.ds(pl.multiple_of(i * 32, 32), 32)
            eg[rows, :] = back(igrad[rows, :], unit[rows, :], length[rows, :]).astype(BF16)

    with jax.named_scope("eg_send"):
        @pl.when(core == 0)
        def _():
            part = pl.ds(RCOLS[1][0], RCOLS[1][1])
            send(0, eg.at[pl.ds(0, R), part], eg.at[pl.ds(R, R), part], (ex_s, 9), ex_r.at[10], me + 1, lambda: eg.at[pl.ds(0, R), pl.ds(RCOLS[1][0], RCOLS[1][1])])

        @pl.when(core == 1)
        def _():
            part = pl.ds(RCOLS[0][0], RCOLS[0][1])
            send(1, eg.at[pl.ds(0, R), part], eg.at[pl.ds(R, R), part], (ex_s, 9), ex_r.at[10], me - 1, lambda: eg.at[pl.ds(0, R), pl.ds(RCOLS[0][0], RCOLS[0][1])])

    def feature_gradient(i):
        cols = pl.ds(i * 512, 512)
        gfeat[:, cols] = dot_nt(eg[pl.ds(0, R), :], w_ref[cols, :]).astype(BF16)

    with jax.named_scope("feat_grad"):
        feature_gradient(0)
        feature_gradient(1)

    def reduce_weight(c):
        c0, cw = RCOLS[c]
        count = [0]
        arrived(eg.at[pl.ds(R, R), pl.ds(c0, cw)], ex_s.at[0], ex_r.at[10])

        def product(j):
            rows = pl.ds(pl.multiple_of(at_y[j], 8), YROWS)
            gpart[rows, pl.ds(0, cw)] = dot(feat_t[rows, :], eg[:, pl.ds(c0, cw)]).astype(BF16)

        def mine(dy, dz):
            return wblock(gpart, dy, dz, 0, cw)

        def buf(i):
            return rbuf.at[i, :, pl.ds(0, cw)]

        def emit(src, i, dy, dz):
            send(c, src, buf(i), (rs_s, count[0]), rs_r.at[i], dev(dy, dz), lambda: buf(0))
            count[0] += 1

        def take(i):
            arrived(buf(i), rs_s.at[0], rs_r.at[i])
            return buf(i)[...].astype(F32)

        if c == Y_CORE:
            product(2)

            @pl.when(r == ROW - 2)
            def _():
                send("i6", slot(0), cross2, (ex_s, 6), ex_r.at[9], first, lambda: slot(0))

            for i, k in enumerate(Z_ORDER + (0,)):
                emit(mine(2, k), k, 2 if i < NEAR else 1 if i % 2 == 0 else -1, 0)
            product(1)
            product(3)
            product(0)
            feature_gradient(2)
            for i, k in enumerate(Z_ORDER + (0,)):
                step = 1 if i % 2 == 0 else -1
                part = mine(step, k)
                other = mine(-step, k)
                emit(other, 8 + k if step == -1 else 16 + k, -step, 0)
                if i >= NEAR:
                    part[...] = (part[...].astype(F32) + take(k)).astype(BF16)
                emit(part, 8 + k if step == 1 else 16 + k, step, 0)
            @pl.when(r == 2)
            def _():
                arrived(cross2, ex_s.at[0], ex_r.at[9])
                send("i2r", cross2, slot(3), (ex_s, 13), ex_r.at[7], first, lambda: slot(0))

            for i, k in enumerate(Z_ORDER + (0,)):
                total = mine(0, k)[...].astype(F32) + take(8 + k) + take(16 + k)
                if i < NEAR:
                    total = total + take(k)
                if k:
                    sbuf[k, :, pl.ds(0, cw)] = total.astype(BF16)
                    emit(sbuf.at[k, :, pl.ds(0, cw)], 24 + k, 0, k)
            @pl.when(r == 0)
            def _():
                arrived(cross2, ex_s.at[0], ex_r.at[9])
                send("i0", cross2, slot(2), (ex_s, 13), ex_r.at[6], near(ROW), lambda: slot(0))

            @pl.when(((r == 4) | (r == 6)) & last)
            def _():
                arrived(cross2, ex_s.at[0], ex_r.at[9])

            @pl.when((r == 6) & last)
            def _():
                send("i6r", cross2, slot(1), (ex_s, 13), ex_r.at[5], dev(0, 1) - r, lambda: slot(0))

            @pl.when((r == 4) & last)
            def _():
                send("i4r", cross2, slot(3), (ex_s, 13), ex_r.at[7], dev(0, 1) - r + 2, lambda: slot(0))

            @pl.when(early)
            def _():
                arrived(slot(1), ex_s.at[0], ex_r.at[5])
                send("i0e", slot(1), slot(3), (ex_s, 7), ex_r.at[7], near(2), lambda: slot(0))

            for k in Z_ARRIVAL[1:]:
                total = total + take(24 + k)
        else:
            order = (2, 1, 3, 0)
            for j in order:
                product(j)
                emit(mine(j, 4), 16 + j, 0, -1)
            feature_gradient(2)
            for h in (3, 2, 1):
                s = 3 - h
                for j in order:
                    for sign, base in ((1, 0), (-1, 16)):
                        part = mine(j, sign * h)
                        if s or sign == -1:
                            part[...] = (part[...].astype(F32) + take(base + 4 * s + j)).astype(BF16)
                        emit(part, base + 4 * (s + 1) + j, 0, sign)
            for j in order:
                total = mine(j, 0)[...].astype(F32) + take(12 + j) + take(28 + j)
                if j:
                    sbuf[j, :, pl.ds(0, cw)] = total.astype(BF16)
                    emit(sbuf.at[j, :, pl.ds(0, cw)], 32 + j, j, 0)
            for j in (1, 3, 2):
                total = total + take(32 + j)

        xrow[:, pl.ds(0, cw)] = total
        for k in range(ROW):
            xs[k, :, pl.ds(0, cw)] = xrow[pl.ds(SH * k, SH), pl.ds(0, cw)]
        for k in (4, 3, 5, 2, 6, 1, 7):
            send(
                c, xs.at[lax.rem(r + k, ROW), :, pl.ds(0, cw)], xr.at[r, :, pl.ds(0, cw)],
                (xg_s, k), xg_r.at[k], row_dev(k), lambda: xs.at[0, :, pl.ds(0, cw)],
            )
        xr[r, :, pl.ds(0, cw)] = xs[r, :, pl.ds(0, cw)]

    with jax.named_scope("reduce"):
        @pl.when(core == 0)
        def _():
            reduce_weight(0)

        @pl.when(core == 1)
        def _():
            reduce_weight(1)

    def similarities(s):
        pair[:, pl.ds(s * R, R)] = derivative(dot_nt(tlow[pl.ds(0, R), :], img[pl.ds(s * R, R), :]), s == 0)

    with jax.named_scope("image_wait"):
        @pl.when((core == 0) & ((r != 0) | (z == 0)))
        def _():
            arrived(slot(1), ex_s.at[0], ex_r.at[5])

        @pl.when(core == 0)
        def _():
            send(0, slot(1), slot(2), (ex_s, 8), ex_r.at[6], near(1), lambda: slot(0))

        @pl.when((core == 0) & (r != 0))
        def _():
            arrived(slot(2), ex_s.at[0], ex_r.at[6])
            send("s2", slot(2), slot(3), (ex_s, 11), ex_r.at[7], near(1), lambda: slot(0))

        @pl.when(core == 1)
        def _():
            arrived(slot(1), ex_s.at[0], ex_r.at[5])

        for s in range(2):
            similarities(s)
        for c0, cw in TILES:
            igrad[:, pl.ds(c0, cw)] = dot(pair[:, pl.ds(0, 2 * R)], img[pl.ds(0, 2 * R), pl.ds(c0, cw)])

        @pl.when(r == 0)
        def _():
            arrived(slot(2), ex_s.at[0], ex_r.at[6])
            send("s0", slot(2), slot(3), (ex_s, 11), ex_r.at[7], near(1), lambda: slot(0))

        @pl.when(core == 1)
        def _():
            arrived(slot(2), ex_s.at[0], ex_r.at[6])

        similarities(2)
        arrived(slot(3), ex_s.at[0], ex_r.at[7])

    with jax.named_scope("text_side"):
        similarities(3)
        for c0, cw in TILES:
            igrad[:, pl.ds(c0, cw)] += dot(pair[:, pl.ds(2 * R, 2 * R)], img[pl.ds(2 * R, 2 * R), pl.ds(c0, cw)])

        @pl.loop(0, R // 32, unroll=2)
        def _(i):
            rows = pl.ds(pl.multiple_of(i * 32, 32), 32)
            inv = tlen[rows, :]
            gtext[rows, :] = back(igrad[rows, :], traw[rows, :].astype(F32) * inv, inv).astype(BF16)

    with jax.named_scope("final"):
        for k in range(1, ROW):
            source = lax.rem(r + (ROW - k), ROW)

            @pl.when(lax.rem(source, 2) == 1)
            def _():
                arrived(xr.at[source, :, pl.ds(0, RCOLS[1][1])], xg_s.at[k], xg_r.at[k])

            @pl.when(lax.rem(source, 2) == 0)
            def _():
                arrived(xr.at[source, :, pl.ds(0, RCOLS[0][1])], xg_s.at[k], xg_r.at[k])

        for c in range(2):
            c0, cw = RCOLS[c]
            total = xr[c, :, pl.ds(0, cw)]
            for k in range(1, NX):
                total = total + xr[2 * k + c, :, pl.ds(0, cw)]
            gout[:, pl.ds(c0, cw)] = total

    with jax.named_scope("drain"):
        for only, wait in pending:
            if only is None:
                wait()
        groups = {
            0: core == 0, 1: core == 1, "r0": r == 0, "r2": r == 2, "r3": r == 3, "r5": r == 5, "r1z": (r == 1) & (z == 0), "r1n": (r == 1) & (z != 0), "r7": r == ROW - 1, "i0": r == 0,
            "o7": (core == 1) & (r != ROW - 1), "t3": (core == 0) & (r != 0), "t4": (core == 0) & (r > 2),
            "t2": (core == 1) & (r != 1), "i3": i3, "s0": r == 0, "s2": (core == 0) & (r != 0), "i0e": early, "i7": i7_last, "i6r": (r == 6) & last, "i4r": (r == 4) & last, "i1": (core == 1) & ((r != ROW - 1) | (z != NZ - 1)),
            "i5": r == 5, "i2r": r == 2, "i6": r == ROW - 2,
            "i2": (core == 0) & (r != ROW - 2),
        }
        for group, inside in groups.items():

            @pl.when(inside)
            def _():
                for only, wait in pending:
                    if only == group:
                        wait()


def put_out(gf, gt, gw, gf_out, gt_out, gw_out, sem):
    copies = [pltpu.make_async_copy(a, b, sem.at[i]) for i, (a, b) in enumerate(((gf, gf_out), (gt, gt_out), (gw, gw_out)))]
    for copy in copies:
        copy.start()
    for copy in copies:
        copy.wait()


def on_device(image_features, head_weight, text_embeds, natural_exponent_factor, logit_bias):
    dma = pltpu.SemaphoreType.DMA
    hbm = pl.BlockSpec(memory_space=pltpu.HBM)
    local = pl.BlockSpec(memory_space=pltpu.VMEM)
    scalar = pl.BlockSpec(memory_space=pltpu.SMEM)
    results = pl.pallas_call(
        kernel,
        out_shape=(
            jax.ShapeDtypeStruct((R, D), BF16),
            jax.ShapeDtypeStruct((R, E), BF16),
            jax.ShapeDtypeStruct((SH, E), F32),
        ),
        in_specs=[hbm, hbm, hbm, scalar, scalar],
        out_specs=(local, local, local),
        scratch_shapes=[
            pltpu.VMEM((D, E), BF16),
            pltpu.VMEM((R, D), BF16),
            pltpu.VMEM((R, D), BF16),
            pltpu.VMEM((D, 2 * R), BF16),
            pltpu.VMEM((R, E), F32),
            pltpu.VMEM((R, 1), F32),
            pltpu.VMEM((S * R, E), BF16),
            pltpu.VMEM((R, E), BF16),
            pltpu.VMEM((S * R, E), BF16),
            pltpu.VMEM((R, 1), F32),
            pltpu.VMEM((R, S * R), BF16),
            pltpu.VMEM((2 * R, E), BF16),
            pltpu.VMEM((D, W2), BF16),
            pltpu.VMEM((ROW, SH, E), BF16),
            pltpu.VMEM((BLK, E), F32),
            pltpu.VMEM((36, BLK, W2), BF16),
            pltpu.VMEM((8, BLK, W2), BF16),
            pltpu.VMEM((BLK, W2), F32),
            pltpu.VMEM((ROW, SH, W2), F32),
            pltpu.VMEM((ROW, SH, W2), F32),
            pltpu.VMEM((R, E), F32),
            pltpu.VMEM((R, E), BF16),
            pltpu.VMEM((R, E), BF16),
            dma((3,)),
            dma((ROW,)), dma((ROW,)),
            dma((32,)), dma((32,)),
            dma((32,)), dma((32,)),
            dma((14,)), dma((11,)),
            dma((40,)), dma((36,)),
            dma((ROW,)), dma((ROW,)),
        ],
        compiler_params=pltpu.CompilerParams(
            collective_id=0, has_side_effects=True, vmem_limit_bytes=52 * 1024 * 1024
        ),
    )(*(pltpu.with_memory_space_constraint(a, pltpu.HBM) for a in (image_features, head_weight, text_embeds)), natural_exponent_factor, logit_bias)
    return pl.pallas_call(
        put_out,
        out_shape=tuple(jax.ShapeDtypeStruct(a.shape, a.dtype) for a in results),
        in_specs=[local] * 3,
        out_specs=[hbm] * 3,
        scratch_shapes=[dma((3,))],
        compiler_params=pltpu.CompilerParams(vmem_limit_bytes=8 * 1024 * 1024),
    )(*results)


def solution(mesh):
    split = P("blk", None)
    return jax.shard_map(
        on_device,
        mesh=mesh,
        in_specs=(split, split, split, P(), P()),
        out_specs=(split, split, split),
        check_vma=False,
    )
```
